32 devices in a mesh: seq: 8 (over z, x), batch: 4 (over y, core).
Axes of the slice: x: 2, y: 2, z: 4, core: 2. Of those that a mesh axis runs over, the one named last changes fastest.
Arguments:
- tokens: bfloat16 [4, 2048, 256], P('batch', 'seq'), may hold values from -6 to 6
- out_grad: bfloat16 [4, 2048, 256], P('batch', 'seq'), may hold values from -6 to 6
- in_weight: bfloat16 [256, 768], replicated, may hold values from -0.375 to 0.375
- out_weight: bfloat16 [256, 256], replicated, may hold values from -0.375 to 0.375
- skip_bias: float32 [256], replicated, may hold values from -4 to 4
- embed_weight: float32 [5, 64], replicated, may hold values from -4 to 4
- embed_bias: float32 [64], replicated, may hold values from -4 to 4
- hidden_weight: float32 [64, 64], replicated, may hold values from -0.75 to 0.75
- hidden_bias: float32 [64], replicated, may hold values from -4 to 4
- filter_weight: float32 [64, 256], replicated, may hold values from -0.75 to 0.75
- sine_freq: float32 [2, 64], replicated, may hold values from 0.5 to 3
- decay_rate: float32 [256], replicated, may hold values from 0.0014990234 to 0.0074951174
Outputs:
- grad_tokens: bfloat16 [4, 2048, 256], P('batch', 'seq')
- grad_in_weight: float32 [256, 768], replicated
- grad_out_weight: float32 [256, 256], replicated
- grad_skip_bias: float32 [256], replicated
- grad_embed_weight: float32 [5, 64], replicated
- grad_embed_bias: float32 [64], replicated
- grad_hidden_weight: float32 [64, 64], replicated
- grad_hidden_bias: float32 [64], replicated
- grad_filter_weight: float32 [64, 256], replicated
- grad_sine_freq: float32 [2, 64], replicated
The draws below stay inside these ranges and needn't reach their ends.
All inputs are finite; a program needn't handle non-finite values.
Results may differ from the reference program's by a relative error of at most 0.013.
Values may be sent and summed in bfloat16 or wider, within the bound.
A program may use at most 64 MiB of HBM per device.

```python
import math
import jax
import jax.numpy as jnp
from jax import lax

D = 256
HID = 64
EMB = 5
BATCH = 4
LEN = 2048


def block_scale(own_key, dims, pieces, least, high):
    def one(dim, parts):
        heights = jax.random.uniform(jax.random.fold_in(jax.random.fold_in(own_key, 6), dim), (parts,), jnp.float32, least / len(pieces), high / len(pieces))
        return jnp.repeat(jnp.exp(heights), dims[dim] // parts).reshape((-1,) + (1,) * (len(dims) - dim - 1))

    gain = one(*pieces[0])
    for cut in pieces[1:]:
        gain = gain * one(*cut)
    return gain


def gaussian(key, dims, spread, reach, shards=(), kind=jnp.bfloat16):
    entries = jax.random.normal(key, dims, jnp.float32) * spread
    if len(shards) > 0:
        entries = block_scale(key, dims, shards, -0.22, 0.18) * entries
    return jnp.clip(entries, min=-reach, max=reach).astype(kind)


def setup_inputs(seed: int = 0) -> dict:
    splits = jax.random.split(jax.random.key(seed), 13)
    return {
        "tokens": gaussian(splits[0], (BATCH, LEN, D), 1.0, 6.0, ((0, 4), (1, 8))),
        "out_grad": gaussian(splits[1], (BATCH, LEN, D), 1.0, 6.0, ((0, 4), (1, 8))),
        "in_weight": gaussian(splits[2], (D, 3 * D), D ** -0.5, 0.375),
        "out_weight": gaussian(splits[3], (D, D), D ** -0.5, 0.375),
        "skip_bias": gaussian(splits[4], (D,), 1.0, 4.0, (), jnp.float32),
        "embed_weight": gaussian(splits[5], (EMB, HID), 1.0, 4.0, (), jnp.float32),
        "embed_bias": gaussian(splits[6], (HID,), 1.0, 4.0, (), jnp.float32),
        "hidden_weight": gaussian(splits[7], (HID, HID), HID ** -0.5, 0.75, (), jnp.float32),
        "hidden_bias": gaussian(splits[8], (HID,), 1.0, 4.0, (), jnp.float32),
        "filter_weight": gaussian(splits[9], (HID, D), HID ** -0.5, 0.75, (), jnp.float32),
        "sine_freq": jnp.clip(jax.random.uniform(splits[10], (2, HID), jnp.float32, 0.5, 3.0), 0.5, 3.0),
        "decay_rate": jnp.clip(jnp.exp(jax.random.uniform(splits[11], (D,), jnp.float32, math.log(0.0014990234), math.log(0.0074951174))), 0.0014990234, 0.0074951174),
    }


highest = lax.Precision.HIGHEST

def embedding(positions, length, band_count):
    scaled = positions / length
    rows_list = [scaled]
    for band_index in range(1, band_count + 1):
        angle = 2.0 * math.pi * band_index * scaled
        rows_list.append(jnp.cos(angle))
        rows_list.append(jnp.sin(angle))
    return jnp.stack(rows_list, axis=1)

def reference(tokens, out_grad, in_weight, out_weight, skip_bias, embed_weight, embed_bias, hidden_weight, hidden_bias, filter_weight, sine_freq, decay_rate):
    positions = jnp.arange(LEN, dtype=jnp.float32)
    band_count = (EMB - 1) // 2
    embed_rows = embedding(positions, LEN, band_count)
    modul = 4.0 * jnp.exp(-decay_rate[None, :] * positions[:, None]) / math.sqrt(LEN)

    def filter_net(weight_one, bias_one, weight_two, bias_two, weight_three, freqs):
        pre_one = jnp.dot(embed_rows, weight_one, precision=highest) + bias_one
        act_one = jnp.sin(freqs[0] * pre_one)
        pre_two = jnp.dot(act_one, weight_two, precision=highest) + bias_two
        act_two = jnp.sin(freqs[1] * pre_two)
        return jnp.dot(act_two, weight_three, precision=highest) * modul
    filt, pullback = jax.vjp(filter_net, embed_weight, embed_bias, hidden_weight, hidden_bias, filter_weight, sine_freq)
    total = 2 * LEN
    filt_spec = jnp.fft.rfft(filt, n=total, axis=0)

    def one_sequence(inputs):
        tokens_one, grads_one = inputs
        projected = jnp.dot(tokens_one, in_weight, preferred_element_type=jnp.float32)
        gate_out = projected[:, :D].astype(jnp.bfloat16)
        gate_in = projected[:, D:2 * D].astype(jnp.bfloat16)
        values_in = projected[:, 2 * D:].astype(jnp.bfloat16)
        mixed = (values_in.astype(jnp.float32) * gate_in.astype(jnp.float32)).astype(jnp.bfloat16)
        grad_gated = jnp.dot(grads_one, out_weight.T, preferred_element_type=jnp.float32).astype(jnp.bfloat16)
        grad_conv = (grad_gated.astype(jnp.float32) * gate_out.astype(jnp.float32)).astype(jnp.bfloat16)
        mixed_float = mixed.astype(jnp.float32)
        grad_float = grad_conv.astype(jnp.float32)
        mixed_spec = jnp.fft.rfft(mixed_float, n=total, axis=0)
        grad_spec = jnp.fft.rfft(grad_float, n=total, axis=0)
        conv = jnp.fft.irfft(mixed_spec * filt_spec, n=total, axis=0)[:LEN]
        conv = (conv + skip_bias[None, :] * mixed_float).astype(jnp.bfloat16)
        grad_mixed = jnp.fft.irfft(grad_spec * jnp.conj(filt_spec), n=total, axis=0)[:LEN]
        grad_mixed = (grad_mixed + skip_bias[None, :] * grad_float).astype(jnp.bfloat16)
        grad_filt = jnp.fft.irfft(grad_spec * jnp.conj(mixed_spec), n=total, axis=0)[:LEN]
        conv_float = conv.astype(jnp.float32)
        gated = (gate_out.astype(jnp.float32) * conv_float).astype(jnp.bfloat16)
        grad_out_w = jnp.dot(gated.T, grads_one, preferred_element_type=jnp.float32)
        grad_gate_out = (grad_gated.astype(jnp.float32) * conv_float).astype(jnp.bfloat16)
        grad_gate_in = (grad_mixed.astype(jnp.float32) * values_in.astype(jnp.float32)).astype(jnp.bfloat16)
        grad_values = (grad_mixed.astype(jnp.float32) * gate_in.astype(jnp.float32)).astype(jnp.bfloat16)
        grad_proj = jnp.concatenate([grad_gate_out, grad_gate_in, grad_values], axis=1)
        grad_tok = jnp.dot(grad_proj, in_weight.T, preferred_element_type=jnp.float32).astype(jnp.bfloat16)
        grad_in_w = jnp.dot(tokens_one.T, grad_proj, preferred_element_type=jnp.float32)
        grad_bias = lax.optimization_barrier(jnp.sum(grad_float * mixed_float, axis=0))
        return (grad_tok, grad_in_w, grad_out_w, grad_bias, grad_filt)
    results = lax.map(one_sequence, (tokens, out_grad))
    grad_scale = 1.0 / math.sqrt(BATCH * LEN)
    filter_scale = grad_scale / 4.0
    grad_filt_total = lax.optimization_barrier(jnp.sum(results[4], axis=0))
    filter_grads = pullback(grad_filt_total)
    return (results[0], lax.optimization_barrier(jnp.sum(results[1], axis=0)) * grad_scale, lax.optimization_barrier(jnp.sum(results[2], axis=0)) * grad_scale, lax.optimization_barrier(jnp.sum(results[3], axis=0)) * grad_scale, filter_grads[0] * filter_scale, filter_grads[1] * filter_scale, filter_grads[2] * filter_scale, filter_grads[3] * filter_scale, filter_grads[4] * filter_scale, filter_grads[5] * filter_scale)
```

```python
import functools
import math

import jax
import jax.numpy as jnp
import numpy as np
from jax import lax
from jax.experimental import pallas as pl
from jax.experimental.pallas import tpu as pltpu
from jax.sharding import PartitionSpec as P

highest = lax.Precision.HIGHEST
MESH = pl.DeviceIdType.MESH
LANES = 128
VMEM_BYTES = 66 * 1000 * 1000


def factor(length):
    total = 2 * length
    first_len = 2
    while first_len * first_len < total and total % (2 * first_len) == 0:
        first_len = first_len * 2
    return first_len, total // first_len


def make_tables(length):
    total = 2 * length
    first_len, second_len = factor(length)
    half = first_len // 2
    kept = half + 1
    pad = -(-kept // 8) * 8
    k1 = np.arange(kept)[None, :, None]
    n1 = np.arange(half)[None, None, :]
    n2 = np.arange(second_len)[:, None, None]
    angle = 2.0 * np.pi * ((k1 * (n1 * second_len + n2)) % total) / total
    fwd = np.zeros((second_len, 2 * pad, half), np.float32)
    fwd[:, :kept] = np.cos(angle)
    fwd[:, pad : pad + kept] = -np.sin(angle)
    weight = np.where((k1 == 0) | (k1 == half), 1.0, 2.0) / total
    inv = np.zeros((second_len, half, 2 * pad), np.float32)
    inv[:, :, :kept] = np.swapaxes(weight * np.cos(angle), 1, 2)
    inv[:, :, pad : pad + kept] = np.swapaxes(-weight * np.sin(angle), 1, 2)
    index = np.arange(second_len)
    small = 2.0 * np.pi * ((index[:, None] * index[None, :]) % second_len) / second_len
    cos, sin = np.cos(small), np.sin(small)
    inner = np.block([[cos, sin], [-sin, cos]])
    outer = np.block([[cos, -sin], [sin, cos]])
    return tuple(jnp.asarray(t, jnp.bfloat16) for t in (fwd, inv, inner, outer))


def lane_roll(value, shift):
    shift = shift % LANES
    return value if shift == 0 else pltpu.roll(value, shift, 1)


def dot_as(left, right, dims):
    return lax.dot_general(
        left,
        right,
        ((dims[:1], dims[1:]), ((), ())),
        precision=highest,
        preferred_element_type=jnp.float32,
    )


def step_kernel(
    axis_n,
    batch_n,
    chan,
    scale,
    tok_hbm,
    og_hbm,
    inw_hbm,
    outw_hbm,
    embed_hbm,
    fwd_hbm,
    inv_hbm,
    inner_hbm,
    outer_hbm,
    embed_raw,
    embed_b,
    hidden_b,
    freqs,
    hidden_w,
    filter_w,
    decay_in,
    skip_in,
    gt_out,
    a_out,
    b_out,
    tok,
    og,
    inw,
    outw,
    embed,
    fwd,
    inv,
    inner,
    outer,
    load_sems,
    send_one,
    recv_one,
    send_two,
    recv_two,
    gates,
    x_buf,
    y_out,
    z_buf,
    v_buf,
    net,
    filt_pk,
    send_grad,
    grad_pk,
    modul,
    conv_buf,
    sems,
    net_sems,
    pk_out,
    extra,
    embed_w,
    vectors,
    *sum_scratch,
):
    n = axis_n
    me = lax.axis_index("seq")
    me_b = lax.axis_index("batch")
    pos, width = tok.shape
    rows = send_one.shape[1]
    fold = pos // rows
    step = 2 * chan
    second_len, double_pad, half = fwd.shape
    pad = double_pad // 2
    kept = half + 1
    f32, bf16 = jnp.float32, jnp.bfloat16

    barrier = pltpu.get_barrier_semaphore()
    for axis, own_at, count in (("seq", me, n), ("batch", me_b, batch_n)):
        for k in range(1, count):
            pl.semaphore_signal(
                barrier, inc=1, device_id={axis: lax.rem(own_at + k, count)}, device_id_type=MESH
            )

    quarter = embed.shape[1]
    own_part = pl.ds(pl.multiple_of(me_b * quarter, LANES), quarter)
    loads = [
        pltpu.make_async_copy(src, dst, load_sems.at[i])
        for i, (src, dst) in enumerate(
            (
                (tok_hbm, tok),
                (inw_hbm, inw),
                (og_hbm, og),
                (outw_hbm, outw),
                (embed_hbm.at[:, own_part], embed),
                (fwd_hbm, fwd),
                (inner_hbm, inner),
                (outer_hbm, outer),
                (inv_hbm, inv),
            )
        )
    ]
    for item in loads:
        item.start()
    for item in loads[:4]:
        item.wait()

    proj = jnp.dot(tok[...], inw[...], preferred_element_type=f32)
    gate_out = proj[:, :width].astype(bf16)
    gate_in = proj[:, width : 2 * width].astype(bf16)
    values = proj[:, 2 * width :].astype(bf16)
    gated_grad = lax.dot_general(
        og[...], outw[...], (((1,), (1,)), ((), ())), preferred_element_type=f32
    ).astype(bf16)
    gates[0] = gate_out
    gates[1] = gate_in
    gates[2] = values
    gates[3] = gated_grad
    mixed = (values.astype(f32) * gate_in.astype(f32)).astype(bf16).astype(f32)
    grad = (gated_grad.astype(f32) * gate_out.astype(f32)).astype(bf16).astype(f32)
    bias_sum = jnp.sum(mixed * grad, axis=0, keepdims=True) * scale

    lane = lax.broadcasted_iota(jnp.int32, (rows, LANES), 1)
    lane_full = lax.broadcasted_iota(jnp.int32, (pos, LANES), 1)
    for d in range(n):
        tile, off = (d * chan) // LANES * LANES, (d * chan) % LANES
        both = jnp.where(
            lane_full < chan,
            lane_roll(mixed[:, tile : tile + LANES], -off),
            lane_roll(grad[:, tile : tile + LANES], chan - off),
        )
        packed = both[:rows]
        for j in range(1, fold):
            packed = jnp.where(
                lane >= j * step, lane_roll(both[j * rows : (j + 1) * rows], j * step), packed
            )
        send_one[d] = packed.astype(bf16)

    pl.semaphore_wait(barrier, n + batch_n - 2)

    def copy(send, recv, which, k):
        dest = lax.rem(me + k, n)
        return pltpu.make_async_remote_copy(
            src_ref=send.at[dest],
            dst_ref=recv.at[me],
            send_sem=sems.at[2 * which, k],
            recv_sem=sems.at[2 * which + 1, k],
            device_id={"seq": dest},
            device_id_type=MESH,
        )

    for k in range(1, n):
        copy(send_one, recv_one, 0, k).start()
    recv_one[me] = send_one[me]
    v_buf[...] = jnp.zeros_like(v_buf)
    extra[...] = jnp.zeros_like(extra)
    length = x_buf.shape[0]
    hid = hidden_w.shape[0]
    tiles = width // LANES

    def select_own(value, target):
        lane_v = lax.broadcasted_iota(jnp.int32, (value.shape[0], LANES), 1)
        got = jnp.zeros((value.shape[0], LANES), f32)
        for i in range(n):
            tile, off = (i * chan) // LANES * LANES, (i * chan) % LANES
            part = lane_roll(value[:, tile : tile + LANES], target - off)
            got = jnp.where(jnp.logical_and(me == i, lane_v >= 0), part, got)
        return jnp.where((lane_v >= target) & (lane_v < target + chan), got, 0.0)

    parts = LANES // chan
    sub = quarter // parts
    weight = select_own(filter_w[...], 0)
    decay_own = select_own(decay_in[...], 0)
    decay = decay_own
    for j in range(1, parts):
        decay = decay + lane_roll(decay_own, j * chan)
    skip = select_own(skip_in[...], 0) + select_own(skip_in[...], chan)
    inputs = embed_raw.shape[0]
    embed_w[...] = jnp.zeros_like(embed_w)
    embed_w[0:inputs, :] = embed_raw[...]
    embed_w[inputs : inputs + 1, :] = embed_b[...]
    vectors[...] = jnp.zeros_like(vectors)
    vectors[0:2, :] = freqs[...]
    vectors[2:3, :] = hidden_b[...]
    eye = (
        lax.broadcasted_iota(jnp.int32, (8, 8), 0) == lax.broadcasted_iota(jnp.int32, (8, 8), 1)
    ).astype(f32)
    columns = dot_as(vectors[...], eye, (0, 0))
    freq_one, freq_two = columns[:, 0:1], columns[:, 1:2]
    tile = min(256, quarter)
    loads[4].wait()

    def net_forward(i, _):
        at = pl.ds(pl.multiple_of(i * tile, LANES), tile)
        pre_one = dot_as(embed_w[...], embed[:, at], (0, 0))
        act_one, cos_one = sine_cosine(freq_one * pre_one)
        pre_two = dot_as(hidden_w[...], act_one, (0, 0)) + columns[:, 2:3]
        act_two, cos_two = sine_cosine(freq_two * pre_two)
        net[0, :, at] = pre_one
        net[1, :, at] = act_one
        net[2, :, at] = cos_one
        net[3, :, at] = pre_two
        net[4, :, at] = act_two
        net[5, :, at] = cos_two
        return 0

    lax.fori_loop(0, quarter // tile, net_forward, 0, unroll=2 if quarter // tile % 2 == 0 else 1)
    lane_s = lax.broadcasted_iota(jnp.int32, (sub, LANES), 1)
    time = lax.broadcasted_iota(jnp.int32, (sub, LANES), 0) + me_b * quarter
    for j in range(1, parts):
        time = time + jnp.where(lane_s >= j * chan, sub, 0)
    modul[...] = jnp.exp(-decay * time.astype(f32)) * (4.0 / math.sqrt(length))
    packed_filt = jnp.zeros((sub, LANES), f32)
    for j in range(parts):
        packed_filt = packed_filt + dot_as(
            net[4, :, j * sub : (j + 1) * sub], lane_roll(weight, j * chan), (0, 0)
        )
    filt_pk[me_b] = (packed_filt * modul[...]).astype(bf16)

    def share(which, k):
        dest = lax.rem(me_b + k, batch_n)
        return pltpu.make_async_remote_copy(
            src_ref=filt_pk.at[me_b] if which == 0 else send_grad.at[dest],
            dst_ref=filt_pk.at[me_b] if which == 0 else grad_pk.at[me_b],
            send_sem=net_sems.at[2 * which, k],
            recv_sem=net_sems.at[2 * which + 1, k],
            device_id={"batch": dest},
            device_id_type=MESH,
        )

    for k in range(1, batch_n):
        share(0, k).start()
    for k in range(1, n):
        copy(send_one, recv_one, 0, k).wait()
    for k in range(1, batch_n):
        share(0, k).wait()

    for s in range(n):
        block = recv_one[s].astype(f32)
        for j in range(fold):
            start = s * pos + j * rows
            q, rest = start // quarter, start % quarter
            p, row = rest // sub, rest % sub
            filt = lane_roll(filt_pk[q, row : row + rows, :].astype(f32), step - p * chan)
            x_buf[pl.ds(start, rows), :] = jnp.where(
                lane < step, lane_roll(block, -j * step), filt
            )
    for item in loads[5:]:
        item.wait()

    def stage_one(n2, _):
        part = x_buf[pl.ds(n2, half, stride=second_len), :].astype(bf16)
        z_buf[pl.ds(pl.multiple_of(n2 * double_pad, 8), double_pad), :] = jnp.dot(
            fwd[n2], part, preferred_element_type=f32
        )
        return 0

    lax.fori_loop(0, second_len, stage_one, 0, unroll=16)

    lane_k = lax.broadcasted_iota(jnp.int32, (second_len, LANES), 1)
    low = lane_k < step
    mid = (lane_k >= chan) & (lane_k < step)
    sign = jnp.where((lane_k >= chan), -1.0, 1.0).astype(f32)

    def stage_two(k1, _):
        stacked = jnp.concatenate(
            [
                z_buf[pl.ds(k1, second_len, stride=double_pad), :],
                z_buf[pl.ds(pad + k1, second_len, stride=double_pad), :],
            ],
            axis=0,
        ).astype(bf16)
        spec = jnp.dot(inner[...], stacked, preferred_element_type=f32)
        re, im = spec[:second_len], spec[second_len:]
        left_re = jnp.where(low, re, lane_roll(re, chan))
        left_im = jnp.where(low, im, lane_roll(im, chan))
        right_re = jnp.where(mid, lane_roll(re, -chan), lane_roll(re, -step))
        right_im = jnp.where(mid, lane_roll(im, -chan), lane_roll(im, -step)) * sign
        corr_re = jnp.where(lane_k < step, right_re, lane_roll(re, step))
        corr_im = jnp.where(lane_k < step, right_im, lane_roll(im, step) * sign)
        out = jnp.concatenate(
            [
                left_re * corr_re - left_im * corr_im,
                left_re * corr_im + left_im * corr_re,
            ],
            axis=0,
        ).astype(bf16)
        back = jnp.dot(outer[...], out, preferred_element_type=f32)
        v_buf[pl.ds(k1, second_len, stride=double_pad), :] = back[:second_len]
        v_buf[pl.ds(pad + k1, second_len, stride=double_pad), :] = back[second_len:]
        return 0

    unroll = 11 if kept % 11 == 0 else 3 if kept % 3 == 0 else 5 if kept % 5 == 0 else 1
    lax.fori_loop(0, kept, stage_two, 0, unroll=unroll)

    def stage_three(n2, _):
        part = v_buf[pl.ds(pl.multiple_of(n2 * double_pad, 8), double_pad), :].astype(bf16)
        at = pl.ds(n2, half, stride=second_len)
        y_out[at, :] = (
            jnp.dot(inv[n2], part, preferred_element_type=f32) + skip * x_buf[at, :]
        )
        return 0

    lax.fori_loop(0, second_len, stage_three, 0, unroll=16)

    for d in range(n):
        packed = y_out[pl.ds(d * pos, rows), :]
        for j in range(1, fold):
            packed = jnp.where(
                lane >= j * step,
                lane_roll(y_out[pl.ds(d * pos + j * rows, rows), :], j * step),
                packed,
            )
        send_two[d] = packed.astype(bf16)
    for k in range(1, n):
        copy(send_two, recv_two, 1, k).start()
    recv_two[me] = send_two[me]

    owned = [(lane_s >= j * chan) & (lane_s < (j + 1) * chan) for j in range(parts)]
    for q in range(batch_n):
        packed = jnp.zeros((sub, LANES), f32)
        for j in range(parts):
            part = y_out[pl.ds(q * quarter + j * sub, sub), :]
            packed = jnp.where(owned[j], lane_roll(part, j * chan - step), packed)
        send_grad[q] = packed.astype(bf16)
    for k in range(1, batch_n):
        share(1, k).start()
    grad_pk[me_b] = send_grad[me_b]
    for k in range(1, batch_n):
        share(1, k).wait()
    total = grad_pk[0].astype(f32)
    for q in range(1, batch_n):
        total = total + grad_pk[q].astype(f32)
    grad_kernel = total * modul[...]

    em = embed.shape[0]
    lane_w = lax.broadcasted_iota(jnp.int32, (hid, LANES), 1)
    grad_weight = jnp.zeros((hid, LANES), f32)
    for j in range(parts):
        at = slice(j * sub, (j + 1) * sub)
        got = dot_as(net[4, :, at], grad_kernel, (1, 0))
        grad_weight = grad_weight + lane_roll(
            jnp.where((lane_w >= j * chan) & (lane_w < (j + 1) * chan), got, 0.0), -j * chan
        )
        net[5, :, at] = dot_as(lane_roll(weight, j * chan), grad_kernel, (1, 1)) * net[5, :, at]

    def net_backward(i, carry):
        at = pl.ds(pl.multiple_of(i * tile, LANES), tile)
        grad_act_two = net[5, :, at]
        grad_pre_two = grad_act_two * freq_two
        grad_hidden = dot_as(net[1, :, at], grad_pre_two, (1, 1))
        grad_act_one = dot_as(hidden_w[...], grad_pre_two, (1, 0)) * net[2, :, at]
        grad_pre_one = grad_act_one * freq_one
        stacked = jnp.concatenate(
            [grad_pre_one, grad_pre_two, grad_act_one * net[0, :, at], grad_act_two * net[3, :, at]],
            axis=0,
        )
        return carry[0] + grad_hidden, carry[1] + dot_as(embed[:, at], stacked, (1, 1))

    zeros = lambda r, c: jnp.zeros((r, c), f32)
    both_sums = lax.fori_loop(
        0,
        quarter // tile,
        net_backward,
        (zeros(hid, hid), zeros(em, 4 * hid)),
        unroll=2 if quarter // tile % 2 == 0 else 1,
    )
    sums = (grad_weight, both_sums[0]) + tuple(
        both_sums[1][:, i * hid : (i + 1) * hid] for i in range(4)
    )
    sums = tuple(term * (scale * 0.25) for term in sums)
    lane_h = lax.broadcasted_iota(jnp.int32, (hid, LANES), 1)
    for tile in range(tiles):
        placed = zeros(hid, LANES)
        for i in range(n):
            if (i * chan) // LANES == tile:
                off = (i * chan) % LANES
                mask = (lane_h >= off) & (lane_h < off + chan) & (me == i)
                placed = jnp.where(mask, lane_roll(sums[0], off), placed)
        extra[tile * hid : (tile + 1) * hid, :] = placed
    base = tiles * hid
    extra[base : base + hid, 0:hid] = sums[1]
    base += hid
    for term in sums[2:]:
        extra[base : base + em, 0:hid] = term
        base += em
    for tile in range(tiles):
        extra[base + tile : base + tile + 1, :] = bias_sum[:, tile * LANES : (tile + 1) * LANES]

    main_sum = make_sum(n, batch_n, pk_out, a_out, sum_scratch[:5], 0)
    extra_sum = make_sum(n, batch_n, extra, b_out, sum_scratch[5:], 1)
    extra_sum.start(0)
    for k in range(1, n):
        copy(send_two, recv_two, 1, k).wait()

    per_tile = LANES // chan
    for tile in range(width // LANES):
        for j in range(fold):
            conv_acc = jnp.zeros((rows, LANES), f32)
            grad_acc = jnp.zeros((rows, LANES), f32)
            for i in range(per_tile):
                block = recv_two[tile * per_tile + i].astype(f32)
                own = (lane >= i * chan) & (lane < (i + 1) * chan)
                conv_acc = jnp.where(own, lane_roll(block, i * chan - j * step), conv_acc)
                grad_acc = jnp.where(own, lane_roll(block, i * chan - j * step - chan), grad_acc)
            at = pl.ds(j * rows, rows)
            conv_buf[0, at, tile * LANES : (tile + 1) * LANES] = conv_acc
            conv_buf[1, at, tile * LANES : (tile + 1) * LANES] = grad_acc

    conv = conv_buf[0]
    grad_mixed = conv_buf[1]
    gated = (gates[0].astype(f32) * conv).astype(bf16)
    grad_proj = jnp.concatenate(
        [
            (gates[3].astype(f32) * conv).astype(bf16),
            (grad_mixed * gates[2].astype(f32)).astype(bf16),
            (grad_mixed * gates[1].astype(f32)).astype(bf16),
        ],
        axis=1,
    )
    first = (((0,), (0,)), ((), ()))
    grad_in = lax.dot_general(tok[...], grad_proj, first, preferred_element_type=f32) * scale
    grad_out = lax.dot_general(gated, og[...], first, preferred_element_type=f32) * scale
    at = 0
    for block in (grad_in, grad_out):
        for j in range(block.shape[1] // LANES):
            pk_out[at : at + width, :] = block[:, j * LANES : (j + 1) * LANES].astype(bf16)
            at += width
    main_sum.start(0)
    gt_out[...] = lax.dot_general(
        grad_proj, inw[...], (((1,), (1,)), ((), ())), preferred_element_type=f32
    ).astype(bf16)
    for phase in range(4):
        for stream in (extra_sum, main_sum):
            stream.finish(phase)
            if phase < 3:
                stream.start(phase + 1)
            else:
                stream.out[...] = stream.whole[...]


class make_sum:
    def __init__(self, ns, nb, src, out, scratch, which):
        self.ns, self.nb, self.src, self.out, self.which = ns, nb, src, out, which
        self.got, self.part, self.got_two, self.whole, self.sems = scratch
        self.me_s, self.me_b = lax.axis_index("seq"), lax.axis_index("batch")
        self.unit = 16 if src.dtype == jnp.bfloat16 else 8
        self.long, self.short = self.got.shape[1], self.got_two.shape[1]

    def rows(self, start, size):
        return pl.ds(pl.multiple_of(start, self.unit), size)

    def copies(self, phase):
        axis, me, n = (
            ("seq", self.me_s, self.ns) if phase in (1, 2) else ("batch", self.me_b, self.nb)
        )
        made = []
        for k in range(1, n):
            dest = lax.rem(me + k, n)
            if phase == 0:
                src, dst = self.src.at[self.rows(dest * self.long, self.long)], self.got.at[k - 1]
            elif phase == 1:
                src = self.part.at[self.rows(dest * self.short, self.short)]
                dst = self.got_two.at[k - 1]
            else:
                start, size = self.me_b * self.long, self.long
                if phase == 2:
                    start, size = start + self.me_s * self.short, self.short
                src = dst = self.whole.at[self.rows(start, size)]
            made.append(
                pltpu.make_async_remote_copy(
                    src_ref=src,
                    dst_ref=dst,
                    send_sem=self.sems.at[phase, 0, k],
                    recv_sem=self.sems.at[phase, 1, k],
                    device_id={axis: dest},
                    device_id_type=MESH,
                )
            )
        return made

    def start(self, phase):
        for item in self.copies(phase):
            item.start()

    def finish(self, phase):
        for item in self.copies(phase):
            item.wait()
        if phase == 0:
            total = self.src[self.rows(self.me_b * self.long, self.long), :].astype(jnp.float32)
            for k in range(1, self.nb):
                total = total + self.got[k - 1].astype(jnp.float32)
            self.part[...] = total.astype(self.part.dtype)
        if phase == 1:
            total = self.part[self.rows(self.me_s * self.short, self.short), :].astype(jnp.float32)
            for k in range(1, self.ns):
                total = total + self.got_two[k - 1].astype(jnp.float32)
            start = self.me_b * self.long + self.me_s * self.short
            self.whole[self.rows(start, self.short), :] = total.astype(self.whole.dtype)


def unpack_kernel(main, extra, tokens_in, tokens_out, g_in, g_out, skip, emb, emb_b, hidden, hidden_b, filt, freq):
    width = g_out.shape[0]
    hid = hidden.shape[0]
    tokens_out[...] = tokens_in[...]
    at = 0
    for ref in (g_in, g_out):
        for j in range(ref.shape[1] // LANES):
            ref[:, j * LANES : (j + 1) * LANES] = main[at : at + width, :].astype(jnp.float32)
            at += width
    tiles = width // LANES
    for j in range(tiles):
        filt[:, j * LANES : (j + 1) * LANES] = extra[j * hid : (j + 1) * hid, :]
    base = tiles * hid
    hidden[...] = extra[base : base + hid, 0:hid]
    base += hid
    count = emb.shape[0]
    em = -(-(count + 1) // 8) * 8
    emb[...] = extra[base : base + count, 0:hid]
    emb_b[...] = extra[base + count : base + count + 1, 0:hid]
    hidden_b[...] = extra[base + em + count : base + em + count + 1, 0:hid]
    freq[0:1, :] = extra[base + 2 * em + count : base + 2 * em + count + 1, 0:hid]
    freq[1:2, :] = extra[base + 3 * em + count : base + 3 * em + count + 1, 0:hid]
    base += 4 * em
    for j in range(tiles):
        skip[:, j * LANES : (j + 1) * LANES] = extra[base + j : base + j + 1, :]


def vmem(count):
    return [pl.BlockSpec(memory_space=pltpu.VMEM)] * count


def sine_cosine(angle):
    turns = jnp.round(angle * (1.0 / (2.0 * math.pi)))
    reduced = angle - turns * 6.28125
    reduced = reduced - turns * 0.0019350051879882812
    reduced = reduced - turns * 3.0199157663146e-07
    half = reduced * 0.5
    square = half * half
    sin = half * (
        1.0
        + square
        * (-1.0 / 6 + square * (1.0 / 120 + square * (-1.0 / 5040 + square * (1.0 / 362880 - square / 39916800.0))))
    )
    cos = 1.0 + square * (
        -0.5
        + square
        * (1.0 / 24 + square * (-1.0 / 720 + square * (1.0 / 40320 + square * (-1.0 / 3628800 + square / 479001600.0))))
    )
    return 2.0 * sin * cos, 1.0 - 2.0 * sin * sin


def embedding(length, count):
    rows = np.zeros((-(-(count + 1) // 8) * 8, length), np.float32)
    scaled = np.arange(length) / length
    rows[0] = scaled
    for band_index in range(1, (count - 1) // 2 + 1):
        rows[2 * band_index - 1] = np.cos(2.0 * np.pi * band_index * scaled)
        rows[2 * band_index] = np.sin(2.0 * np.pi * band_index * scaled)
    rows[count] = 1.0
    return jnp.asarray(rows)


def shards(
    tokens,
    out_grad,
    in_weight,
    out_weight,
    skip_bias,
    embed_weight,
    embed_bias,
    hidden_weight,
    hidden_bias,
    filter_weight,
    sine_freq,
    decay_rate,
):
    f32, bf16 = jnp.float32, jnp.bfloat16
    tok, og = tokens[0], out_grad[0]
    pos, width = tok.shape
    ns, nb = lax.axis_size("seq"), lax.axis_size("batch")
    length = pos * ns
    chan = width // ns
    hid = hidden_weight.shape[0]
    count = embed_weight.shape[0]
    embed = embedding(length, count)
    em = embed.shape[0]

    fwd, inv, inner, outer = make_tables(length)
    second_len, double_pad, half = fwd.shape
    rows = pos // (LANES // (2 * chan))
    tiles = width // LANES
    unit = ns * nb * 16
    main_rows = -(-4 * width * tiles // unit) * unit
    unit = ns * nb * 8
    extra_rows = -(-(tiles * hid + hid + 4 * em + tiles) // unit) * unit
    pair = (ns, rows, LANES)
    shared = (nb, length // nb // (LANES // chan), LANES)
    spectral = (second_len * double_pad, LANES)
    scratch = []
    for total, kind in ((main_rows, bf16), (extra_rows, f32)):
        scratch += [
            pltpu.VMEM((nb - 1, total // nb, LANES), kind),
            pltpu.VMEM((total // nb, LANES), kind),
            pltpu.VMEM((ns - 1, total // nb // ns, LANES), kind),
            pltpu.VMEM((total, LANES), kind),
            pltpu.SemaphoreType.DMA((4, 2, max(ns, nb))),
        ]
    grad_tokens, main, extra = pl.pallas_call(
        functools.partial(step_kernel, ns, nb, chan, 1.0 / math.sqrt(nb * length)),
        out_shape=(
            jax.ShapeDtypeStruct((pos, width), bf16),
            jax.ShapeDtypeStruct((main_rows, LANES), bf16),
            jax.ShapeDtypeStruct((extra_rows, LANES), f32),
        ),
        in_specs=[pl.BlockSpec(memory_space=pl.ANY)] * 9 + vmem(8),
        out_specs=tuple(vmem(3)),
        scratch_shapes=[
            pltpu.VMEM(tok.shape, bf16),
            pltpu.VMEM(og.shape, bf16),
            pltpu.VMEM(in_weight.shape, bf16),
            pltpu.VMEM(out_weight.shape, bf16),
            pltpu.VMEM((em, length // nb), f32),
            pltpu.VMEM(fwd.shape, bf16),
            pltpu.VMEM(inv.shape, bf16),
            pltpu.VMEM(inner.shape, bf16),
            pltpu.VMEM(outer.shape, bf16),
            pltpu.SemaphoreType.DMA((9,)),
            pltpu.VMEM(pair, bf16),
            pltpu.VMEM(pair, bf16),
            pltpu.VMEM(pair, bf16),
            pltpu.VMEM(pair, bf16),
            pltpu.VMEM((4, pos, width), bf16),
            pltpu.VMEM((length, LANES), f32),
            pltpu.VMEM((length, LANES), f32),
            pltpu.VMEM(spectral, f32),
            pltpu.VMEM(spectral, f32),
            pltpu.VMEM((6, hid, length // nb), f32),
            pltpu.VMEM(shared, bf16),
            pltpu.VMEM(shared, bf16),
            pltpu.VMEM(shared, bf16),
            pltpu.VMEM(shared[1:], f32),
            pltpu.VMEM((2, pos, width), f32),
            pltpu.SemaphoreType.DMA((4, ns)),
            pltpu.SemaphoreType.DMA((4, nb)),
            pltpu.VMEM((main_rows, LANES), bf16),
            pltpu.VMEM((extra_rows, LANES), f32),
            pltpu.VMEM((em, hid), f32),
            pltpu.VMEM((8, hid), f32),
        ]
        + scratch,
        compiler_params=pltpu.CompilerParams(
            collective_id=0, has_side_effects=True, vmem_limit_bytes=VMEM_BYTES
        ),
        name="step",
    )(
        tok,
        og,
        in_weight,
        out_weight,
        embed,
        fwd,
        inv,
        inner,
        outer,
        embed_weight,
        embed_bias[None],
        hidden_bias[None],
        sine_freq,
        hidden_weight,
        filter_weight,
        decay_rate[None],
        skip_bias[None],
    )

    shapes = (
        (width, 3 * width),
        (width, width),
        (1, width),
        (count, hid),
        (1, hid),
        (hid, hid),
        (1, hid),
        (hid, width),
        (2, hid),
    )
    out = pl.pallas_call(
        unpack_kernel,
        out_shape=(jax.ShapeDtypeStruct((pos, width), bf16),)
        + tuple(jax.ShapeDtypeStruct(shape, f32) for shape in shapes),
        in_specs=vmem(3),
        out_specs=tuple(vmem(1 + len(shapes))),
        name="unpack",
    )(main, extra, grad_tokens)
    return (
        out[0][None],
        out[1],
        out[2],
        out[3][0],
        out[4],
        out[5][0],
        out[6],
        out[7][0],
        out[8],
        out[9],
    )


def solution(mesh):
    batched = P("batch", "seq", None)
    return jax.shard_map(
        shards,
        mesh=mesh,
        in_specs=(batched, batched) + (P(),) * 10,
        out_specs=(batched,) + (P(),) * 9,
        check_vma=False,
    )
```

```python
import functools
import math

import jax
import jax.numpy as jnp
import numpy as np
from jax import lax
from jax.experimental import pallas as pl
from jax.experimental.pallas import tpu as pltpu
from jax.sharding import PartitionSpec as P

highest = lax.Precision.HIGHEST
MESH = pl.DeviceIdType.MESH
LANES = 128
VMEM_BYTES = 66 * 1000 * 1000


def factor(length):
    total = 2 * length
    first_len = 2
    while first_len * first_len < total and total % (2 * first_len) == 0:
        first_len = first_len * 2
    return first_len, total // first_len


def make_tables(length):
    total = 2 * length
    first_len, second_len = factor(length)
    half = first_len // 2
    kept = half + 1
    pad = -(-kept // 8) * 8
    k1 = np.arange(kept)[None, :, None]
    n1 = np.arange(half)[None, None, :]
    n2 = np.arange(second_len)[:, None, None]
    angle = 2.0 * np.pi * ((k1 * (n1 * second_len + n2)) % total) / total
    fwd = np.zeros((second_len, 2 * pad, half), np.float32)
    fwd[:, :kept] = np.cos(angle)
    fwd[:, pad : pad + kept] = -np.sin(angle)
    weight = np.where((k1 == 0) | (k1 == half), 1.0, 2.0) / total
    inv = np.zeros((second_len, half, 2 * pad), np.float32)
    inv[:, :, :kept] = np.swapaxes(weight * np.cos(angle), 1, 2)
    inv[:, :, pad : pad + kept] = np.swapaxes(-weight * np.sin(angle), 1, 2)
    index = np.arange(second_len)
    small = 2.0 * np.pi * ((index[:, None] * index[None, :]) % second_len) / second_len
    cos, sin = np.cos(small), np.sin(small)
    inner = np.block([[cos, sin], [-sin, cos]])
    outer = np.block([[cos, -sin], [sin, cos]])
    return tuple(jnp.asarray(t, jnp.bfloat16) for t in (fwd, inv, inner, outer))


def lane_roll(value, shift):
    shift = shift % LANES
    return value if shift == 0 else pltpu.roll(value, shift, 1)


def dot_as(left, right, dims):
    return lax.dot_general(
        left,
        right,
        ((dims[:1], dims[1:]), ((), ())),
        precision=highest,
        preferred_element_type=jnp.float32,
    )


def step_kernel(
    axis_n,
    batch_n,
    chan,
    scale,
    tok_hbm,
    og_hbm,
    inw_hbm,
    outw_hbm,
    embed_hbm,
    fwd_hbm,
    inv_hbm,
    inner_hbm,
    outer_hbm,
    embed_raw_hbm,
    embed_b_hbm,
    hidden_b_hbm,
    freqs_hbm,
    hidden_w_hbm,
    filter_w_hbm,
    decay_hbm,
    skip_hbm,
    gt_hbm,
    a_hbm,
    b_hbm,
    gt_out,
    out_sems,
    tok,
    og,
    inw,
    outw,
    embed,
    fwd,
    inv,
    inner,
    outer,
    embed_raw,
    embed_b,
    hidden_b,
    freqs,
    hidden_w,
    filter_w,
    decay_in,
    skip_in,
    load_sems,
    send_one,
    recv_one,
    send_two,
    recv_two,
    gates,
    x_buf,
    y_out,
    z_buf,
    v_buf,
    net,
    filt_pk,
    send_grad,
    grad_pk,
    modul,
    conv_buf,
    sems,
    net_sems,
    pk_out,
    extra,
    embed_w,
    vectors,
    *sum_scratch,
):
    n = axis_n
    me = lax.axis_index("seq")
    me_b = lax.axis_index("batch")
    pos, width = tok.shape
    rows = send_one.shape[1]
    fold = pos // rows
    step = 2 * chan
    second_len, double_pad, half = fwd.shape
    pad = double_pad // 2
    kept = half + 1
    f32, bf16 = jnp.float32, jnp.bfloat16

    barrier = pltpu.get_barrier_semaphore()
    everyone = n * batch_n
    own_at = me * batch_n + me_b
    for k in range(1, everyone):
        other = lax.rem(own_at + k, everyone)
        pl.semaphore_signal(
            barrier,
            inc=1,
            device_id={"seq": lax.div(other, batch_n), "batch": lax.rem(other, batch_n)},
            device_id_type=MESH,
        )

    quarter = embed.shape[1]
    own_part = pl.ds(pl.multiple_of(me_b * quarter, LANES), quarter)
    loads = [
        pltpu.make_async_copy(src, dst, load_sems.at[i])
        for i, (src, dst) in enumerate(
            (
                (tok_hbm, tok),
                (inw_hbm, inw),
                (og_hbm, og),
                (outw_hbm, outw),
                (embed_hbm.at[:, own_part], embed),
                (embed_raw_hbm, embed_raw),
                (embed_b_hbm, embed_b),
                (hidden_b_hbm, hidden_b),
                (freqs_hbm, freqs),
                (hidden_w_hbm, hidden_w),
                (filter_w_hbm, filter_w),
                (decay_hbm, decay_in),
                (skip_hbm, skip_in),
                (fwd_hbm, fwd),
                (inner_hbm, inner),
                (outer_hbm, outer),
                (inv_hbm, inv),
            )
        )
    ]
    for item in loads:
        item.start()
    for item in loads[:4]:
        item.wait()

    proj = jnp.dot(tok[...], inw[...], preferred_element_type=f32)
    gate_out = proj[:, :width].astype(bf16)
    gate_in = proj[:, width : 2 * width].astype(bf16)
    values = proj[:, 2 * width :].astype(bf16)
    gated_grad = lax.dot_general(
        og[...], outw[...], (((1,), (1,)), ((), ())), preferred_element_type=f32
    ).astype(bf16)
    gates[0] = gate_out
    gates[1] = gate_in
    gates[2] = values
    gates[3] = gated_grad
    mixed = (values.astype(f32) * gate_in.astype(f32)).astype(bf16).astype(f32)
    grad = (gated_grad.astype(f32) * gate_out.astype(f32)).astype(bf16).astype(f32)
    bias_sum = jnp.sum(mixed * grad, axis=0, keepdims=True) * scale

    lane = lax.broadcasted_iota(jnp.int32, (rows, LANES), 1)
    lane_full = lax.broadcasted_iota(jnp.int32, (pos, LANES), 1)
    for d in range(n):
        tile, off = (d * chan) // LANES * LANES, (d * chan) % LANES
        both = jnp.where(
            lane_full < chan,
            lane_roll(mixed[:, tile : tile + LANES], -off),
            lane_roll(grad[:, tile : tile + LANES], chan - off),
        )
        packed = both[:rows]
        for j in range(1, fold):
            packed = jnp.where(
                lane >= j * step, lane_roll(both[j * rows : (j + 1) * rows], j * step), packed
            )
        send_one[d] = packed.astype(bf16)

    pl.semaphore_wait(barrier, everyone - 1)

    def copy(send, recv, which, k):
        dest = lax.rem(me + k, n)
        return pltpu.make_async_remote_copy(
            src_ref=send.at[dest],
            dst_ref=recv.at[me],
            send_sem=sems.at[2 * which],
            recv_sem=sems.at[2 * which + 1],
            device_id={"seq": dest},
            device_id_type=MESH,
        )

    def wait_all(send, recv, which):
        others = pl.ds(0, n - 1)
        pltpu.make_async_remote_copy(
            src_ref=send.at[others],
            dst_ref=recv.at[others],
            send_sem=sems.at[2 * which],
            recv_sem=sems.at[2 * which + 1],
            device_id={"seq": me},
            device_id_type=MESH,
        ).wait()

    for k in range(1, n):
        copy(send_one, recv_one, 0, k).start()
    recv_one[me] = send_one[me]
    v_buf[...] = jnp.zeros_like(v_buf)
    extra[...] = jnp.zeros_like(extra)
    length = x_buf.shape[0]
    hid = hidden_w.shape[0]
    tiles = width // LANES

    def select_own(value, target):
        lane_v = lax.broadcasted_iota(jnp.int32, (value.shape[0], LANES), 1)
        got = jnp.zeros((value.shape[0], LANES), f32)
        for i in range(n):
            tile, off = (i * chan) // LANES * LANES, (i * chan) % LANES
            part = lane_roll(value[:, tile : tile + LANES], target - off)
            got = jnp.where(jnp.logical_and(me == i, lane_v >= 0), part, got)
        return jnp.where((lane_v >= target) & (lane_v < target + chan), got, 0.0)

    parts = LANES // chan
    sub = quarter // parts
    for item in loads[4:13]:
        item.wait()
    weight = select_own(filter_w[...], 0)
    decay_own = select_own(decay_in[...], 0)
    decay = decay_own
    for j in range(1, parts):
        decay = decay + lane_roll(decay_own, j * chan)
    skip = select_own(skip_in[...], 0) + select_own(skip_in[...], chan)
    inputs = embed_raw.shape[0]
    embed_w[...] = jnp.zeros_like(embed_w)
    embed_w[0:inputs, :] = embed_raw[...]
    embed_w[inputs : inputs + 1, :] = embed_b[...]
    vectors[...] = jnp.zeros_like(vectors)
    vectors[0:2, :] = freqs[...]
    vectors[2:3, :] = hidden_b[...]
    eye = (
        lax.broadcasted_iota(jnp.int32, (8, 8), 0) == lax.broadcasted_iota(jnp.int32, (8, 8), 1)
    ).astype(f32)
    columns = dot_as(vectors[...], eye, (0, 0))
    freq_one, freq_two = columns[:, 0:1], columns[:, 1:2]
    tile = min(256, quarter)
    def net_forward(i, _):
        at = pl.ds(pl.multiple_of(i * tile, LANES), tile)
        pre_one = dot_as(embed_w[...], embed[:, at], (0, 0))
        act_one, cos_one = sine_cosine(freq_one * pre_one)
        pre_two = dot_as(hidden_w[...], act_one, (0, 0)) + columns[:, 2:3]
        act_two, cos_two = sine_cosine(freq_two * pre_two)
        net[0, :, at] = pre_one
        net[1, :, at] = act_one
        net[2, :, at] = cos_one
        net[3, :, at] = pre_two
        net[4, :, at] = act_two
        net[5, :, at] = cos_two
        return 0

    lax.fori_loop(0, quarter // tile, net_forward, 0, unroll=2 if quarter // tile % 2 == 0 else 1)
    lane_s = lax.broadcasted_iota(jnp.int32, (sub, LANES), 1)
    time = lax.broadcasted_iota(jnp.int32, (sub, LANES), 0) + me_b * quarter
    for j in range(1, parts):
        time = time + jnp.where(lane_s >= j * chan, sub, 0)
    modul[...] = jnp.exp(-decay * time.astype(f32)) * (4.0 / math.sqrt(length))
    packed_filt = jnp.zeros((sub, LANES), f32)
    for j in range(parts):
        packed_filt = packed_filt + dot_as(
            net[4, :, j * sub : (j + 1) * sub], lane_roll(weight, j * chan), (0, 0)
        )
    filt_pk[me_b] = (packed_filt * modul[...]).astype(bf16)

    def share(which, k):
        dest = lax.rem(me_b + k, batch_n)
        return pltpu.make_async_remote_copy(
            src_ref=filt_pk.at[me_b] if which == 0 else send_grad.at[dest],
            dst_ref=filt_pk.at[me_b] if which == 0 else grad_pk.at[me_b],
            send_sem=net_sems.at[2 * which],
            recv_sem=net_sems.at[2 * which + 1],
            device_id={"batch": dest},
            device_id_type=MESH,
        )

    def share_wait(which):
        others = pl.ds(0, batch_n - 1)
        pltpu.make_async_remote_copy(
            src_ref=grad_pk.at[others],
            dst_ref=grad_pk.at[others],
            send_sem=net_sems.at[2 * which],
            recv_sem=net_sems.at[2 * which + 1],
            device_id={"batch": me_b},
            device_id_type=MESH,
        ).wait()

    for k in range(1, batch_n):
        share(0, k).start()
    wait_all(send_one, recv_one, 0)
    share_wait(0)

    for s in range(n):
        block = recv_one[s].astype(f32)
        for j in range(fold):
            start = s * pos + j * rows
            q, rest = start // quarter, start % quarter
            p, row = rest // sub, rest % sub
            filt = lane_roll(filt_pk[q, row : row + rows, :].astype(f32), step - p * chan)
            x_buf[pl.ds(start, rows), :] = jnp.where(
                lane < step, lane_roll(block, -j * step), filt
            )
    for item in loads[13:]:
        item.wait()

    def stage_one(n2, _):
        part = x_buf[pl.ds(n2, half, stride=second_len), :].astype(bf16)
        z_buf[pl.ds(pl.multiple_of(n2 * double_pad, 8), double_pad), :] = jnp.dot(
            fwd[n2], part, preferred_element_type=f32
        )
        return 0

    lax.fori_loop(0, second_len, stage_one, 0, unroll=16)

    lane_k = lax.broadcasted_iota(jnp.int32, (second_len, LANES), 1)
    low = lane_k < step
    mid = (lane_k >= chan) & (lane_k < step)
    sign = jnp.where((lane_k >= chan), -1.0, 1.0).astype(f32)

    def stage_two(k1, _):
        stacked = jnp.concatenate(
            [
                z_buf[pl.ds(k1, second_len, stride=double_pad), :],
                z_buf[pl.ds(pad + k1, second_len, stride=double_pad), :],
            ],
            axis=0,
        ).astype(bf16)
        spec = jnp.dot(inner[...], stacked, preferred_element_type=f32)
        re, im = spec[:second_len], spec[second_len:]
        left_re = jnp.where(low, re, lane_roll(re, chan))
        left_im = jnp.where(low, im, lane_roll(im, chan))
        right_re = jnp.where(mid, lane_roll(re, -chan), lane_roll(re, -step))
        right_im = jnp.where(mid, lane_roll(im, -chan), lane_roll(im, -step)) * sign
        corr_re = jnp.where(lane_k < step, right_re, lane_roll(re, step))
        corr_im = jnp.where(lane_k < step, right_im, lane_roll(im, step) * sign)
        out = jnp.concatenate(
            [
                left_re * corr_re - left_im * corr_im,
                left_re * corr_im + left_im * corr_re,
            ],
            axis=0,
        ).astype(bf16)
        back = jnp.dot(outer[...], out, preferred_element_type=f32)
        v_buf[pl.ds(k1, second_len, stride=double_pad), :] = back[:second_len]
        v_buf[pl.ds(pad + k1, second_len, stride=double_pad), :] = back[second_len:]
        return 0

    unroll = 11 if kept % 11 == 0 else 3 if kept % 3 == 0 else 5 if kept % 5 == 0 else 1
    lax.fori_loop(0, kept, stage_two, 0, unroll=unroll)

    def stage_three(n2, _):
        part = v_buf[pl.ds(pl.multiple_of(n2 * double_pad, 8), double_pad), :].astype(bf16)
        at = pl.ds(n2, half, stride=second_len)
        y_out[at, :] = (
            jnp.dot(inv[n2], part, preferred_element_type=f32) + skip * x_buf[at, :]
        )
        return 0

    lax.fori_loop(0, second_len, stage_three, 0, unroll=16)

    for d in range(n):
        packed = y_out[pl.ds(d * pos, rows), :]
        for j in range(1, fold):
            packed = jnp.where(
                lane >= j * step,
                lane_roll(y_out[pl.ds(d * pos + j * rows, rows), :], j * step),
                packed,
            )
        send_two[d] = packed.astype(bf16)
    for k in range(1, n):
        copy(send_two, recv_two, 1, k).start()
    recv_two[me] = send_two[me]

    owned = [(lane_s >= j * chan) & (lane_s < (j + 1) * chan) for j in range(parts)]
    for q in range(batch_n):
        packed = jnp.zeros((sub, LANES), f32)
        for j in range(parts):
            part = y_out[pl.ds(q * quarter + j * sub, sub), :]
            packed = jnp.where(owned[j], lane_roll(part, j * chan - step), packed)
        send_grad[q] = packed.astype(bf16)
    for k in range(1, batch_n):
        share(1, k).start()
    grad_pk[me_b] = send_grad[me_b]
    share_wait(1)
    total = grad_pk[0].astype(f32)
    for q in range(1, batch_n):
        total = total + grad_pk[q].astype(f32)
    grad_kernel = total * modul[...]

    em = embed.shape[0]
    lane_w = lax.broadcasted_iota(jnp.int32, (hid, LANES), 1)
    grad_weight = jnp.zeros((hid, LANES), f32)
    for j in range(parts):
        at = slice(j * sub, (j + 1) * sub)
        got = dot_as(net[4, :, at], grad_kernel, (1, 0))
        grad_weight = grad_weight + lane_roll(
            jnp.where((lane_w >= j * chan) & (lane_w < (j + 1) * chan), got, 0.0), -j * chan
        )
        net[5, :, at] = dot_as(lane_roll(weight, j * chan), grad_kernel, (1, 1)) * net[5, :, at]

    def net_backward(i, carry):
        at = pl.ds(pl.multiple_of(i * tile, LANES), tile)
        grad_act_two = net[5, :, at]
        grad_pre_two = grad_act_two * freq_two
        grad_hidden = dot_as(net[1, :, at], grad_pre_two, (1, 1))
        grad_act_one = dot_as(hidden_w[...], grad_pre_two, (1, 0)) * net[2, :, at]
        grad_pre_one = grad_act_one * freq_one
        stacked = jnp.concatenate(
            [grad_pre_one, grad_pre_two, grad_act_one * net[0, :, at], grad_act_two * net[3, :, at]],
            axis=0,
        )
        return carry[0] + grad_hidden, carry[1] + dot_as(embed[:, at], stacked, (1, 1))

    zeros = lambda r, c: jnp.zeros((r, c), f32)
    both_sums = lax.fori_loop(
        0,
        quarter // tile,
        net_backward,
        (zeros(hid, hid), zeros(em, 4 * hid)),
        unroll=2 if quarter // tile % 2 == 0 else 1,
    )
    sums = (grad_weight, both_sums[0]) + tuple(
        both_sums[1][:, i * hid : (i + 1) * hid] for i in range(4)
    )
    sums = tuple(term * (scale * 0.25) for term in sums)
    lane_h = lax.broadcasted_iota(jnp.int32, (hid, LANES), 1)
    for tile in range(tiles):
        placed = zeros(hid, LANES)
        for i in range(n):
            if (i * chan) // LANES == tile:
                off = (i * chan) % LANES
                mask = (lane_h >= off) & (lane_h < off + chan) & (me == i)
                placed = jnp.where(mask, lane_roll(sums[0], off), placed)
        extra[tile * hid : (tile + 1) * hid, :] = placed
    base = tiles * hid
    extra[base : base + hid, 0:hid] = sums[1]
    base += hid
    for term in sums[2:]:
        extra[base : base + em, 0:hid] = term
        base += em
    for tile in range(tiles):
        extra[base + tile : base + tile + 1, :] = bias_sum[:, tile * LANES : (tile + 1) * LANES]

    main_scratch, extra_scratch = sum_scratch[:5], sum_scratch[5:]
    blocks = main_scratch[1].shape[0]
    stream = [pair_sum(n, batch_n, pk_out, main_scratch, b) for b in range(blocks)]
    extra_sum = pair_sum(n, batch_n, extra, extra_scratch, 0)
    extra_sum.start_pair()
    wait_all(send_two, recv_two, 1)

    per_tile = LANES // chan
    for tile in range(width // LANES):
        for j in range(fold):
            conv_acc = jnp.zeros((rows, LANES), f32)
            grad_acc = jnp.zeros((rows, LANES), f32)
            for i in range(per_tile):
                block = recv_two[tile * per_tile + i].astype(f32)
                own = (lane >= i * chan) & (lane < (i + 1) * chan)
                conv_acc = jnp.where(own, lane_roll(block, i * chan - j * step), conv_acc)
                grad_acc = jnp.where(own, lane_roll(block, i * chan - j * step - chan), grad_acc)
            at = pl.ds(j * rows, rows)
            conv_buf[0, at, tile * LANES : (tile + 1) * LANES] = conv_acc
            conv_buf[1, at, tile * LANES : (tile + 1) * LANES] = grad_acc

    conv = conv_buf[0]
    grad_mixed = conv_buf[1]
    gated = (gates[0].astype(f32) * conv).astype(bf16)
    grad_proj = jnp.concatenate(
        [
            (gates[3].astype(f32) * conv).astype(bf16),
            (grad_mixed * gates[2].astype(f32)).astype(bf16),
            (grad_mixed * gates[1].astype(f32)).astype(bf16),
        ],
        axis=1,
    )
    first = (((0,), (0,)), ((), ()))
    pieces = [(gated, og[...])] + [
        (tok[...], grad_proj[:, j * width : (j + 1) * width]) for j in range(3)
    ]
    per_block = len(pieces) // blocks if blocks > 1 else len(pieces)
    for i, (left, right) in enumerate(pieces):
        block = lax.dot_general(left, right, first, preferred_element_type=f32) * scale
        for j in range(tiles):
            at = (i * tiles + j) * width
            pk_out[at : at + width, :] = block[:, j * LANES : (j + 1) * LANES].astype(bf16)
        if (i + 1) % per_block == 0:
            done = (i + 1) // per_block - 1
            stream[done].start_pair()
            if done == 0:
                extra_sum.finish_pair()
                extra_sum.start_scatter()
            else:
                stream[done - 1].finish_pair()
                stream[done - 1].start_scatter()
    gt_out[...] = lax.dot_general(
        grad_proj, inw[...], (((1,), (1,)), ((), ())), preferred_element_type=f32
    ).astype(bf16)
    stream[-1].finish_pair()
    stream[-1].start_scatter()
    outs = [pltpu.make_async_copy(gt_out, gt_hbm, out_sems.at[0])]
    outs[0].start()
    every = [extra_sum] + stream
    for item in every:
        item.finish_scatter()
        item.start_gather()
    for item in every:
        item.finish_gather()
        item.start_swap()
    for i, item in enumerate(every):
        item.finish_swap()
        if i == 0:
            target = b_hbm
        else:
            target = a_hbm.at[pl.ds((i - 1) * item.size, item.size), :]
        outs.append(pltpu.make_async_copy(item.whole, target, out_sems.at[1 + i]))
        outs[-1].start()
    for item in outs:
        item.wait()


class pair_sum:
    def __init__(self, ns, nb, src, scratch, block):
        got_pair, part, got, whole, sems = (ref.at[block] for ref in scratch)
        self.got_pair, self.part, self.got, self.whole, self.sems = got_pair, part, got, whole, sems
        self.src, self.pairs = src, nb // 2
        me_s, me_b = lax.axis_index("seq"), lax.axis_index("batch")
        self.core = lax.rem(me_b, 2)
        self.chips = ns * self.pairs
        self.own = me_s * self.pairs + lax.div(me_b, 2)
        self.partner = me_b + 1 - 2 * self.core
        self.half = part.shape[0]
        self.size = 2 * self.half
        self.base = block * self.size
        self.unit = self.half // self.chips

    def rows(self, start, size):
        return pl.ds(pl.multiple_of(start, self.unit), size)

    def to_partner(self, which):
        if which == 0:
            src = self.src.at[self.rows(self.base + (1 - self.core) * self.half, self.half)]
            dst = self.got_pair
        else:
            src = dst = self.whole.at[self.rows(self.core * self.half, self.half)]
        return pltpu.make_async_remote_copy(
            src_ref=src,
            dst_ref=dst,
            send_sem=self.sems.at[which, 0, 0],
            recv_sem=self.sems.at[which, 1, 0],
            device_id={"batch": self.partner},
            device_id_type=MESH,
        )

    def to_chips(self, which):
        made = []
        for k in range(1, self.chips):
            dest = lax.rem(self.own + k, self.chips)
            if which == 0:
                src = self.part.at[self.rows(dest * self.unit, self.unit)]
                dst = self.got.at[k - 1]
            else:
                at = self.rows(self.core * self.half + self.own * self.unit, self.unit)
                src = dst = self.whole.at[at]
            made.append(
                pltpu.make_async_remote_copy(
                    src_ref=src,
                    dst_ref=dst,
                    send_sem=self.sems.at[which, 0, 1],
                    recv_sem=self.sems.at[which, 1, 1],
                    device_id={
                        "seq": lax.div(dest, self.pairs),
                        "batch": 2 * lax.rem(dest, self.pairs) + self.core,
                    },
                    device_id_type=MESH,
                )
            )
        return made

    def wait_chips(self, which):
        pltpu.make_async_remote_copy(
            src_ref=self.got,
            dst_ref=self.got,
            send_sem=self.sems.at[which, 0, 1],
            recv_sem=self.sems.at[which, 1, 1],
            device_id={"batch": self.partner},
            device_id_type=MESH,
        ).wait()

    def start_pair(self):
        self.to_partner(0).start()

    def finish_pair(self):
        self.to_partner(0).wait()
        mine = self.src[self.rows(self.base + self.core * self.half, self.half), :]
        total = mine.astype(jnp.float32) + self.got_pair[...].astype(jnp.float32)
        self.part[...] = total.astype(self.part.dtype)

    def start_scatter(self):
        for item in self.to_chips(0):
            item.start()

    def finish_scatter(self):
        self.wait_chips(0)
        total = self.part[self.rows(self.own * self.unit, self.unit), :].astype(jnp.float32)
        for k in range(1, self.chips):
            total = total + self.got[k - 1].astype(jnp.float32)
        at = self.rows(self.core * self.half + self.own * self.unit, self.unit)
        self.whole[at, :] = total.astype(self.whole.dtype)

    def start_gather(self):
        for item in self.to_chips(1):
            item.start()

    def finish_gather(self):
        self.wait_chips(1)

    def start_swap(self):
        self.to_partner(1).start()

    def finish_swap(self):
        self.to_partner(1).wait()


def unpack_kernel(main, extra, tokens_in, tokens_out, g_in, g_out, skip, emb, emb_b, hidden, hidden_b, filt, freq):
    width = g_out.shape[0]
    hid = hidden.shape[0]
    tokens_out[...] = tokens_in[...]
    at = 0
    for ref in (g_out, g_in):
        for j in range(ref.shape[1] // LANES):
            ref[:, j * LANES : (j + 1) * LANES] = main[at : at + width, :].astype(jnp.float32)
            at += width
    tiles = width // LANES
    for j in range(tiles):
        filt[:, j * LANES : (j + 1) * LANES] = extra[j * hid : (j + 1) * hid, :]
    base = tiles * hid
    hidden[...] = extra[base : base + hid, 0:hid]
    base += hid
    count = emb.shape[0]
    em = -(-(count + 1) // 8) * 8
    emb[...] = extra[base : base + count, 0:hid]
    emb_b[...] = extra[base + count : base + count + 1, 0:hid]
    hidden_b[...] = extra[base + em + count : base + em + count + 1, 0:hid]
    freq[0:1, :] = extra[base + 2 * em + count : base + 2 * em + count + 1, 0:hid]
    freq[1:2, :] = extra[base + 3 * em + count : base + 3 * em + count + 1, 0:hid]
    base += 4 * em
    for j in range(tiles):
        skip[:, j * LANES : (j + 1) * LANES] = extra[base + j : base + j + 1, :]


def vmem(count):
    return [pl.BlockSpec(memory_space=pltpu.VMEM)] * count


def sine_cosine(angle):
    turns = jnp.round(angle * (1.0 / (2.0 * math.pi)))
    reduced = angle - turns * 6.28125
    reduced = reduced - turns * 0.0019350051879882812
    reduced = reduced - turns * 3.0199157663146e-07
    half = reduced * 0.5
    square = half * half
    sin = half * (
        1.0
        + square
        * (-1.0 / 6 + square * (1.0 / 120 + square * (-1.0 / 5040 + square * (1.0 / 362880 - square / 39916800.0))))
    )
    cos = 1.0 + square * (
        -0.5
        + square
        * (1.0 / 24 + square * (-1.0 / 720 + square * (1.0 / 40320 + square * (-1.0 / 3628800 + square / 479001600.0))))
    )
    return 2.0 * sin * cos, 1.0 - 2.0 * sin * sin


def embedding(length, count):
    rows = np.zeros((-(-(count + 1) // 8) * 8, length), np.float32)
    scaled = np.arange(length) / length
    rows[0] = scaled
    for band_index in range(1, (count - 1) // 2 + 1):
        rows[2 * band_index - 1] = np.cos(2.0 * np.pi * band_index * scaled)
        rows[2 * band_index] = np.sin(2.0 * np.pi * band_index * scaled)
    rows[count] = 1.0
    return jnp.asarray(rows)


def shards(
    tokens,
    out_grad,
    in_weight,
    out_weight,
    skip_bias,
    embed_weight,
    embed_bias,
    hidden_weight,
    hidden_bias,
    filter_weight,
    sine_freq,
    decay_rate,
):
    f32, bf16 = jnp.float32, jnp.bfloat16
    tok, og = tokens[0], out_grad[0]
    pos, width = tok.shape
    ns, nb = lax.axis_size("seq"), lax.axis_size("batch")
    length = pos * ns
    chan = width // ns
    hid = hidden_weight.shape[0]
    count = embed_weight.shape[0]
    embed = embedding(length, count)
    em = embed.shape[0]

    fwd, inv, inner, outer = make_tables(length)
    second_len, double_pad, half = fwd.shape
    rows = pos // (LANES // (2 * chan))
    tiles = width // LANES
    chips = ns * (nb // 2)
    unit = 2 * chips * 16
    main_rows = -(-4 * width * tiles // unit) * unit
    blocks = max(b for b in (1, 2, 4) if main_rows % (b * unit) == 0)
    unit = 2 * chips * 8
    extra_rows = -(-(tiles * hid + hid + 4 * em + tiles) // unit) * unit
    pair = (ns, rows, LANES)
    shared = (nb, length // nb // (LANES // chan), LANES)
    spectral = (second_len * double_pad, LANES)
    scratch = []
    for total, kind, count_at in ((main_rows, bf16, blocks), (extra_rows, f32, 1)):
        half_rows = total // count_at // 2
        scratch += [
            pltpu.VMEM((count_at, half_rows, LANES), kind),
            pltpu.VMEM((count_at, half_rows, LANES), kind),
            pltpu.VMEM((count_at, chips - 1, half_rows // chips, LANES), kind),
            pltpu.VMEM((count_at, 2 * half_rows, LANES), kind),
            pltpu.SemaphoreType.DMA((count_at, 2, 2, 2)),
        ]
    grad_tokens, main, extra = pl.pallas_call(
        functools.partial(step_kernel, ns, nb, chan, 1.0 / math.sqrt(nb * length)),
        out_shape=(
            jax.ShapeDtypeStruct((pos, width), bf16),
            jax.ShapeDtypeStruct((main_rows, LANES), bf16),
            jax.ShapeDtypeStruct((extra_rows, LANES), f32),
        ),
        in_specs=[pl.BlockSpec(memory_space=pl.ANY)] * 17,
        out_specs=(pl.BlockSpec(memory_space=pl.ANY),) * 3,
        scratch_shapes=[
            pltpu.VMEM((pos, width), bf16),
            pltpu.SemaphoreType.DMA((2 + blocks,)),
            pltpu.VMEM(tok.shape, bf16),
            pltpu.VMEM(og.shape, bf16),
            pltpu.VMEM(in_weight.shape, bf16),
            pltpu.VMEM(out_weight.shape, bf16),
            pltpu.VMEM((em, length // nb), f32),
            pltpu.VMEM(fwd.shape, bf16),
            pltpu.VMEM(inv.shape, bf16),
            pltpu.VMEM(inner.shape, bf16),
            pltpu.VMEM(outer.shape, bf16),
            pltpu.VMEM(embed_weight.shape, f32),
            pltpu.VMEM((1, hid), f32),
            pltpu.VMEM((1, hid), f32),
            pltpu.VMEM(sine_freq.shape, f32),
            pltpu.VMEM(hidden_weight.shape, f32),
            pltpu.VMEM(filter_weight.shape, f32),
            pltpu.VMEM((1, width), f32),
            pltpu.VMEM((1, width), f32),
            pltpu.SemaphoreType.DMA((17,)),
            pltpu.VMEM(pair, bf16),
            pltpu.VMEM(pair, bf16),
            pltpu.VMEM(pair, bf16),
            pltpu.VMEM(pair, bf16),
            pltpu.VMEM((4, pos, width), bf16),
            pltpu.VMEM((length, LANES), f32),
            pltpu.VMEM((length, LANES), f32),
            pltpu.VMEM(spectral, f32),
            pltpu.VMEM(spectral, f32),
            pltpu.VMEM((6, hid, length // nb), f32),
            pltpu.VMEM(shared, bf16),
            pltpu.VMEM(shared, bf16),
            pltpu.VMEM(shared, bf16),
            pltpu.VMEM(shared[1:], f32),
            pltpu.VMEM((2, pos, width), f32),
            pltpu.SemaphoreType.DMA((4,)),
            pltpu.SemaphoreType.DMA((4,)),
            pltpu.VMEM((main_rows, LANES), bf16),
            pltpu.VMEM((extra_rows, LANES), f32),
            pltpu.VMEM((em, hid), f32),
            pltpu.VMEM((8, hid), f32),
        ]
        + scratch,
        compiler_params=pltpu.CompilerParams(
            collective_id=0, has_side_effects=True, vmem_limit_bytes=VMEM_BYTES
        ),
        name="step",
    )(
        tok,
        og,
        in_weight,
        out_weight,
        embed,
        fwd,
        inv,
        inner,
        outer,
        embed_weight,
        embed_bias[None],
        hidden_bias[None],
        sine_freq,
        hidden_weight,
        filter_weight,
        decay_rate[None],
        skip_bias[None],
    )

    shapes = (
        (width, 3 * width),
        (width, width),
        (1, width),
        (count, hid),
        (1, hid),
        (hid, hid),
        (1, hid),
        (hid, width),
        (2, hid),
    )
    out = pl.pallas_call(
        unpack_kernel,
        out_shape=(jax.ShapeDtypeStruct((pos, width), bf16),)
        + tuple(jax.ShapeDtypeStruct(shape, f32) for shape in shapes),
        in_specs=vmem(3),
        out_specs=tuple(vmem(1 + len(shapes))),
        name="unpack",
    )(main, extra, grad_tokens)
    return (
        out[0][None],
        out[1],
        out[2],
        out[3][0],
        out[4],
        out[5][0],
        out[6],
        out[7][0],
        out[8],
        out[9],
    )


def solution(mesh):
    batched = P("batch", "seq", None)
    return jax.shard_map(
        shards,
        mesh=mesh,
        in_specs=(batched, batched) + (P(),) * 10,
        out_specs=(batched,) + (P(),) * 9,
        check_vma=False,
    )
```

```python
import functools
import math

import jax
import jax.numpy as jnp
import numpy as np
from jax import lax
from jax.experimental import pallas as pl
from jax.experimental.pallas import tpu as pltpu
from jax.sharding import PartitionSpec as P

highest = lax.Precision.HIGHEST
MESH = pl.DeviceIdType.MESH
LANES = 128
VMEM_BYTES = 66 * 1000 * 1000


def factor(length):
    total = 2 * length
    first_len = 2
    while first_len * first_len < total and total % (2 * first_len) == 0:
        first_len = first_len * 2
    return first_len, total // first_len


def make_tables(length):
    total = 2 * length
    first_len, second_len = factor(length)
    half = first_len // 2
    kept = half + 1
    pad = -(-kept // 8) * 8
    k1 = np.arange(kept)[None, :, None]
    n1 = np.arange(half)[None, None, :]
    n2 = np.arange(second_len)[:, None, None]
    angle = 2.0 * np.pi * ((k1 * (n1 * second_len + n2)) % total) / total
    fwd = np.zeros((second_len, 2 * pad, half), np.float32)
    fwd[:, :kept] = np.cos(angle)
    fwd[:, pad : pad + kept] = -np.sin(angle)
    weight = np.where((k1 == 0) | (k1 == half), 1.0, 2.0) / total
    inv = np.zeros((second_len, half, 2 * pad), np.float32)
    inv[:, :, :kept] = np.swapaxes(weight * np.cos(angle), 1, 2)
    inv[:, :, pad : pad + kept] = np.swapaxes(-weight * np.sin(angle), 1, 2)
    index = np.arange(second_len)
    small = 2.0 * np.pi * ((index[:, None] * index[None, :]) % second_len) / second_len
    cos, sin = np.cos(small), np.sin(small)
    inner = np.block([[cos, sin], [-sin, cos]])
    outer = np.block([[cos, -sin], [sin, cos]])
    return tuple(jnp.asarray(t, jnp.bfloat16) for t in (fwd, inv, inner, outer))


def selections(chan, dense):
    parts = LANES // chan
    fold = parts // 2
    if not dense:
        return tuple(jnp.zeros(s, jnp.bfloat16) for s in ((16, LANES), (1, 16, LANES), (16, LANES)))
    swap = np.zeros((parts * LANES, parts * LANES), np.float32)
    place = np.zeros((parts, 2 * LANES, LANES), np.float32)
    gather = np.zeros((parts * LANES, 3 * LANES), np.float32)
    c = np.arange(chan)
    for i in range(parts):
        for u in range(parts):
            swap[u * LANES + i * chan + c, i * LANES + u * chan + c] = 1.0
    for p in range(parts):
        e, j = p // fold, p % fold
        place[p, j * chan + c, c] = 1.0
        place[p, j * chan + c, 3 * chan + c] = 1.0
        place[p, (fold + j) * chan + c, 2 * chan + c] = 1.0
        place[p, LANES + p * chan + c, chan + c] = 1.0
        gather[p * LANES + chan + c, e * LANES + j * chan + c] = 1.0
        gather[p * LANES + 2 * chan + c, e * LANES + (fold + j) * chan + c] = 1.0
        gather[p * LANES + 3 * chan + c, 2 * LANES + p * chan + c] = 1.0
    return tuple(jnp.asarray(t, jnp.bfloat16) for t in (swap, place, gather))


def lane_roll(value, shift):
    shift = shift % LANES
    return value if shift == 0 else pltpu.roll(value, shift, 1)


def dot_as(left, right, dims):
    return lax.dot_general(
        left,
        right,
        ((dims[:1], dims[1:]), ((), ())),
        precision=highest,
        preferred_element_type=jnp.float32,
    )


def step_kernel(
    axis_n,
    batch_n,
    chan,
    scale,
    tok_hbm,
    og_hbm,
    inw_hbm,
    outw_hbm,
    embed_hbm,
    fwd_hbm,
    inv_hbm,
    inner_hbm,
    outer_hbm,
    embed_raw_hbm,
    embed_b_hbm,
    hidden_b_hbm,
    freqs_hbm,
    hidden_w_hbm,
    filter_w_hbm,
    decay_hbm,
    skip_hbm,
    swap_hbm,
    place_hbm,
    gather_hbm,
    gt_hbm,
    a_hbm,
    b_hbm,
    gt_out,
    out_sems,
    tok,
    og,
    inw,
    outw,
    embed,
    fwd,
    inv,
    inner,
    outer,
    embed_raw,
    embed_b,
    hidden_b,
    freqs,
    hidden_w,
    filter_w,
    decay_in,
    skip_in,
    swap,
    place,
    gather,
    load_sems,
    send_one,
    recv_one,
    send_two,
    recv_two,
    gates,
    x_buf,
    y_out,
    z_buf,
    v_buf,
    net,
    filt_pk,
    send_grad,
    grad_pk,
    modul,
    conv_buf,
    sems,
    net_sems,
    pk_out,
    extra,
    embed_w,
    vectors,
    *sum_scratch,
):
    n = axis_n
    me = lax.axis_index("seq")
    me_b = lax.axis_index("batch")
    pos, width = tok.shape
    rows = send_one.shape[1]
    fold = pos // rows
    step = 2 * chan
    second_len, double_pad, half = fwd.shape
    pad = double_pad // 2
    kept = half + 1
    f32, bf16 = jnp.float32, jnp.bfloat16

    barrier = pltpu.get_barrier_semaphore()
    everyone = n * batch_n
    own_at = me * batch_n + me_b
    for k in range(1, everyone):
        other = lax.rem(own_at + k, everyone)
        pl.semaphore_signal(
            barrier,
            inc=1,
            device_id={"seq": lax.div(other, batch_n), "batch": lax.rem(other, batch_n)},
            device_id_type=MESH,
        )

    quarter = embed.shape[1]
    own_part = pl.ds(pl.multiple_of(me_b * quarter, LANES), quarter)
    loads = [
        pltpu.make_async_copy(src, dst, load_sems.at[i])
        for i, (src, dst) in enumerate(
            (
                (tok_hbm, tok),
                (inw_hbm, inw),
                (og_hbm, og),
                (outw_hbm, outw),
                (swap_hbm, swap),
                (embed_hbm.at[:, own_part], embed),
                (embed_raw_hbm, embed_raw),
                (embed_b_hbm, embed_b),
                (hidden_b_hbm, hidden_b),
                (freqs_hbm, freqs),
                (hidden_w_hbm, hidden_w),
                (filter_w_hbm, filter_w),
                (decay_hbm, decay_in),
                (skip_hbm, skip_in),
                (place_hbm, place),
                (fwd_hbm, fwd),
                (inner_hbm, inner),
                (outer_hbm, outer),
                (inv_hbm, inv),
                (gather_hbm, gather),
            )
        )
    ]
    for item in loads:
        item.start()
    for item in loads[:4]:
        item.wait()

    proj = jnp.dot(tok[...], inw[...], preferred_element_type=f32)
    gate_out = proj[:, :width].astype(bf16)
    gate_in = proj[:, width : 2 * width].astype(bf16)
    values = proj[:, 2 * width :].astype(bf16)
    gated_grad = lax.dot_general(
        og[...], outw[...], (((1,), (1,)), ((), ())), preferred_element_type=f32
    ).astype(bf16)
    gates[0] = gate_out
    gates[1] = gate_in
    gates[2] = values
    gates[3] = gated_grad
    mixed = (values.astype(f32) * gate_in.astype(f32)).astype(bf16).astype(f32)
    grad = (gated_grad.astype(f32) * gate_out.astype(f32)).astype(bf16).astype(f32)
    bias_sum = jnp.sum(mixed * grad, axis=0, keepdims=True) * scale

    lane = lax.broadcasted_iota(jnp.int32, (rows, LANES), 1)
    half_lanes = fold * chan
    parts = LANES // chan
    tiles = width // LANES
    dense = swap.shape[0] == parts * LANES
    loads[4].wait()
    if dense:
        for t in range(tiles):
            at = slice(t * LANES, (t + 1) * LANES)
            left = jnp.concatenate(
                [
                    source[j * rows : (j + 1) * rows, at].astype(bf16)
                    for source in (mixed, grad)
                    for j in range(fold)
                ],
                axis=1,
            )
            packed = jnp.dot(left, swap[...], preferred_element_type=f32).astype(bf16)
            for i in range(parts):
                send_one[t * parts + i] = packed[:, i * LANES : (i + 1) * LANES]
    for d in range(0 if dense else n):
        tile, off = (d * chan) // LANES * LANES, (d * chan) % LANES
        packed = None
        for i in range(2 * fold):
            source, j = (mixed, i) if i < fold else (grad, i - fold)
            part = lane_roll(source[j * rows : (j + 1) * rows, tile : tile + LANES], i * chan - off)
            packed = part if packed is None else jnp.where(lane >= i * chan, part, packed)
        send_one[d] = packed.astype(bf16)

    pl.semaphore_wait(barrier, everyone - 1)

    def copy(send, recv, which, k):
        dest = lax.rem(me + k, n)
        return pltpu.make_async_remote_copy(
            src_ref=send.at[dest],
            dst_ref=recv.at[me],
            send_sem=sems.at[2 * which],
            recv_sem=sems.at[2 * which + 1],
            device_id={"seq": dest},
            device_id_type=MESH,
        )

    def wait_all(send, recv, which):
        others = pl.ds(0, n - 1)
        pltpu.make_async_remote_copy(
            src_ref=send.at[others],
            dst_ref=recv.at[others],
            send_sem=sems.at[2 * which],
            recv_sem=sems.at[2 * which + 1],
            device_id={"seq": me},
            device_id_type=MESH,
        ).wait()

    for k in range(1, n):
        copy(send_one, recv_one, 0, k).start()
    recv_one[me] = send_one[me]
    v_buf[...] = jnp.zeros_like(v_buf)
    extra[...] = jnp.zeros_like(extra)
    length = n * pos
    group = second_len + 1
    stride = double_pad + 1
    hid = hidden_w.shape[0]

    def select_own(value, target):
        lane_v = lax.broadcasted_iota(jnp.int32, (value.shape[0], LANES), 1)
        got = jnp.zeros((value.shape[0], LANES), f32)
        for i in range(n):
            tile, off = (i * chan) // LANES * LANES, (i * chan) % LANES
            part = lane_roll(value[:, tile : tile + LANES], target - off)
            got = jnp.where(jnp.logical_and(me == i, lane_v >= 0), part, got)
        return jnp.where((lane_v >= target) & (lane_v < target + chan), got, 0.0)

    sub = quarter // parts
    for item in loads[5:15]:
        item.wait()
    weight = select_own(filter_w[...], 0)
    decay_own = select_own(decay_in[...], 0)
    decay = decay_own
    for j in range(1, parts):
        decay = decay + lane_roll(decay_own, j * chan)
    skip_own = select_own(skip_in[...], chan)
    skip_other = select_own(skip_in[...], step)
    inputs = embed_raw.shape[0]
    embed_w[...] = jnp.zeros_like(embed_w)
    embed_w[0:inputs, :] = embed_raw[...]
    embed_w[inputs : inputs + 1, :] = embed_b[...]
    vectors[...] = jnp.zeros_like(vectors)
    vectors[0:2, :] = freqs[...]
    vectors[2:3, :] = hidden_b[...]
    eye = (
        lax.broadcasted_iota(jnp.int32, (8, 8), 0) == lax.broadcasted_iota(jnp.int32, (8, 8), 1)
    ).astype(f32)
    columns = dot_as(vectors[...], eye, (0, 0))
    freq_one, freq_two = columns[:, 0:1], columns[:, 1:2]
    tile = min(256, quarter)
    def net_forward(i, _):
        at = pl.ds(pl.multiple_of(i * tile, LANES), tile)
        pre_one = dot_as(embed_w[...], embed[:, at], (0, 0))
        act_one, cos_one = sine_cosine(freq_one * pre_one)
        pre_two = dot_as(hidden_w[...], act_one, (0, 0)) + columns[:, 2:3]
        act_two, cos_two = sine_cosine(freq_two * pre_two)
        net[0, :, at] = pre_one
        net[1, :, at] = act_one
        net[2, :, at] = cos_one
        net[3, :, at] = pre_two
        net[4, :, at] = act_two
        net[5, :, at] = cos_two
        return 0

    lax.fori_loop(0, quarter // tile, net_forward, 0, unroll=2 if quarter // tile % 2 == 0 else 1)
    lane_s = lax.broadcasted_iota(jnp.int32, (sub, LANES), 1)
    time = lax.broadcasted_iota(jnp.int32, (sub, LANES), 0) + me_b * quarter
    for j in range(1, parts):
        time = time + jnp.where(lane_s >= j * chan, sub, 0)
    modul[...] = jnp.exp(-decay * time.astype(f32)) * (4.0 / math.sqrt(length))
    packed_filt = jnp.zeros((sub, LANES), f32)
    for j in range(parts):
        packed_filt = packed_filt + dot_as(
            net[4, :, j * sub : (j + 1) * sub], lane_roll(weight, j * chan), (0, 0)
        )
    filt_pk[me_b] = (packed_filt * modul[...]).astype(bf16)

    def share(which, k):
        dest = lax.rem(me_b + k, batch_n)
        return pltpu.make_async_remote_copy(
            src_ref=filt_pk.at[me_b] if which == 0 else send_grad.at[dest],
            dst_ref=filt_pk.at[me_b] if which == 0 else grad_pk.at[me_b],
            send_sem=net_sems.at[2 * which],
            recv_sem=net_sems.at[2 * which + 1],
            device_id={"batch": dest},
            device_id_type=MESH,
        )

    def share_wait(which):
        others = pl.ds(0, batch_n - 1)
        pltpu.make_async_remote_copy(
            src_ref=grad_pk.at[others],
            dst_ref=grad_pk.at[others],
            send_sem=net_sems.at[2 * which],
            recv_sem=net_sems.at[2 * which + 1],
            device_id={"batch": me_b},
            device_id_type=MESH,
        ).wait()

    for k in range(1, batch_n):
        share(0, k).start()
    wait_all(send_one, recv_one, 0)
    share_wait(0)

    piece = min(rows, second_len)
    lane_p = lax.broadcasted_iota(jnp.int32, (piece, LANES), 1)

    def row_of(position):
        return position // second_len * group + position % second_len

    for block in range(n * fold if dense else 0):
        q, p = block // parts, block % parts
        both = jnp.concatenate([recv_one[block // fold], filt_pk[q]], axis=1)
        placed = jnp.dot(both, place[p], preferred_element_type=f32)
        for low in range(0, rows, piece):
            x_buf[pl.ds(row_of(block * rows + low), piece), :] = placed[low : low + piece]
    for s in range(0 if dense else n):
        for j in range(fold):
            for low in range(0, rows, piece):
                start = s * pos + j * rows + low
                q, rest = start // quarter, start % quarter
                p, row = rest // sub, rest % sub
                block = recv_one[s, low : low + piece, :].astype(f32)
                filt = filt_pk[q, row : row + piece, :].astype(f32)
                x_buf[pl.ds(row_of(start), piece), :] = jnp.where(
                    lane_p < chan,
                    lane_roll(block, -j * chan),
                    jnp.where(
                        lane_p < step,
                        lane_roll(filt, (1 - p) * chan),
                        jnp.where(
                            lane_p < step + chan,
                            lane_roll(block, step - half_lanes - j * chan),
                            lane_roll(block, (3 - j) * chan),
                        ),
                    ),
                )
    for item in loads[15:]:
        item.wait()

    def stage_one(n2, _):
        part = x_buf[pl.ds(n2, half, stride=group), :].astype(bf16)
        z_buf[pl.ds(n2 * stride, double_pad), :] = jnp.dot(
            fwd[n2], part, preferred_element_type=f32
        )
        return 0

    lax.fori_loop(0, second_len, stage_one, 0, unroll=16)

    lane_k = lax.broadcasted_iota(jnp.int32, (second_len, LANES), 1)
    own_sign = jnp.where((lane_k >= 3 * chan) & (lane_k < 4 * chan), -1.0, 1.0).astype(f32)
    other_sign = jnp.where((lane_k >= step) & (lane_k < 3 * chan), -1.0, 1.0).astype(f32)

    def stage_two(k1, _):
        stacked = jnp.concatenate(
            [
                z_buf[pl.ds(k1, second_len, stride=stride), :],
                z_buf[pl.ds(pad + k1, second_len, stride=stride), :],
            ],
            axis=0,
        ).astype(bf16)
        spec = jnp.dot(inner[...], stacked, preferred_element_type=f32)
        re, im = spec[:second_len], spec[second_len:]
        other_re = lane_roll(re, chan) + skip_other
        re = re + skip_own
        other_im = lane_roll(im, chan) * other_sign
        im = im * own_sign
        out = jnp.concatenate(
            [re * other_re - im * other_im, re * other_im + im * other_re], axis=0
        ).astype(bf16)
        back = jnp.dot(outer[...], out, preferred_element_type=f32)
        v_buf[pl.ds(k1, second_len, stride=stride), :] = back[:second_len]
        v_buf[pl.ds(pad + k1, second_len, stride=stride), :] = back[second_len:]
        return 0

    unroll = 11 if kept % 11 == 0 else 3 if kept % 3 == 0 else 5 if kept % 5 == 0 else 1
    lax.fori_loop(0, kept, stage_two, 0, unroll=unroll)

    def stage_three(n2, _):
        part = v_buf[pl.ds(n2 * stride, double_pad), :].astype(bf16)
        y_out[pl.ds(n2, half, stride=group), :] = jnp.dot(
            inv[n2], part, preferred_element_type=f32
        )
        return 0

    lax.fori_loop(0, second_len, stage_three, 0, unroll=16)

    for q in range(batch_n if dense else 0):
        left = jnp.concatenate(
            [
                jnp.concatenate(
                    [
                        y_out[pl.ds(row_of((q * parts + p) * rows + low), piece), :]
                        for low in range(0, rows, piece)
                    ],
                    axis=0,
                ).astype(bf16)
                for p in range(parts)
            ],
            axis=1,
        )
        packed = jnp.dot(left, gather[...], preferred_element_type=f32).astype(bf16)
        send_two[2 * q] = packed[:, :LANES]
        send_two[2 * q + 1] = packed[:, LANES : 2 * LANES]
        send_grad[q] = packed[:, 2 * LANES :]
    for d in range(0 if dense else n):
        for low in range(0, rows, piece):
            packed = None
            for j in range(fold):
                at = pl.ds(row_of(d * pos + j * rows + low), piece)
                part = lane_roll(y_out[at, :], j * step - chan)
                packed = part if j == 0 else jnp.where(lane_p >= j * step, part, packed)
            send_two[d, low : low + piece, :] = packed.astype(bf16)
    for k in range(1, n):
        copy(send_two, recv_two, 1, k).start()
    recv_two[me] = send_two[me]

    small = min(sub, piece)
    lane_q = lax.broadcasted_iota(jnp.int32, (small, LANES), 1)
    for q in range(0 if dense else batch_n):
        for low in range(0, sub, small):
            packed = None
            for j in range(parts):
                at = pl.ds(row_of(q * quarter + j * sub + low), small)
                part = lane_roll(y_out[at, :], (j - 3) * chan)
                packed = part if j == 0 else jnp.where(lane_q >= j * chan, part, packed)
            send_grad[q, low : low + small, :] = packed.astype(bf16)
    for k in range(1, batch_n):
        share(1, k).start()
    grad_pk[me_b] = send_grad[me_b]
    share_wait(1)
    total = grad_pk[0].astype(f32)
    for q in range(1, batch_n):
        total = total + grad_pk[q].astype(f32)
    grad_kernel = total * modul[...]

    em = embed.shape[0]
    lane_w = lax.broadcasted_iota(jnp.int32, (hid, LANES), 1)
    grad_weight = jnp.zeros((hid, LANES), f32)
    for j in range(parts):
        at = slice(j * sub, (j + 1) * sub)
        got = dot_as(net[4, :, at], grad_kernel, (1, 0))
        grad_weight = grad_weight + lane_roll(
            jnp.where((lane_w >= j * chan) & (lane_w < (j + 1) * chan), got, 0.0), -j * chan
        )
        net[5, :, at] = dot_as(lane_roll(weight, j * chan), grad_kernel, (1, 1)) * net[5, :, at]

    def net_backward(i, carry):
        at = pl.ds(pl.multiple_of(i * tile, LANES), tile)
        grad_act_two = net[5, :, at]
        grad_pre_two = grad_act_two * freq_two
        grad_hidden = dot_as(net[1, :, at], grad_pre_two, (1, 1))
        grad_act_one = dot_as(hidden_w[...], grad_pre_two, (1, 0)) * net[2, :, at]
        grad_pre_one = grad_act_one * freq_one
        stacked = jnp.concatenate(
            [grad_pre_one, grad_pre_two, grad_act_one * net[0, :, at], grad_act_two * net[3, :, at]],
            axis=0,
        )
        return carry[0] + grad_hidden, carry[1] + dot_as(embed[:, at], stacked, (1, 1))

    zeros = lambda r, c: jnp.zeros((r, c), f32)
    both_sums = lax.fori_loop(
        0,
        quarter // tile,
        net_backward,
        (zeros(hid, hid), zeros(em, 4 * hid)),
        unroll=2 if quarter // tile % 2 == 0 else 1,
    )
    sums = (grad_weight, both_sums[0]) + tuple(
        both_sums[1][:, i * hid : (i + 1) * hid] for i in range(4)
    )
    sums = tuple(term * (scale * 0.25) for term in sums)
    lane_h = lax.broadcasted_iota(jnp.int32, (hid, LANES), 1)
    for tile in range(tiles):
        placed = zeros(hid, LANES)
        for i in range(n):
            if (i * chan) // LANES == tile:
                off = (i * chan) % LANES
                mask = (lane_h >= off) & (lane_h < off + chan) & (me == i)
                placed = jnp.where(mask, lane_roll(sums[0], off), placed)
        extra[tile * hid : (tile + 1) * hid, :] = placed
    base = tiles * hid
    extra[base : base + hid, 0:hid] = sums[1]
    base += hid
    for term in sums[2:]:
        extra[base : base + em, 0:hid] = term
        base += em
    for tile in range(tiles):
        extra[base + tile : base + tile + 1, :] = bias_sum[:, tile * LANES : (tile + 1) * LANES]

    main_scratch, extra_scratch = sum_scratch[:5], sum_scratch[5:]
    blocks = main_scratch[1].shape[0]
    stream = [pair_sum(n, batch_n, pk_out, main_scratch, b) for b in range(blocks)]
    extra_sum = pair_sum(n, batch_n, extra, extra_scratch, 0)
    extra_sum.start_pair()
    wait_all(send_two, recv_two, 1)

    per_tile = LANES // chan
    for t in range(tiles if dense else 0):
        at = slice(t * LANES, (t + 1) * LANES)
        left = jnp.concatenate([recv_two[t * parts + i] for i in range(parts)], axis=1)
        back = jnp.dot(left, swap[...], preferred_element_type=f32)
        for u in range(parts):
            j = u % fold
            conv_buf[u // fold, j * rows : (j + 1) * rows, at] = back[:, u * LANES : (u + 1) * LANES]
    for tile in range(0 if dense else width // LANES):
        for j in range(fold):
            conv_acc = jnp.zeros((rows, LANES), f32)
            grad_acc = jnp.zeros((rows, LANES), f32)
            for i in range(per_tile):
                block = recv_two[tile * per_tile + i].astype(f32)
                own = (lane >= i * chan) & (lane < (i + 1) * chan)
                conv_acc = jnp.where(own, lane_roll(block, i * chan - j * step), conv_acc)
                grad_acc = jnp.where(own, lane_roll(block, i * chan - j * step - chan), grad_acc)
            at = pl.ds(j * rows, rows)
            conv_buf[0, at, tile * LANES : (tile + 1) * LANES] = conv_acc
            conv_buf[1, at, tile * LANES : (tile + 1) * LANES] = grad_acc

    conv = conv_buf[0]
    grad_mixed = conv_buf[1]
    gated = (gates[0].astype(f32) * conv).astype(bf16)
    grad_proj = jnp.concatenate(
        [
            (gates[3].astype(f32) * conv).astype(bf16),
            (grad_mixed * gates[2].astype(f32)).astype(bf16),
            (grad_mixed * gates[1].astype(f32)).astype(bf16),
        ],
        axis=1,
    )
    first = (((0,), (0,)), ((), ()))
    pieces = [(gated, og[...])] + [
        (tok[...], grad_proj[:, j * width : (j + 1) * width]) for j in range(3)
    ]
    per_block = len(pieces) // blocks if blocks > 1 else len(pieces)
    for i, (left, right) in enumerate(pieces):
        block = lax.dot_general(left, right, first, preferred_element_type=f32) * scale
        for j in range(tiles):
            at = (i * tiles + j) * width
            pk_out[at : at + width, :] = block[:, j * LANES : (j + 1) * LANES].astype(bf16)
        if (i + 1) % per_block == 0:
            done = (i + 1) // per_block - 1
            stream[done].start_pair()
            if done == 0:
                extra_sum.finish_pair()
                extra_sum.start_scatter()
            else:
                stream[done - 1].finish_pair()
                stream[done - 1].start_scatter()
    gt_out[...] = lax.dot_general(
        grad_proj, inw[...], (((1,), (1,)), ((), ())), preferred_element_type=f32
    ).astype(bf16)
    stream[-1].finish_pair()
    stream[-1].start_scatter()
    outs = [pltpu.make_async_copy(gt_out, gt_hbm, out_sems.at[0])]
    outs[0].start()
    every = [extra_sum] + stream
    for item in every:
        item.finish_scatter()
        item.start_gather()
    for item in every:
        item.finish_gather()
        item.start_swap()
    for i, item in enumerate(every):
        item.finish_swap()
        if i == 0:
            target = b_hbm
        else:
            target = a_hbm.at[pl.ds((i - 1) * item.size, item.size), :]
        outs.append(pltpu.make_async_copy(item.whole, target, out_sems.at[1 + i]))
        outs[-1].start()
    for item in outs:
        item.wait()


class pair_sum:
    def __init__(self, ns, nb, src, scratch, block):
        got_pair, part, got, whole, sems = (ref.at[block] for ref in scratch)
        self.got_pair, self.part, self.got, self.whole, self.sems = got_pair, part, got, whole, sems
        self.src, self.pairs = src, nb // 2
        me_s, me_b = lax.axis_index("seq"), lax.axis_index("batch")
        self.core = lax.rem(me_b, 2)
        self.chips = ns * self.pairs
        self.own = me_s * self.pairs + lax.div(me_b, 2)
        self.partner = me_b + 1 - 2 * self.core
        self.half = part.shape[0]
        self.size = 2 * self.half
        self.base = block * self.size
        self.unit = self.half // self.chips

    def rows(self, start, size):
        return pl.ds(pl.multiple_of(start, self.unit), size)

    def to_partner(self, which):
        if which == 0:
            src = self.src.at[self.rows(self.base + (1 - self.core) * self.half, self.half)]
            dst = self.got_pair
        else:
            src = dst = self.whole.at[self.rows(self.core * self.half, self.half)]
        return pltpu.make_async_remote_copy(
            src_ref=src,
            dst_ref=dst,
            send_sem=self.sems.at[which, 0, 0],
            recv_sem=self.sems.at[which, 1, 0],
            device_id={"batch": self.partner},
            device_id_type=MESH,
        )

    def to_chips(self, which):
        made = []
        for k in range(1, self.chips):
            dest = lax.rem(self.own + k, self.chips)
            if which == 0:
                src = self.part.at[self.rows(dest * self.unit, self.unit)]
                dst = self.got.at[k - 1]
            else:
                at = self.rows(self.core * self.half + self.own * self.unit, self.unit)
                src = dst = self.whole.at[at]
            made.append(
                pltpu.make_async_remote_copy(
                    src_ref=src,
                    dst_ref=dst,
                    send_sem=self.sems.at[which, 0, 1],
                    recv_sem=self.sems.at[which, 1, 1],
                    device_id={
                        "seq": lax.div(dest, self.pairs),
                        "batch": 2 * lax.rem(dest, self.pairs) + self.core,
                    },
                    device_id_type=MESH,
                )
            )
        return made

    def wait_chips(self, which):
        pltpu.make_async_remote_copy(
            src_ref=self.got,
            dst_ref=self.got,
            send_sem=self.sems.at[which, 0, 1],
            recv_sem=self.sems.at[which, 1, 1],
            device_id={"batch": self.partner},
            device_id_type=MESH,
        ).wait()

    def start_pair(self):
        self.to_partner(0).start()

    def finish_pair(self):
        self.to_partner(0).wait()
        mine = self.src[self.rows(self.base + self.core * self.half, self.half), :]
        total = mine.astype(jnp.float32) + self.got_pair[...].astype(jnp.float32)
        self.part[...] = total.astype(self.part.dtype)

    def start_scatter(self):
        for item in self.to_chips(0):
            item.start()

    def finish_scatter(self):
        self.wait_chips(0)
        total = self.part[self.rows(self.own * self.unit, self.unit), :].astype(jnp.float32)
        for k in range(1, self.chips):
            total = total + self.got[k - 1].astype(jnp.float32)
        at = self.rows(self.core * self.half + self.own * self.unit, self.unit)
        self.whole[at, :] = total.astype(self.whole.dtype)

    def start_gather(self):
        for item in self.to_chips(1):
            item.start()

    def finish_gather(self):
        self.wait_chips(1)

    def start_swap(self):
        self.to_partner(1).start()

    def finish_swap(self):
        self.to_partner(1).wait()


def unpack_kernel(main, extra, tokens_in, tokens_out, g_in, g_out, skip, emb, emb_b, hidden, hidden_b, filt, freq):
    width = g_out.shape[0]
    hid = hidden.shape[0]
    tokens_out[...] = tokens_in[...]
    at = 0
    for ref in (g_out, g_in):
        for j in range(ref.shape[1] // LANES):
            ref[:, j * LANES : (j + 1) * LANES] = main[at : at + width, :].astype(jnp.float32)
            at += width
    tiles = width // LANES
    for j in range(tiles):
        filt[:, j * LANES : (j + 1) * LANES] = extra[j * hid : (j + 1) * hid, :]
    base = tiles * hid
    hidden[...] = extra[base : base + hid, 0:hid]
    base += hid
    count = emb.shape[0]
    em = -(-(count + 1) // 8) * 8
    emb[...] = extra[base : base + count, 0:hid]
    emb_b[...] = extra[base + count : base + count + 1, 0:hid]
    hidden_b[...] = extra[base + em + count : base + em + count + 1, 0:hid]
    freq[0:1, :] = extra[base + 2 * em + count : base + 2 * em + count + 1, 0:hid]
    freq[1:2, :] = extra[base + 3 * em + count : base + 3 * em + count + 1, 0:hid]
    base += 4 * em
    for j in range(tiles):
        skip[:, j * LANES : (j + 1) * LANES] = extra[base + j : base + j + 1, :]


def vmem(count):
    return [pl.BlockSpec(memory_space=pltpu.VMEM)] * count


def sine_cosine(angle):
    turns = jnp.round(angle * (1.0 / (2.0 * math.pi)))
    reduced = angle - turns * 6.28125
    reduced = reduced - turns * 0.0019350051879882812
    reduced = reduced - turns * 3.0199157663146e-07
    half = reduced * 0.5
    square = half * half
    sin = half * (
        1.0
        + square
        * (-1.0 / 6 + square * (1.0 / 120 + square * (-1.0 / 5040 + square * (1.0 / 362880 - square / 39916800.0))))
    )
    cos = 1.0 + square * (
        -0.5
        + square
        * (1.0 / 24 + square * (-1.0 / 720 + square * (1.0 / 40320 + square * (-1.0 / 3628800 + square / 479001600.0))))
    )
    return 2.0 * sin * cos, 1.0 - 2.0 * sin * sin


def embedding(length, count):
    rows = np.zeros((-(-(count + 1) // 8) * 8, length), np.float32)
    scaled = np.arange(length) / length
    rows[0] = scaled
    for band_index in range(1, (count - 1) // 2 + 1):
        rows[2 * band_index - 1] = np.cos(2.0 * np.pi * band_index * scaled)
        rows[2 * band_index] = np.sin(2.0 * np.pi * band_index * scaled)
    rows[count] = 1.0
    return jnp.asarray(rows)


def shards(
    tokens,
    out_grad,
    in_weight,
    out_weight,
    skip_bias,
    embed_weight,
    embed_bias,
    hidden_weight,
    hidden_bias,
    filter_weight,
    sine_freq,
    decay_rate,
):
    f32, bf16 = jnp.float32, jnp.bfloat16
    tok, og = tokens[0], out_grad[0]
    pos, width = tok.shape
    ns, nb = lax.axis_size("seq"), lax.axis_size("batch")
    length = pos * ns
    chan = width // ns
    hid = hidden_weight.shape[0]
    count = embed_weight.shape[0]
    embed = embedding(length, count)
    em = embed.shape[0]

    fwd, inv, inner, outer = make_tables(length)
    second_len, double_pad, half = fwd.shape
    rows = pos // (LANES // (2 * chan))
    tiles = width // LANES
    parts = LANES // chan
    chips = ns * (nb // 2)
    unit = 2 * chips * 16
    main_rows = -(-4 * width * tiles // unit) * unit
    blocks = max(b for b in (1, 2, 4) if main_rows % (b * unit) == 0)
    unit = 2 * chips * 8
    extra_rows = -(-(tiles * hid + hid + 4 * em + tiles) // unit) * unit
    swap, place, gather = selections(
        chan, second_len <= rows and nb * parts * rows == length and parts * LANES <= 512
    )
    pair = (ns, rows, LANES)
    shared = (nb, length // nb // (LANES // chan), LANES)
    spectral = (second_len * (double_pad + 1), LANES)
    spaced = (half * (second_len + 1), LANES)
    scratch = []
    for total, kind, count_at in ((main_rows, bf16, blocks), (extra_rows, f32, 1)):
        half_rows = total // count_at // 2
        scratch += [
            pltpu.VMEM((count_at, half_rows, LANES), kind),
            pltpu.VMEM((count_at, half_rows, LANES), kind),
            pltpu.VMEM((count_at, chips - 1, half_rows // chips, LANES), kind),
            pltpu.VMEM((count_at, 2 * half_rows, LANES), kind),
            pltpu.SemaphoreType.DMA((count_at, 2, 2, 2)),
        ]
    grad_tokens, main, extra = pl.pallas_call(
        functools.partial(step_kernel, ns, nb, chan, 1.0 / math.sqrt(nb * length)),
        out_shape=(
            jax.ShapeDtypeStruct((pos, width), bf16),
            jax.ShapeDtypeStruct((main_rows, LANES), bf16),
            jax.ShapeDtypeStruct((extra_rows, LANES), f32),
        ),
        in_specs=[pl.BlockSpec(memory_space=pl.ANY)] * 20,
        out_specs=(pl.BlockSpec(memory_space=pl.ANY),) * 3,
        scratch_shapes=[
            pltpu.VMEM((pos, width), bf16),
            pltpu.SemaphoreType.DMA((2 + blocks,)),
            pltpu.VMEM(tok.shape, bf16),
            pltpu.VMEM(og.shape, bf16),
            pltpu.VMEM(in_weight.shape, bf16),
            pltpu.VMEM(out_weight.shape, bf16),
            pltpu.VMEM((em, length // nb), f32),
            pltpu.VMEM(fwd.shape, bf16),
            pltpu.VMEM(inv.shape, bf16),
            pltpu.VMEM(inner.shape, bf16),
            pltpu.VMEM(outer.shape, bf16),
            pltpu.VMEM(embed_weight.shape, f32),
            pltpu.VMEM((1, hid), f32),
            pltpu.VMEM((1, hid), f32),
            pltpu.VMEM(sine_freq.shape, f32),
            pltpu.VMEM(hidden_weight.shape, f32),
            pltpu.VMEM(filter_weight.shape, f32),
            pltpu.VMEM((1, width), f32),
            pltpu.VMEM((1, width), f32),
            pltpu.VMEM(swap.shape, bf16),
            pltpu.VMEM(place.shape, bf16),
            pltpu.VMEM(gather.shape, bf16),
            pltpu.SemaphoreType.DMA((20,)),
            pltpu.VMEM(pair, bf16),
            pltpu.VMEM(pair, bf16),
            pltpu.VMEM(pair, bf16),
            pltpu.VMEM(pair, bf16),
            pltpu.VMEM((4, pos, width), bf16),
            pltpu.VMEM(spaced, f32),
            pltpu.VMEM(spaced, f32),
            pltpu.VMEM(spectral, f32),
            pltpu.VMEM(spectral, f32),
            pltpu.VMEM((6, hid, length // nb), f32),
            pltpu.VMEM(shared, bf16),
            pltpu.VMEM(shared, bf16),
            pltpu.VMEM(shared, bf16),
            pltpu.VMEM(shared[1:], f32),
            pltpu.VMEM((2, pos, width), f32),
            pltpu.SemaphoreType.DMA((4,)),
            pltpu.SemaphoreType.DMA((4,)),
            pltpu.VMEM((main_rows, LANES), bf16),
            pltpu.VMEM((extra_rows, LANES), f32),
            pltpu.VMEM((em, hid), f32),
            pltpu.VMEM((8, hid), f32),
        ]
        + scratch,
        compiler_params=pltpu.CompilerParams(
            collective_id=0, has_side_effects=True, vmem_limit_bytes=VMEM_BYTES
        ),
        name="step",
    )(
        tok,
        og,
        in_weight,
        out_weight,
        embed,
        fwd,
        inv,
        inner,
        outer,
        embed_weight,
        embed_bias[None],
        hidden_bias[None],
        sine_freq,
        hidden_weight,
        filter_weight,
        decay_rate[None],
        skip_bias[None],
        swap,
        place,
        gather,
    )

    shapes = (
        (width, 3 * width),
        (width, width),
        (1, width),
        (count, hid),
        (1, hid),
        (hid, hid),
        (1, hid),
        (hid, width),
        (2, hid),
    )
    out = pl.pallas_call(
        unpack_kernel,
        out_shape=(jax.ShapeDtypeStruct((pos, width), bf16),)
        + tuple(jax.ShapeDtypeStruct(shape, f32) for shape in shapes),
        in_specs=vmem(3),
        out_specs=tuple(vmem(1 + len(shapes))),
        name="unpack",
    )(main, extra, grad_tokens)
    return (
        out[0][None],
        out[1],
        out[2],
        out[3][0],
        out[4],
        out[5][0],
        out[6],
        out[7][0],
        out[8],
        out[9],
    )


def solution(mesh):
    batched = P("batch", "seq", None)
    return jax.shard_map(
        shards,
        mesh=mesh,
        in_specs=(batched, batched) + (P(),) * 10,
        out_specs=(batched,) + (P(),) * 9,
        check_vma=False,
    )
```

```python
import functools
import math

import jax
import jax.numpy as jnp
import numpy as np
from jax import lax
from jax.experimental import pallas as pl
from jax.experimental.pallas import tpu as pltpu
from jax.sharding import PartitionSpec as P

highest = lax.Precision.HIGHEST
MESH = pl.DeviceIdType.MESH
LANES = 128
BLOCKS = (1, 2)
VMEM_BYTES = 66 * 1000 * 1000


def factor(length):
    total = 2 * length
    first_len = 2
    while first_len * first_len < total and total % (2 * first_len) == 0:
        first_len = first_len * 2
    return first_len, total // first_len


def make_tables(length):
    total = 2 * length
    first_len, second_len = factor(length)
    half = first_len // 2
    kept = half + 1
    pad = -(-kept // 8) * 8
    k1 = np.arange(kept)[None, :, None]
    n1 = np.arange(half)[None, None, :]
    n2 = np.arange(second_len)[:, None, None]
    angle = 2.0 * np.pi * ((k1 * (n1 * second_len + n2)) % total) / total
    fwd = np.zeros((second_len, 2 * pad, half), np.float32)
    fwd[:, :kept] = np.cos(angle)
    fwd[:, pad : pad + kept] = -np.sin(angle)
    weight = np.where((k1 == 0) | (k1 == half), 1.0, 2.0) / total
    inv = np.zeros((second_len, half, 2 * pad), np.float32)
    inv[:, :, :kept] = np.swapaxes(weight * np.cos(angle), 1, 2)
    inv[:, :, pad : pad + kept] = np.swapaxes(-weight * np.sin(angle), 1, 2)
    index = np.arange(second_len)
    small = 2.0 * np.pi * ((index[:, None] * index[None, :]) % second_len) / second_len
    cos, sin = np.cos(small), np.sin(small)
    inner = np.block([[cos, sin], [-sin, cos]])
    outer = np.block([[cos, -sin], [sin, cos]])
    return tuple(jnp.asarray(t, jnp.bfloat16) for t in (fwd, inv, inner, outer))


def selections(chan, dense):
    parts = LANES // chan
    fold = parts // 2
    if not dense:
        return tuple(jnp.zeros(s, jnp.bfloat16) for s in ((16, LANES), (1, 16, LANES), (16, LANES)))
    swap = np.zeros((parts * LANES, parts * LANES), np.float32)
    place = np.zeros((parts, 2 * LANES, LANES), np.float32)
    gather = np.zeros((parts * LANES, 3 * LANES), np.float32)
    c = np.arange(chan)
    for i in range(parts):
        for u in range(parts):
            swap[u * LANES + i * chan + c, i * LANES + u * chan + c] = 1.0
    for p in range(parts):
        e, j = p // fold, p % fold
        place[p, j * chan + c, c] = 1.0
        place[p, j * chan + c, 3 * chan + c] = 1.0
        place[p, (fold + j) * chan + c, 2 * chan + c] = 1.0
        place[p, LANES + p * chan + c, chan + c] = 1.0
        gather[p * LANES + chan + c, e * LANES + j * chan + c] = 1.0
        gather[p * LANES + 2 * chan + c, e * LANES + (fold + j) * chan + c] = 1.0
        gather[p * LANES + 3 * chan + c, 2 * LANES + p * chan + c] = 1.0
    return tuple(jnp.asarray(t, jnp.bfloat16) for t in (swap, place, gather))


def lane_roll(value, shift):
    shift = shift % LANES
    return value if shift == 0 else pltpu.roll(value, shift, 1)


def dot_as(left, right, dims):
    return lax.dot_general(
        left,
        right,
        ((dims[:1], dims[1:]), ((), ())),
        precision=highest,
        preferred_element_type=jnp.float32,
    )


def step_kernel(
    axis_n,
    batch_n,
    chan,
    scale,
    tok_hbm,
    og_hbm,
    inw_hbm,
    outw_hbm,
    embed_hbm,
    fwd_hbm,
    inv_hbm,
    inner_hbm,
    outer_hbm,
    embed_raw_hbm,
    embed_b_hbm,
    hidden_b_hbm,
    freqs_hbm,
    hidden_w_hbm,
    filter_w_hbm,
    decay_hbm,
    skip_hbm,
    swap_hbm,
    place_hbm,
    gather_hbm,
    gt_hbm,
    a_hbm,
    b_hbm,
    gt_out,
    out_sems,
    tok,
    og,
    inw,
    outw,
    embed,
    fwd,
    inv,
    inner,
    outer,
    embed_raw,
    embed_b,
    hidden_b,
    freqs,
    hidden_w,
    filter_w,
    decay_in,
    skip_in,
    swap,
    place,
    gather,
    load_sems,
    send_one,
    recv_one,
    send_two,
    recv_two,
    gates,
    x_buf,
    y_out,
    z_buf,
    v_buf,
    net,
    filt_pk,
    send_grad,
    grad_pk,
    modul,
    conv_buf,
    sems,
    net_sems,
    pk_out,
    extra,
    embed_w,
    vectors,
    *sum_scratch,
):
    n = axis_n
    me = lax.axis_index("seq")
    me_b = lax.axis_index("batch")
    pos, width = tok.shape
    rows = send_one.shape[1]
    fold = pos // rows
    step = 2 * chan
    second_len, double_pad, half = fwd.shape
    pad = double_pad // 2
    kept = half + 1
    f32, bf16 = jnp.float32, jnp.bfloat16

    seq_dests = shifted_all(me, n)
    pairs = batch_n // 2
    chip_dests = [
        (dest, lax.div(dest, pairs), 2 * lax.rem(dest, pairs) + lax.rem(me_b, 2))
        for dest in shifted_all(me * pairs + lax.div(me_b, 2), n * pairs)
    ]
    quarter = embed.shape[1]
    own_part = pl.ds(pl.multiple_of(me_b * quarter, LANES), quarter)
    loads = [
        pltpu.make_async_copy(src, dst, load_sems.at[i])
        for i, (src, dst) in enumerate(
            (
                (tok_hbm, tok),
                (inw_hbm, inw),
                (og_hbm, og),
                (outw_hbm, outw),
                (swap_hbm, swap),
                (embed_hbm.at[:, own_part], embed),
                (embed_raw_hbm, embed_raw),
                (embed_b_hbm, embed_b),
                (hidden_b_hbm, hidden_b),
                (freqs_hbm, freqs),
                (hidden_w_hbm, hidden_w),
                (filter_w_hbm, filter_w),
                (decay_hbm, decay_in),
                (skip_hbm, skip_in),
                (place_hbm, place),
                (fwd_hbm, fwd),
                (inner_hbm, inner),
                (outer_hbm, outer),
                (inv_hbm, inv),
                (gather_hbm, gather),
            )
        )
    ]
    for item in loads:
        item.start()
    barrier = pltpu.get_barrier_semaphore()
    other_core = [
        lax.rem(me_b + k, batch_n) for k in range(1, batch_n, 2)
    ]
    for seq, batch in [dest[1:] for dest in chip_dests] + [(me, peer) for peer in other_core]:
        pl.semaphore_signal(
            barrier, inc=1, device_id={"seq": seq, "batch": batch}, device_id_type=MESH
        )
    for item in loads[:4]:
        item.wait()

    proj = jnp.dot(tok[...], inw[...], preferred_element_type=f32)
    gate_out = proj[:, :width].astype(bf16)
    gate_in = proj[:, width : 2 * width].astype(bf16)
    values = proj[:, 2 * width :].astype(bf16)
    gated_grad = lax.dot_general(
        og[...], outw[...], (((1,), (1,)), ((), ())), preferred_element_type=f32
    ).astype(bf16)
    gates[0] = gate_out
    gates[1] = gate_in
    gates[2] = values
    gates[3] = gated_grad
    mixed = (values.astype(f32) * gate_in.astype(f32)).astype(bf16).astype(f32)
    grad = (gated_grad.astype(f32) * gate_out.astype(f32)).astype(bf16).astype(f32)

    lane = lax.broadcasted_iota(jnp.int32, (rows, LANES), 1)
    half_lanes = fold * chan
    parts = LANES // chan
    tiles = width // LANES
    dense = swap.shape[0] == parts * LANES
    loads[4].wait()
    if dense:
        for t in range(tiles):
            at = slice(t * LANES, (t + 1) * LANES)
            left = jnp.concatenate(
                [
                    source[j * rows : (j + 1) * rows, at].astype(bf16)
                    for source in (mixed, grad)
                    for j in range(fold)
                ],
                axis=1,
            )
            packed = jnp.dot(left, swap[...], preferred_element_type=f32).astype(bf16)
            for i in range(parts):
                send_one[t * parts + i] = packed[:, i * LANES : (i + 1) * LANES]
    for d in range(0 if dense else n):
        tile, off = (d * chan) // LANES * LANES, (d * chan) % LANES
        packed = None
        for i in range(2 * fold):
            source, j = (mixed, i) if i < fold else (grad, i - fold)
            part = lane_roll(source[j * rows : (j + 1) * rows, tile : tile + LANES], i * chan - off)
            packed = part if packed is None else jnp.where(lane >= i * chan, part, packed)
        send_one[d] = packed.astype(bf16)

    pl.semaphore_wait(barrier, len(chip_dests) + len(other_core))


    def copy(send, recv, which, k):
        dest = seq_dests[k - 1]
        return pltpu.make_async_remote_copy(
            src_ref=send.at[dest],
            dst_ref=recv.at[me],
            send_sem=sems.at[2 * which],
            recv_sem=sems.at[2 * which + 1],
            device_id={"seq": dest},
            device_id_type=MESH,
        )

    def wait_all(send, recv, which):
        others = pl.ds(0, n - 1)
        pltpu.make_async_remote_copy(
            src_ref=send.at[others],
            dst_ref=recv.at[others],
            send_sem=sems.at[2 * which],
            recv_sem=sems.at[2 * which + 1],
            device_id={"seq": me},
            device_id_type=MESH,
        ).wait()

    for k in range(1, n):
        copy(send_one, recv_one, 0, k).start()
    recv_one[me] = send_one[me]
    mixed = (gates[2].astype(f32) * gates[1].astype(f32)).astype(bf16).astype(f32)
    grad = (gates[3].astype(f32) * gates[0].astype(f32)).astype(bf16).astype(f32)
    bias_sum = jnp.sum(mixed * grad, axis=0, keepdims=True) * scale
    v_buf[...] = jnp.zeros_like(v_buf)
    extra[...] = jnp.zeros_like(extra)
    length = n * pos
    group = second_len + 1
    stride = double_pad + 1
    hid = hidden_w.shape[0]

    def select_own(value, target):
        lane_v = lax.broadcasted_iota(jnp.int32, (value.shape[0], LANES), 1)
        got = jnp.zeros((value.shape[0], LANES), f32)
        for i in range(n):
            tile, off = (i * chan) // LANES * LANES, (i * chan) % LANES
            part = lane_roll(value[:, tile : tile + LANES], target - off)
            got = jnp.where(jnp.logical_and(me == i, lane_v >= 0), part, got)
        return jnp.where((lane_v >= target) & (lane_v < target + chan), got, 0.0)

    sub = quarter // parts
    for item in loads[5:15]:
        item.wait()
    weight = select_own(filter_w[...], 0)
    decay_own = select_own(decay_in[...], 0)
    decay = decay_own
    for j in range(1, parts):
        decay = decay + lane_roll(decay_own, j * chan)
    skip_own = select_own(skip_in[...], chan)
    skip_other = select_own(skip_in[...], step)
    inputs = embed_raw.shape[0]
    embed_w[...] = jnp.zeros_like(embed_w)
    embed_w[0:inputs, :] = embed_raw[...]
    embed_w[inputs : inputs + 1, :] = embed_b[...]
    vectors[...] = jnp.zeros_like(vectors)
    vectors[0:2, :] = freqs[...]
    vectors[2:3, :] = hidden_b[...]
    eye = (
        lax.broadcasted_iota(jnp.int32, (8, 8), 0) == lax.broadcasted_iota(jnp.int32, (8, 8), 1)
    ).astype(f32)
    columns = dot_as(vectors[...], eye, (0, 0))
    freq_one, freq_two = columns[:, 0:1], columns[:, 1:2]
    tile = min(256, quarter)
    def net_forward(i, _):
        at = pl.ds(pl.multiple_of(i * tile, LANES), tile)
        pre_one = dot_as(embed_w[...], embed[:, at], (0, 0))
        act_one, cos_one = sine_cosine(freq_one * pre_one)
        pre_two = dot_as(hidden_w[...], act_one, (0, 0)) + columns[:, 2:3]
        act_two, cos_two = sine_cosine(freq_two * pre_two)
        net[0, :, at] = pre_one
        net[1, :, at] = act_one
        net[2, :, at] = cos_one
        net[3, :, at] = pre_two
        net[4, :, at] = act_two
        net[5, :, at] = cos_two
        return 0

    lax.fori_loop(0, quarter // tile, net_forward, 0, unroll=2 if quarter // tile % 2 == 0 else 1)
    lane_s = lax.broadcasted_iota(jnp.int32, (sub, LANES), 1)
    time = lax.broadcasted_iota(jnp.int32, (sub, LANES), 0) + me_b * quarter
    for j in range(1, parts):
        time = time + jnp.where(lane_s >= j * chan, sub, 0)
    modul[...] = jnp.exp(-decay * time.astype(f32)) * (4.0 / math.sqrt(length))
    packed_filt = jnp.zeros((sub, LANES), f32)
    for j in range(parts):
        packed_filt = packed_filt + dot_as(
            net[4, :, j * sub : (j + 1) * sub], lane_roll(weight, j * chan), (0, 0)
        )
    filt_pk[me_b] = (packed_filt * modul[...]).astype(bf16)

    def share(which, k):
        dest = lax.rem(me_b + k, batch_n)
        return pltpu.make_async_remote_copy(
            src_ref=filt_pk.at[me_b] if which == 0 else send_grad.at[dest],
            dst_ref=filt_pk.at[me_b] if which == 0 else grad_pk.at[me_b],
            send_sem=net_sems.at[2 * which],
            recv_sem=net_sems.at[2 * which + 1],
            device_id={"batch": dest},
            device_id_type=MESH,
        )

    def share_wait(which):
        others = pl.ds(0, batch_n - 1)
        pltpu.make_async_remote_copy(
            src_ref=grad_pk.at[others],
            dst_ref=grad_pk.at[others],
            send_sem=net_sems.at[2 * which],
            recv_sem=net_sems.at[2 * which + 1],
            device_id={"batch": me_b},
            device_id_type=MESH,
        ).wait()

    for k in range(1, batch_n):
        share(0, k).start()
    wait_all(send_one, recv_one, 0)
    share_wait(0)

    piece = min(rows, second_len)
    lane_p = lax.broadcasted_iota(jnp.int32, (piece, LANES), 1)

    def row_of(position):
        return position // second_len * group + position % second_len

    for block in range(n * fold if dense else 0):
        q, p = block // parts, block % parts
        both = jnp.concatenate([recv_one[block // fold], filt_pk[q]], axis=1)
        placed = jnp.dot(both, place[p], preferred_element_type=f32)
        for low in range(0, rows, piece):
            x_buf[pl.ds(row_of(block * rows + low), piece), :] = placed[low : low + piece]
    for s in range(0 if dense else n):
        for j in range(fold):
            for low in range(0, rows, piece):
                start = s * pos + j * rows + low
                q, rest = start // quarter, start % quarter
                p, row = rest // sub, rest % sub
                block = recv_one[s, low : low + piece, :].astype(f32)
                filt = filt_pk[q, row : row + piece, :].astype(f32)
                x_buf[pl.ds(row_of(start), piece), :] = jnp.where(
                    lane_p < chan,
                    lane_roll(block, -j * chan),
                    jnp.where(
                        lane_p < step,
                        lane_roll(filt, (1 - p) * chan),
                        jnp.where(
                            lane_p < step + chan,
                            lane_roll(block, step - half_lanes - j * chan),
                            lane_roll(block, (3 - j) * chan),
                        ),
                    ),
                )
    for item in loads[15:]:
        item.wait()

    def stage_one(n2, _):
        part = x_buf[pl.ds(n2, half, stride=group), :].astype(bf16)
        z_buf[pl.ds(n2 * stride, double_pad), :] = jnp.dot(
            fwd[n2], part, preferred_element_type=f32
        )
        return 0

    lax.fori_loop(0, second_len, stage_one, 0, unroll=16)

    lane_k = lax.broadcasted_iota(jnp.int32, (second_len, LANES), 1)
    own_sign = jnp.where((lane_k >= 3 * chan) & (lane_k < 4 * chan), -1.0, 1.0).astype(f32)
    other_sign = jnp.where((lane_k >= step) & (lane_k < 3 * chan), -1.0, 1.0).astype(f32)

    def stage_two(k1, _):
        stacked = jnp.concatenate(
            [
                z_buf[pl.ds(k1, second_len, stride=stride), :],
                z_buf[pl.ds(pad + k1, second_len, stride=stride), :],
            ],
            axis=0,
        ).astype(bf16)
        spec = jnp.dot(inner[...], stacked, preferred_element_type=f32)
        re, im = spec[:second_len], spec[second_len:]
        other_re = lane_roll(re, chan) + skip_other
        re = re + skip_own
        other_im = lane_roll(im, chan) * other_sign
        im = im * own_sign
        out = jnp.concatenate(
            [re * other_re - im * other_im, re * other_im + im * other_re], axis=0
        ).astype(bf16)
        back = jnp.dot(outer[...], out, preferred_element_type=f32)
        v_buf[pl.ds(k1, second_len, stride=stride), :] = back[:second_len]
        v_buf[pl.ds(pad + k1, second_len, stride=stride), :] = back[second_len:]
        return 0

    unroll = 11 if kept % 11 == 0 else 3 if kept % 3 == 0 else 5 if kept % 5 == 0 else 1
    lax.fori_loop(0, kept, stage_two, 0, unroll=unroll)

    def stage_three(n2, _):
        part = v_buf[pl.ds(n2 * stride, double_pad), :].astype(bf16)
        y_out[pl.ds(n2, half, stride=group), :] = jnp.dot(
            inv[n2], part, preferred_element_type=f32
        )
        return 0

    lax.fori_loop(0, second_len, stage_three, 0, unroll=16)

    for q in range(batch_n if dense else 0):
        left = jnp.concatenate(
            [
                jnp.concatenate(
                    [
                        y_out[pl.ds(row_of((q * parts + p) * rows + low), piece), :]
                        for low in range(0, rows, piece)
                    ],
                    axis=0,
                ).astype(bf16)
                for p in range(parts)
            ],
            axis=1,
        )
        packed = jnp.dot(left, gather[...], preferred_element_type=f32).astype(bf16)
        send_two[2 * q] = packed[:, :LANES]
        send_two[2 * q + 1] = packed[:, LANES : 2 * LANES]
        send_grad[q] = packed[:, 2 * LANES :]
    for d in range(0 if dense else n):
        for low in range(0, rows, piece):
            packed = None
            for j in range(fold):
                at = pl.ds(row_of(d * pos + j * rows + low), piece)
                part = lane_roll(y_out[at, :], j * step - chan)
                packed = part if j == 0 else jnp.where(lane_p >= j * step, part, packed)
            send_two[d, low : low + piece, :] = packed.astype(bf16)
    for k in range(1, n):
        copy(send_two, recv_two, 1, k).start()
    recv_two[me] = send_two[me]

    small = min(sub, piece)
    lane_q = lax.broadcasted_iota(jnp.int32, (small, LANES), 1)
    for q in range(0 if dense else batch_n):
        for low in range(0, sub, small):
            packed = None
            for j in range(parts):
                at = pl.ds(row_of(q * quarter + j * sub + low), small)
                part = lane_roll(y_out[at, :], (j - 3) * chan)
                packed = part if j == 0 else jnp.where(lane_q >= j * chan, part, packed)
            send_grad[q, low : low + small, :] = packed.astype(bf16)
    for k in range(1, batch_n):
        share(1, k).start()
    grad_pk[me_b] = send_grad[me_b]
    share_wait(1)
    total = grad_pk[0].astype(f32)
    for q in range(1, batch_n):
        total = total + grad_pk[q].astype(f32)
    grad_kernel = total * modul[...]

    em = embed.shape[0]
    lane_w = lax.broadcasted_iota(jnp.int32, (hid, LANES), 1)
    grad_weight = jnp.zeros((hid, LANES), f32)
    for j in range(parts):
        at = slice(j * sub, (j + 1) * sub)
        got = dot_as(net[4, :, at], grad_kernel, (1, 0))
        grad_weight = grad_weight + lane_roll(
            jnp.where((lane_w >= j * chan) & (lane_w < (j + 1) * chan), got, 0.0), -j * chan
        )
        net[5, :, at] = dot_as(lane_roll(weight, j * chan), grad_kernel, (1, 1)) * net[5, :, at]

    def net_backward(i, carry):
        at = pl.ds(pl.multiple_of(i * tile, LANES), tile)
        grad_act_two = net[5, :, at]
        grad_pre_two = grad_act_two * freq_two
        grad_hidden = dot_as(net[1, :, at], grad_pre_two, (1, 1))
        grad_act_one = dot_as(hidden_w[...], grad_pre_two, (1, 0)) * net[2, :, at]
        grad_pre_one = grad_act_one * freq_one
        stacked = jnp.concatenate(
            [grad_pre_one, grad_pre_two, grad_act_one * net[0, :, at], grad_act_two * net[3, :, at]],
            axis=0,
        )
        return carry[0] + grad_hidden, carry[1] + dot_as(embed[:, at], stacked, (1, 1))

    zeros = lambda r, c: jnp.zeros((r, c), f32)
    both_sums = lax.fori_loop(
        0,
        quarter // tile,
        net_backward,
        (zeros(hid, hid), zeros(em, 4 * hid)),
        unroll=2 if quarter // tile % 2 == 0 else 1,
    )
    sums = (grad_weight, both_sums[0]) + tuple(
        both_sums[1][:, i * hid : (i + 1) * hid] for i in range(4)
    )
    sums = tuple(term * (scale * 0.25) for term in sums)
    lane_h = lax.broadcasted_iota(jnp.int32, (hid, LANES), 1)
    for tile in range(tiles):
        placed = zeros(hid, LANES)
        for i in range(n):
            if (i * chan) // LANES == tile:
                off = (i * chan) % LANES
                mask = (lane_h >= off) & (lane_h < off + chan) & (me == i)
                placed = jnp.where(mask, lane_roll(sums[0], off), placed)
        extra[tile * hid : (tile + 1) * hid, :] = placed
    base = tiles * hid
    extra[base : base + hid, 0:hid] = sums[1]
    base += hid
    for term in sums[2:]:
        extra[base : base + em, 0:hid] = term
        base += em
    for tile in range(tiles):
        extra[base + tile : base + tile + 1, :] = bias_sum[:, tile * LANES : (tile + 1) * LANES]

    main_scratch, extra_scratch = sum_scratch[:5], sum_scratch[5:]
    blocks = main_scratch[1].shape[0]
    stream = [pair_sum(n, batch_n, pk_out, main_scratch, b, chip_dests) for b in range(blocks)]
    extra_sum = pair_sum(n, batch_n, extra, extra_scratch, 0, chip_dests)
    extra_sum.start_pair()
    wait_all(send_two, recv_two, 1)

    per_tile = LANES // chan
    for t in range(tiles if dense else 0):
        at = slice(t * LANES, (t + 1) * LANES)
        left = jnp.concatenate([recv_two[t * parts + i] for i in range(parts)], axis=1)
        back = jnp.dot(left, swap[...], preferred_element_type=f32)
        for u in range(parts):
            j = u % fold
            conv_buf[u // fold, j * rows : (j + 1) * rows, at] = back[:, u * LANES : (u + 1) * LANES]
    for tile in range(0 if dense else width // LANES):
        for j in range(fold):
            conv_acc = jnp.zeros((rows, LANES), f32)
            grad_acc = jnp.zeros((rows, LANES), f32)
            for i in range(per_tile):
                block = recv_two[tile * per_tile + i].astype(f32)
                own = (lane >= i * chan) & (lane < (i + 1) * chan)
                conv_acc = jnp.where(own, lane_roll(block, i * chan - j * step), conv_acc)
                grad_acc = jnp.where(own, lane_roll(block, i * chan - j * step - chan), grad_acc)
            at = pl.ds(j * rows, rows)
            conv_buf[0, at, tile * LANES : (tile + 1) * LANES] = conv_acc
            conv_buf[1, at, tile * LANES : (tile + 1) * LANES] = grad_acc

    conv = conv_buf[0]
    grad_mixed = conv_buf[1]
    gated = (gates[0].astype(f32) * conv).astype(bf16)
    grad_proj = jnp.concatenate(
        [
            (gates[3].astype(f32) * conv).astype(bf16),
            (grad_mixed * gates[2].astype(f32)).astype(bf16),
            (grad_mixed * gates[1].astype(f32)).astype(bf16),
        ],
        axis=1,
    )
    first = (((0,), (0,)), ((), ()))
    pieces = [(gated, og[...])] + [
        (tok[...], grad_proj[:, j * width : (j + 1) * width]) for j in range(3)
    ]
    per_block = len(pieces) // blocks if blocks > 1 else len(pieces)
    for i, (left, right) in enumerate(pieces):
        block = lax.dot_general(left, right, first, preferred_element_type=f32) * scale
        for j in range(tiles):
            at = (i * tiles + j) * width
            pk_out[at : at + width, :] = block[:, j * LANES : (j + 1) * LANES].astype(bf16)
        if (i + 1) % per_block == 0:
            done = (i + 1) // per_block - 1
            stream[done].start_pair()
            if done == 0:
                extra_sum.finish_pair()
                extra_sum.start_scatter()
            else:
                stream[done - 1].finish_pair()
                stream[done - 1].start_scatter()
    stream[-1].finish_pair()
    stream[-1].start_scatter()
    extra_sum.finish_scatter()
    extra_sum.start_gather()
    gt_out[...] = lax.dot_general(
        grad_proj, inw[...], (((1,), (1,)), ((), ())), preferred_element_type=f32
    ).astype(bf16)
    outs = [pltpu.make_async_copy(gt_out, gt_hbm, out_sems.at[0, 0])]
    outs[0].start()
    for item in stream:
        item.finish_scatter()
        item.start_gather()
    extra_sum.finish_gather()
    extra_sum.start_swap()

    def finish(i, item):
        target, base = (b_hbm, 0) if i == 0 else (a_hbm, (i - 1) * item.size)
        for side in range(2):
            core = item.core if side == 0 else 1 - item.core
            at = item.rows(core * item.half, item.half)
            to = item.rows(base + core * item.half, item.half)
            outs.append(
                pltpu.make_async_copy(item.whole.at[at], target.at[to], out_sems.at[1 + i, side])
            )
            if side == 1:
                item.finish_swap()
            outs[-1].start()

    finish(0, extra_sum)
    for item in stream:
        item.finish_gather()
        item.start_swap()
    for i, item in enumerate(stream):
        finish(1 + i, item)
    for item in outs:
        item.wait()


def digits_of(count):
    radices = []
    while count % 2 == 0 and count > 4 and len(radices) < 2:
        radices.append(2)
        count = count // 2
    return [count] + radices


def far_first(count):
    radices = digits_of(count)
    moves = [()]
    for radix in radices:
        moves = [m + (d,) for m in moves for d in range(radix)]
    moves = [m for m in moves if any(m)]
    return sorted(moves, key=lambda m: -2 * min(m[0], radices[0] - m[0]) - sum(m[1:]))


def shifted_all(own, count):
    radices = digits_of(count)
    below, tables = count, []
    for radix in radices:
        below = below // radix
        digit = lax.rem(lax.div(own, below), radix)
        tables.append([lax.rem(digit + step, radix) * below for step in range(radix)])
    made = []
    for move in far_first(count):
        total = tables[0][move[0]]
        for table, step in zip(tables[1:], move[1:]):
            total = total + table[step]
        made.append(total)
    return made


class pair_sum:
    def __init__(self, ns, nb, src, scratch, block, dests):
        self.dests = dests
        got_pair, part, got, whole, sems = (ref.at[block] for ref in scratch)
        self.got_pair, self.part, self.got, self.whole, self.sems = got_pair, part, got, whole, sems
        self.src, self.pairs = src, nb // 2
        me_s, me_b = lax.axis_index("seq"), lax.axis_index("batch")
        self.core = lax.rem(me_b, 2)
        self.chips = ns * self.pairs
        self.own = me_s * self.pairs + lax.div(me_b, 2)
        self.partner = me_b + 1 - 2 * self.core
        self.half = part.shape[0]
        self.size = 2 * self.half
        self.base = block * self.size
        self.unit = self.half // self.chips

    def rows(self, start, size):
        return pl.ds(pl.multiple_of(start, self.unit), size)

    def to_partner(self, which):
        if which == 0:
            src = self.src.at[self.rows(self.base + (1 - self.core) * self.half, self.half)]
            dst = self.got_pair
        else:
            src = dst = self.whole.at[self.rows(self.core * self.half, self.half)]
        return pltpu.make_async_remote_copy(
            src_ref=src,
            dst_ref=dst,
            send_sem=self.sems.at[which, 0, 0],
            recv_sem=self.sems.at[which, 1, 0],
            device_id={"batch": self.partner},
            device_id_type=MESH,
        )

    def to_chips(self, which):
        made = []
        for i, (dest, seq, batch) in enumerate(self.dests):
            if which == 0:
                src = self.part.at[self.rows(dest * self.unit, self.unit)]
                dst = self.got.at[i]
            else:
                at = self.rows(self.core * self.half + self.own * self.unit, self.unit)
                src = dst = self.whole.at[at]
            made.append(
                pltpu.make_async_remote_copy(
                    src_ref=src,
                    dst_ref=dst,
                    send_sem=self.sems.at[which, 0, 1],
                    recv_sem=self.sems.at[which, 1, 1],
                    device_id={"seq": seq, "batch": batch},
                    device_id_type=MESH,
                )
            )
        return made

    def wait_chips(self, which):
        pltpu.make_async_remote_copy(
            src_ref=self.got,
            dst_ref=self.got,
            send_sem=self.sems.at[which, 0, 1],
            recv_sem=self.sems.at[which, 1, 1],
            device_id={"batch": self.partner},
            device_id_type=MESH,
        ).wait()

    def start_pair(self):
        self.to_partner(0).start()

    def finish_pair(self):
        self.to_partner(0).wait()
        mine = self.src[self.rows(self.base + self.core * self.half, self.half), :]
        total = mine.astype(jnp.float32) + self.got_pair[...].astype(jnp.float32)
        self.part[...] = total.astype(self.part.dtype)

    def start_scatter(self):
        for item in self.to_chips(0):
            item.start()

    def finish_scatter(self):
        self.wait_chips(0)
        total = self.part[self.rows(self.own * self.unit, self.unit), :].astype(jnp.float32)
        for k in range(1, self.chips):
            total = total + self.got[k - 1].astype(jnp.float32)
        at = self.rows(self.core * self.half + self.own * self.unit, self.unit)
        self.whole[at, :] = total.astype(self.whole.dtype)

    def start_gather(self):
        for item in self.to_chips(1):
            item.start()

    def finish_gather(self):
        self.wait_chips(1)

    def start_swap(self):
        self.to_partner(1).start()

    def finish_swap(self):
        self.to_partner(1).wait()


def unpack_kernel(main, extra, tokens_in, tokens_out, g_in, g_out, skip, emb, emb_b, hidden, hidden_b, filt, freq):
    width = g_out.shape[0]
    hid = hidden.shape[0]
    tokens_out[...] = tokens_in[...]
    at = 0
    for ref in (g_out, g_in):
        for j in range(ref.shape[1] // LANES):
            ref[:, j * LANES : (j + 1) * LANES] = main[at : at + width, :].astype(jnp.float32)
            at += width
    tiles = width // LANES
    for j in range(tiles):
        filt[:, j * LANES : (j + 1) * LANES] = extra[j * hid : (j + 1) * hid, :]
    base = tiles * hid
    hidden[...] = extra[base : base + hid, 0:hid]
    base += hid
    count = emb.shape[0]
    em = -(-(count + 1) // 8) * 8
    emb[...] = extra[base : base + count, 0:hid]
    emb_b[...] = extra[base + count : base + count + 1, 0:hid]
    hidden_b[...] = extra[base + em + count : base + em + count + 1, 0:hid]
    freq[0:1, :] = extra[base + 2 * em + count : base + 2 * em + count + 1, 0:hid]
    freq[1:2, :] = extra[base + 3 * em + count : base + 3 * em + count + 1, 0:hid]
    base += 4 * em
    for j in range(tiles):
        skip[:, j * LANES : (j + 1) * LANES] = extra[base + j : base + j + 1, :]


def vmem(count):
    return [pl.BlockSpec(memory_space=pltpu.VMEM)] * count


def sine_cosine(angle):
    turns = jnp.round(angle * (1.0 / (2.0 * math.pi)))
    reduced = angle - turns * 6.28125
    reduced = reduced - turns * 0.0019350051879882812
    reduced = reduced - turns * 3.0199157663146e-07
    half = reduced * 0.5
    square = half * half
    sin = half * (
        1.0
        + square
        * (-1.0 / 6 + square * (1.0 / 120 + square * (-1.0 / 5040 + square * (1.0 / 362880 - square / 39916800.0))))
    )
    cos = 1.0 + square * (
        -0.5
        + square
        * (1.0 / 24 + square * (-1.0 / 720 + square * (1.0 / 40320 + square * (-1.0 / 3628800 + square / 479001600.0))))
    )
    return 2.0 * sin * cos, 1.0 - 2.0 * sin * sin


def embedding(length, count):
    rows = np.zeros((-(-(count + 1) // 8) * 8, length), np.float32)
    scaled = np.arange(length) / length
    rows[0] = scaled
    for band_index in range(1, (count - 1) // 2 + 1):
        rows[2 * band_index - 1] = np.cos(2.0 * np.pi * band_index * scaled)
        rows[2 * band_index] = np.sin(2.0 * np.pi * band_index * scaled)
    rows[count] = 1.0
    return jnp.asarray(rows)


def shards(
    tokens,
    out_grad,
    in_weight,
    out_weight,
    skip_bias,
    embed_weight,
    embed_bias,
    hidden_weight,
    hidden_bias,
    filter_weight,
    sine_freq,
    decay_rate,
):
    f32, bf16 = jnp.float32, jnp.bfloat16
    tok, og = tokens[0], out_grad[0]
    pos, width = tok.shape
    ns, nb = lax.axis_size("seq"), lax.axis_size("batch")
    length = pos * ns
    chan = width // ns
    hid = hidden_weight.shape[0]
    count = embed_weight.shape[0]
    embed = embedding(length, count)
    em = embed.shape[0]

    fwd, inv, inner, outer = make_tables(length)
    second_len, double_pad, half = fwd.shape
    rows = pos // (LANES // (2 * chan))
    tiles = width // LANES
    parts = LANES // chan
    chips = ns * (nb // 2)
    unit = 2 * chips * 16
    main_rows = -(-4 * width * tiles // unit) * unit
    blocks = max(b for b in BLOCKS if main_rows % (b * unit) == 0)
    unit = 2 * chips * 8
    extra_rows = -(-(tiles * hid + hid + 4 * em + tiles) // unit) * unit
    swap, place, gather = selections(
        chan, second_len <= rows and nb * parts * rows == length and parts * LANES <= 512
    )
    pair = (ns, rows, LANES)
    shared = (nb, length // nb // (LANES // chan), LANES)
    spectral = (second_len * (double_pad + 1), LANES)
    spaced = (half * (second_len + 1), LANES)
    scratch = []
    for total, kind, count_at in ((main_rows, bf16, blocks), (extra_rows, f32, 1)):
        half_rows = total // count_at // 2
        scratch += [
            pltpu.VMEM((count_at, half_rows, LANES), kind),
            pltpu.VMEM((count_at, half_rows, LANES), kind),
            pltpu.VMEM((count_at, chips - 1, half_rows // chips, LANES), kind),
            pltpu.VMEM((count_at, 2 * half_rows, LANES), kind),
            pltpu.SemaphoreType.DMA((count_at, 2, 2, 2)),
        ]
    grad_tokens, main, extra = pl.pallas_call(
        functools.partial(step_kernel, ns, nb, chan, 1.0 / math.sqrt(nb * length)),
        out_shape=(
            jax.ShapeDtypeStruct((pos, width), bf16),
            jax.ShapeDtypeStruct((main_rows, LANES), bf16),
            jax.ShapeDtypeStruct((extra_rows, LANES), f32),
        ),
        in_specs=[pl.BlockSpec(memory_space=pl.ANY)] * 20,
        out_specs=(pl.BlockSpec(memory_space=pl.ANY),) * 3,
        scratch_shapes=[
            pltpu.VMEM((pos, width), bf16),
            pltpu.SemaphoreType.DMA((2 + blocks, 2)),
            pltpu.VMEM(tok.shape, bf16),
            pltpu.VMEM(og.shape, bf16),
            pltpu.VMEM(in_weight.shape, bf16),
            pltpu.VMEM(out_weight.shape, bf16),
            pltpu.VMEM((em, length // nb), f32),
            pltpu.VMEM(fwd.shape, bf16),
            pltpu.VMEM(inv.shape, bf16),
            pltpu.VMEM(inner.shape, bf16),
            pltpu.VMEM(outer.shape, bf16),
            pltpu.VMEM(embed_weight.shape, f32),
            pltpu.VMEM((1, hid), f32),
            pltpu.VMEM((1, hid), f32),
            pltpu.VMEM(sine_freq.shape, f32),
            pltpu.VMEM(hidden_weight.shape, f32),
            pltpu.VMEM(filter_weight.shape, f32),
            pltpu.VMEM((1, width), f32),
            pltpu.VMEM((1, width), f32),
            pltpu.VMEM(swap.shape, bf16),
            pltpu.VMEM(place.shape, bf16),
            pltpu.VMEM(gather.shape, bf16),
            pltpu.SemaphoreType.DMA((20,)),
            pltpu.VMEM(pair, bf16),
            pltpu.VMEM(pair, bf16),
            pltpu.VMEM(pair, bf16),
            pltpu.VMEM(pair, bf16),
            pltpu.VMEM((4, pos, width), bf16),
            pltpu.VMEM(spaced, f32),
            pltpu.VMEM(spaced, f32),
            pltpu.VMEM(spectral, f32),
            pltpu.VMEM(spectral, f32),
            pltpu.VMEM((6, hid, length // nb), f32),
            pltpu.VMEM(shared, bf16),
            pltpu.VMEM(shared, bf16),
            pltpu.VMEM(shared, bf16),
            pltpu.VMEM(shared[1:], f32),
            pltpu.VMEM((2, pos, width), f32),
            pltpu.SemaphoreType.DMA((4,)),
            pltpu.SemaphoreType.DMA((4,)),
            pltpu.VMEM((main_rows, LANES), bf16),
            pltpu.VMEM((extra_rows, LANES), f32),
            pltpu.VMEM((em, hid), f32),
            pltpu.VMEM((8, hid), f32),
        ]
        + scratch,
        compiler_params=pltpu.CompilerParams(
            collective_id=0, has_side_effects=True, vmem_limit_bytes=VMEM_BYTES
        ),
        name="step",
    )(
        tok,
        og,
        in_weight,
        out_weight,
        embed,
        fwd,
        inv,
        inner,
        outer,
        embed_weight,
        embed_bias[None],
        hidden_bias[None],
        sine_freq,
        hidden_weight,
        filter_weight,
        decay_rate[None],
        skip_bias[None],
        swap,
        place,
        gather,
    )

    shapes = (
        (width, 3 * width),
        (width, width),
        (1, width),
        (count, hid),
        (1, hid),
        (hid, hid),
        (1, hid),
        (hid, width),
        (2, hid),
    )
    out = pl.pallas_call(
        unpack_kernel,
        out_shape=(jax.ShapeDtypeStruct((pos, width), bf16),)
        + tuple(jax.ShapeDtypeStruct(shape, f32) for shape in shapes),
        in_specs=vmem(3),
        out_specs=tuple(vmem(1 + len(shapes))),
        name="unpack",
    )(main, extra, grad_tokens)
    return (
        out[0][None],
        out[1],
        out[2],
        out[3][0],
        out[4],
        out[5][0],
        out[6],
        out[7][0],
        out[8],
        out[9],
    )


def solution(mesh):
    batched = P("batch", "seq", None)
    return jax.shard_map(
        shards,
        mesh=mesh,
        in_specs=(batched, batched) + (P(),) * 10,
        out_specs=(batched,) + (P(),) * 9,
        check_vma=False,
    )
```

```python
import functools
import math

import jax
import jax.numpy as jnp
import numpy as np
from jax import lax
from jax.experimental import pallas as pl
from jax.experimental.pallas import tpu as pltpu
from jax.sharding import PartitionSpec as P

highest = lax.Precision.HIGHEST
MESH = pl.DeviceIdType.MESH
LANES = 128
BLOCKS = (1, 2)
VMEM_BYTES = 66 * 1000 * 1000


def factor(length):
    total = 2 * length
    first_len = 2
    while first_len * first_len < total and total % (2 * first_len) == 0:
        first_len = first_len * 2
    return first_len, total // first_len


def make_tables(length):
    total = 2 * length
    first_len, second_len = factor(length)
    half = first_len // 2
    kept = half + 1
    pad = -(-kept // 8) * 8
    k1 = np.arange(kept)[None, :, None]
    n1 = np.arange(half)[None, None, :]
    n2 = np.arange(second_len)[:, None, None]
    angle = 2.0 * np.pi * ((k1 * (n1 * second_len + n2)) % total) / total
    fwd = np.zeros((second_len, 2 * pad, half), np.float32)
    fwd[:, :kept] = np.cos(angle)
    fwd[:, pad : pad + kept] = -np.sin(angle)
    weight = np.where((k1 == 0) | (k1 == half), 1.0, 2.0) / total
    inv = np.zeros((second_len, half, 2 * pad), np.float32)
    inv[:, :, :kept] = np.swapaxes(weight * np.cos(angle), 1, 2)
    inv[:, :, pad : pad + kept] = np.swapaxes(-weight * np.sin(angle), 1, 2)
    index = np.arange(second_len)
    small = 2.0 * np.pi * ((index[:, None] * index[None, :]) % second_len) / second_len
    cos, sin = np.cos(small), np.sin(small)
    inner = np.block([[cos, sin], [-sin, cos]])
    outer = np.block([[cos, -sin], [sin, cos]])
    return tuple(jnp.asarray(t, jnp.bfloat16) for t in (fwd, inv, inner, outer))


def selections(chan, dense):
    parts = LANES // chan
    fold = parts // 2
    if not dense:
        return tuple(jnp.zeros(s, jnp.bfloat16) for s in ((16, LANES), (1, 16, LANES), (16, LANES)))
    swap = np.zeros((parts * LANES, parts * LANES), np.float32)
    place = np.zeros((parts, 2 * LANES, LANES), np.float32)
    gather = np.zeros((parts * LANES, 3 * LANES), np.float32)
    c = np.arange(chan)
    for i in range(parts):
        for u in range(parts):
            swap[u * LANES + i * chan + c, i * LANES + u * chan + c] = 1.0
    for p in range(parts):
        e, j = p // fold, p % fold
        place[p, j * chan + c, c] = 1.0
        place[p, j * chan + c, 3 * chan + c] = 1.0
        place[p, (fold + j) * chan + c, 2 * chan + c] = 1.0
        place[p, LANES + p * chan + c, chan + c] = 1.0
        gather[p * LANES + chan + c, e * LANES + j * chan + c] = 1.0
        gather[p * LANES + 2 * chan + c, e * LANES + (fold + j) * chan + c] = 1.0
        gather[p * LANES + 3 * chan + c, 2 * LANES + p * chan + c] = 1.0
    return tuple(jnp.asarray(t, jnp.bfloat16) for t in (swap, place, gather))


def lane_roll(value, shift):
    shift = shift % LANES
    return value if shift == 0 else pltpu.roll(value, shift, 1)


def dot_as(left, right, dims):
    return lax.dot_general(
        left,
        right,
        ((dims[:1], dims[1:]), ((), ())),
        precision=highest,
        preferred_element_type=jnp.float32,
    )


def step_kernel(
    axis_n,
    batch_n,
    chan,
    scale,
    tok_hbm,
    og_hbm,
    inw_hbm,
    outw_hbm,
    embed_hbm,
    fwd_hbm,
    inv_hbm,
    inner_hbm,
    outer_hbm,
    embed_raw_hbm,
    embed_b_hbm,
    hidden_b_hbm,
    freqs_hbm,
    hidden_w_hbm,
    filter_w_hbm,
    decay_hbm,
    skip_hbm,
    swap_hbm,
    place_hbm,
    gather_hbm,
    gt_hbm,
    a_hbm,
    b_hbm,
    gt_out,
    out_sems,
    tok,
    og,
    inw,
    outw,
    embed,
    fwd,
    inv,
    inner,
    outer,
    embed_raw,
    embed_b,
    hidden_b,
    freqs,
    hidden_w,
    filter_w,
    decay_in,
    skip_in,
    swap,
    place,
    gather,
    load_sems,
    send_one,
    recv_one,
    send_two,
    recv_two,
    gates,
    x_buf,
    y_out,
    z_buf,
    v_buf,
    net,
    filt_pk,
    send_grad,
    grad_pk,
    modul,
    conv_buf,
    sems,
    net_sems,
    pk_out,
    extra,
    embed_w,
    vectors,
    *sum_scratch,
):
    n = axis_n
    me = lax.axis_index("seq")
    me_b = lax.axis_index("batch")
    pos, width = tok.shape
    rows = send_one.shape[1]
    fold = pos // rows
    step = 2 * chan
    second_len, double_pad, half = fwd.shape
    pad = double_pad // 2
    kept = half + 1
    f32, bf16 = jnp.float32, jnp.bfloat16

    seq_dests = shifted_all(me, n)
    pairs = batch_n // 2
    chip_dests = [
        (dest, lax.div(dest, pairs), 2 * lax.rem(dest, pairs) + lax.rem(me_b, 2))
        for dest in shifted_all(me * pairs + lax.div(me_b, 2), n * pairs)
    ]
    quarter = embed.shape[1]
    own_part = pl.ds(pl.multiple_of(me_b * quarter, LANES), quarter)
    loads = [
        pltpu.make_async_copy(src, dst, load_sems.at[i])
        for i, (src, dst) in enumerate(
            (
                (tok_hbm, tok),
                (inw_hbm, inw),
                (og_hbm, og),
                (outw_hbm, outw),
                (swap_hbm, swap),
                (embed_hbm.at[:, own_part], embed),
                (embed_raw_hbm, embed_raw),
                (embed_b_hbm, embed_b),
                (hidden_b_hbm, hidden_b),
                (freqs_hbm, freqs),
                (hidden_w_hbm, hidden_w),
                (filter_w_hbm, filter_w),
                (decay_hbm, decay_in),
                (skip_hbm, skip_in),
                (place_hbm, place),
                (fwd_hbm, fwd),
                (inner_hbm, inner),
                (outer_hbm, outer),
                (inv_hbm, inv),
                (gather_hbm, gather),
            )
        )
    ]
    for item in loads:
        item.start()
    barrier = pltpu.get_barrier_semaphore()
    other_core = [
        lax.rem(me_b + k, batch_n) for k in range(1, batch_n, 2)
    ]
    for seq, batch in [dest[1:] for dest in chip_dests] + [(me, peer) for peer in other_core]:
        pl.semaphore_signal(
            barrier, inc=1, device_id={"seq": seq, "batch": batch}, device_id_type=MESH
        )
    for item in loads[:4]:
        item.wait()

    proj = jnp.dot(tok[...], inw[...], preferred_element_type=f32)
    gate_out = proj[:, :width].astype(bf16)
    gate_in = proj[:, width : 2 * width].astype(bf16)
    values = proj[:, 2 * width :].astype(bf16)
    gated_grad = lax.dot_general(
        og[...], outw[...], (((1,), (1,)), ((), ())), preferred_element_type=f32
    ).astype(bf16)
    gates[0] = gate_out
    gates[1] = gate_in
    gates[2] = values
    gates[3] = gated_grad
    mixed = (values.astype(f32) * gate_in.astype(f32)).astype(bf16).astype(f32)
    grad = (gated_grad.astype(f32) * gate_out.astype(f32)).astype(bf16).astype(f32)

    lane = lax.broadcasted_iota(jnp.int32, (rows, LANES), 1)
    half_lanes = fold * chan
    parts = LANES // chan
    tiles = width // LANES
    dense = swap.shape[0] == parts * LANES
    loads[4].wait()
    if dense:
        for t in range(tiles):
            at = slice(t * LANES, (t + 1) * LANES)
            left = jnp.concatenate(
                [
                    source[j * rows : (j + 1) * rows, at].astype(bf16)
                    for source in (mixed, grad)
                    for j in range(fold)
                ],
                axis=1,
            )
            packed = jnp.dot(left, swap[...], preferred_element_type=f32).astype(bf16)
            for i in range(parts):
                send_one[t * parts + i] = packed[:, i * LANES : (i + 1) * LANES]
    for d in range(0 if dense else n):
        tile, off = (d * chan) // LANES * LANES, (d * chan) % LANES
        packed = None
        for i in range(2 * fold):
            source, j = (mixed, i) if i < fold else (grad, i - fold)
            part = lane_roll(source[j * rows : (j + 1) * rows, tile : tile + LANES], i * chan - off)
            packed = part if packed is None else jnp.where(lane >= i * chan, part, packed)
        send_one[d] = packed.astype(bf16)

    pl.semaphore_wait(barrier, len(chip_dests) + len(other_core))


    def copy(send, recv, which, k):
        dest = seq_dests[k - 1]
        return pltpu.make_async_remote_copy(
            src_ref=send.at[dest],
            dst_ref=recv.at[me],
            send_sem=sems.at[2 * which],
            recv_sem=sems.at[2 * which + 1],
            device_id={"seq": dest},
            device_id_type=MESH,
        )

    def wait_all(send, recv, which):
        others = pl.ds(0, n - 1)
        pltpu.make_async_remote_copy(
            src_ref=send.at[others],
            dst_ref=recv.at[others],
            send_sem=sems.at[2 * which],
            recv_sem=sems.at[2 * which + 1],
            device_id={"seq": me},
            device_id_type=MESH,
        ).wait()

    for k in range(1, n):
        copy(send_one, recv_one, 0, k).start()
    recv_one[me] = send_one[me]
    mixed = (gates[2].astype(f32) * gates[1].astype(f32)).astype(bf16).astype(f32)
    grad = (gates[3].astype(f32) * gates[0].astype(f32)).astype(bf16).astype(f32)
    bias_sum = jnp.sum(mixed * grad, axis=0, keepdims=True) * scale
    v_buf[...] = jnp.zeros_like(v_buf)
    extra[...] = jnp.zeros_like(extra)
    length = n * pos
    group = second_len + 1
    stride = double_pad + 1
    hid = hidden_w.shape[0]

    def select_own(value, target):
        lane_v = lax.broadcasted_iota(jnp.int32, (value.shape[0], LANES), 1)
        got = jnp.zeros((value.shape[0], LANES), f32)
        for i in range(n):
            tile, off = (i * chan) // LANES * LANES, (i * chan) % LANES
            part = lane_roll(value[:, tile : tile + LANES], target - off)
            got = jnp.where(jnp.logical_and(me == i, lane_v >= 0), part, got)
        return jnp.where((lane_v >= target) & (lane_v < target + chan), got, 0.0)

    sub = quarter // parts
    for item in loads[5:15]:
        item.wait()
    weight = select_own(filter_w[...], 0)
    decay_own = select_own(decay_in[...], 0)
    decay = decay_own
    for j in range(1, parts):
        decay = decay + lane_roll(decay_own, j * chan)
    skip_own = select_own(skip_in[...], chan)
    skip_other = select_own(skip_in[...], step)
    inputs = embed_raw.shape[0]
    embed_w[...] = jnp.zeros_like(embed_w)
    embed_w[0:inputs, :] = embed_raw[...]
    embed_w[inputs : inputs + 1, :] = embed_b[...]
    vectors[...] = jnp.zeros_like(vectors)
    vectors[0:2, :] = freqs[...]
    vectors[2:3, :] = hidden_b[...]
    eye = (
        lax.broadcasted_iota(jnp.int32, (8, 8), 0) == lax.broadcasted_iota(jnp.int32, (8, 8), 1)
    ).astype(f32)
    columns = dot_as(vectors[...], eye, (0, 0))
    freq_one, freq_two = columns[:, 0:1], columns[:, 1:2]
    tile = min(256, quarter)
    def net_forward(i, _):
        at = pl.ds(pl.multiple_of(i * tile, LANES), tile)
        pre_one = dot_as(embed_w[...], embed[:, at], (0, 0))
        act_one, cos_one = sine_cosine(freq_one * pre_one)
        pre_two = dot_as(hidden_w[...], act_one, (0, 0)) + columns[:, 2:3]
        act_two, cos_two = sine_cosine(freq_two * pre_two)
        net[0, :, at] = pre_one
        net[1, :, at] = act_one
        net[2, :, at] = cos_one
        net[3, :, at] = pre_two
        net[4, :, at] = act_two
        net[5, :, at] = cos_two
        return 0

    lax.fori_loop(0, quarter // tile, net_forward, 0, unroll=2 if quarter // tile % 2 == 0 else 1)
    lane_s = lax.broadcasted_iota(jnp.int32, (sub, LANES), 1)
    time = lax.broadcasted_iota(jnp.int32, (sub, LANES), 0) + me_b * quarter
    for j in range(1, parts):
        time = time + jnp.where(lane_s >= j * chan, sub, 0)
    modul[...] = jnp.exp(-decay * time.astype(f32)) * (4.0 / math.sqrt(length))
    packed_filt = jnp.zeros((sub, LANES), f32)
    for j in range(parts):
        packed_filt = packed_filt + dot_as(
            net[4, :, j * sub : (j + 1) * sub], lane_roll(weight, j * chan), (0, 0)
        )
    filt_pk[me_b] = (packed_filt * modul[...]).astype(bf16)

    def share(which, k):
        dest = lax.rem(me_b + k, batch_n)
        return pltpu.make_async_remote_copy(
            src_ref=filt_pk.at[me_b] if which == 0 else send_grad.at[dest],
            dst_ref=filt_pk.at[me_b] if which == 0 else grad_pk.at[me_b],
            send_sem=net_sems.at[2 * which],
            recv_sem=net_sems.at[2 * which + 1],
            device_id={"batch": dest},
            device_id_type=MESH,
        )

    def share_wait(which):
        others = pl.ds(0, batch_n - 1)
        pltpu.make_async_remote_copy(
            src_ref=grad_pk.at[others],
            dst_ref=grad_pk.at[others],
            send_sem=net_sems.at[2 * which],
            recv_sem=net_sems.at[2 * which + 1],
            device_id={"batch": me_b},
            device_id_type=MESH,
        ).wait()

    for k in range(1, batch_n):
        share(0, k).start()
    wait_all(send_one, recv_one, 0)
    share_wait(0)

    piece = min(rows, second_len)
    lane_p = lax.broadcasted_iota(jnp.int32, (piece, LANES), 1)

    def row_of(position):
        return position // second_len * group + position % second_len

    for block in range(n * fold if dense else 0):
        q, p = block // parts, block % parts
        both = jnp.concatenate([recv_one[block // fold], filt_pk[q]], axis=1)
        placed = jnp.dot(both, place[p], preferred_element_type=f32)
        for low in range(0, rows, piece):
            x_buf[pl.ds(row_of(block * rows + low), piece), :] = placed[low : low + piece]
    for s in range(0 if dense else n):
        for j in range(fold):
            for low in range(0, rows, piece):
                start = s * pos + j * rows + low
                q, rest = start // quarter, start % quarter
                p, row = rest // sub, rest % sub
                block = recv_one[s, low : low + piece, :].astype(f32)
                filt = filt_pk[q, row : row + piece, :].astype(f32)
                x_buf[pl.ds(row_of(start), piece), :] = jnp.where(
                    lane_p < chan,
                    lane_roll(block, -j * chan),
                    jnp.where(
                        lane_p < step,
                        lane_roll(filt, (1 - p) * chan),
                        jnp.where(
                            lane_p < step + chan,
                            lane_roll(block, step - half_lanes - j * chan),
                            lane_roll(block, (3 - j) * chan),
                        ),
                    ),
                )
    for item in loads[15:]:
        item.wait()

    def stage_one(n2, _):
        part = x_buf[pl.ds(n2, half, stride=group), :].astype(bf16)
        z_buf[pl.ds(n2 * stride, double_pad), :] = jnp.dot(
            fwd[n2], part, preferred_element_type=f32
        )
        return 0

    lax.fori_loop(0, second_len, stage_one, 0, unroll=32)

    lane_k = lax.broadcasted_iota(jnp.int32, (second_len, LANES), 1)
    own_sign = jnp.where((lane_k >= 3 * chan) & (lane_k < 4 * chan), -1.0, 1.0).astype(f32)
    other_sign = jnp.where((lane_k >= step) & (lane_k < 3 * chan), -1.0, 1.0).astype(f32)

    def stage_two(k1, _):
        stacked = jnp.concatenate(
            [
                z_buf[pl.ds(k1, second_len, stride=stride), :],
                z_buf[pl.ds(pad + k1, second_len, stride=stride), :],
            ],
            axis=0,
        ).astype(bf16)
        spec = jnp.dot(inner[...], stacked, preferred_element_type=f32)
        re, im = spec[:second_len], spec[second_len:]
        other_re = lane_roll(re, chan) + skip_other
        re = re + skip_own
        other_im = lane_roll(im, chan) * other_sign
        im = im * own_sign
        out = jnp.concatenate(
            [re * other_re - im * other_im, re * other_im + im * other_re], axis=0
        ).astype(bf16)
        back = jnp.dot(outer[...], out, preferred_element_type=f32)
        v_buf[pl.ds(k1, second_len, stride=stride), :] = back[:second_len]
        v_buf[pl.ds(pad + k1, second_len, stride=stride), :] = back[second_len:]
        return 0

    unroll = 33 if kept == 33 else 13 if kept % 13 == 0 else 3 if kept % 3 == 0 else 5 if kept % 5 == 0 else 1
    lax.fori_loop(0, kept, stage_two, 0, unroll=unroll)

    def stage_three(n2, _):
        part = v_buf[pl.ds(n2 * stride, double_pad), :].astype(bf16)
        y_out[pl.ds(n2, half, stride=group), :] = jnp.dot(
            inv[n2], part, preferred_element_type=f32
        )
        return 0

    lax.fori_loop(0, second_len, stage_three, 0, unroll=32)

    for q in range(batch_n if dense else 0):
        left = jnp.concatenate(
            [
                jnp.concatenate(
                    [
                        y_out[pl.ds(row_of((q * parts + p) * rows + low), piece), :]
                        for low in range(0, rows, piece)
                    ],
                    axis=0,
                ).astype(bf16)
                for p in range(parts)
            ],
            axis=1,
        )
        packed = jnp.dot(left, gather[...], preferred_element_type=f32).astype(bf16)
        send_two[2 * q] = packed[:, :LANES]
        send_two[2 * q + 1] = packed[:, LANES : 2 * LANES]
        send_grad[q] = packed[:, 2 * LANES :]
    for d in range(0 if dense else n):
        for low in range(0, rows, piece):
            packed = None
            for j in range(fold):
                at = pl.ds(row_of(d * pos + j * rows + low), piece)
                part = lane_roll(y_out[at, :], j * step - chan)
                packed = part if j == 0 else jnp.where(lane_p >= j * step, part, packed)
            send_two[d, low : low + piece, :] = packed.astype(bf16)
    for k in range(1, n):
        copy(send_two, recv_two, 1, k).start()
    recv_two[me] = send_two[me]

    small = min(sub, piece)
    lane_q = lax.broadcasted_iota(jnp.int32, (small, LANES), 1)
    for q in range(0 if dense else batch_n):
        for low in range(0, sub, small):
            packed = None
            for j in range(parts):
                at = pl.ds(row_of(q * quarter + j * sub + low), small)
                part = lane_roll(y_out[at, :], (j - 3) * chan)
                packed = part if j == 0 else jnp.where(lane_q >= j * chan, part, packed)
            send_grad[q, low : low + small, :] = packed.astype(bf16)
    for k in range(1, batch_n):
        share(1, k).start()
    grad_pk[me_b] = send_grad[me_b]
    share_wait(1)
    total = grad_pk[0].astype(f32)
    for q in range(1, batch_n):
        total = total + grad_pk[q].astype(f32)
    grad_kernel = total * modul[...]

    em = embed.shape[0]
    lane_w = lax.broadcasted_iota(jnp.int32, (hid, LANES), 1)
    grad_weight = jnp.zeros((hid, LANES), f32)
    for j in range(parts):
        at = slice(j * sub, (j + 1) * sub)
        got = dot_as(net[4, :, at], grad_kernel, (1, 0))
        grad_weight = grad_weight + lane_roll(
            jnp.where((lane_w >= j * chan) & (lane_w < (j + 1) * chan), got, 0.0), -j * chan
        )
        net[5, :, at] = dot_as(lane_roll(weight, j * chan), grad_kernel, (1, 1)) * net[5, :, at]

    def net_backward(i, carry):
        at = pl.ds(pl.multiple_of(i * tile, LANES), tile)
        grad_act_two = net[5, :, at]
        grad_pre_two = grad_act_two * freq_two
        grad_hidden = dot_as(net[1, :, at], grad_pre_two, (1, 1))
        grad_act_one = dot_as(hidden_w[...], grad_pre_two, (1, 0)) * net[2, :, at]
        grad_pre_one = grad_act_one * freq_one
        stacked = jnp.concatenate(
            [grad_pre_one, grad_pre_two, grad_act_one * net[0, :, at], grad_act_two * net[3, :, at]],
            axis=0,
        )
        return carry[0] + grad_hidden, carry[1] + dot_as(embed[:, at], stacked, (1, 1))

    zeros = lambda r, c: jnp.zeros((r, c), f32)
    both_sums = lax.fori_loop(
        0,
        quarter // tile,
        net_backward,
        (zeros(hid, hid), zeros(em, 4 * hid)),
        unroll=2 if quarter // tile % 2 == 0 else 1,
    )
    sums = (grad_weight, both_sums[0]) + tuple(
        both_sums[1][:, i * hid : (i + 1) * hid] for i in range(4)
    )
    sums = tuple(term * (scale * 0.25) for term in sums)
    lane_h = lax.broadcasted_iota(jnp.int32, (hid, LANES), 1)
    for tile in range(tiles):
        placed = zeros(hid, LANES)
        for i in range(n):
            if (i * chan) // LANES == tile:
                off = (i * chan) % LANES
                mask = (lane_h >= off) & (lane_h < off + chan) & (me == i)
                placed = jnp.where(mask, lane_roll(sums[0], off), placed)
        extra[tile * hid : (tile + 1) * hid, :] = placed
    base = tiles * hid
    extra[base : base + hid, 0:hid] = sums[1]
    base += hid
    for term in sums[2:]:
        extra[base : base + em, 0:hid] = term
        base += em
    for tile in range(tiles):
        extra[base + tile : base + tile + 1, :] = bias_sum[:, tile * LANES : (tile + 1) * LANES]

    main_scratch, extra_scratch = sum_scratch[:5], sum_scratch[5:]
    blocks = main_scratch[1].shape[0]
    stream = [pair_sum(n, batch_n, pk_out, main_scratch, b, chip_dests) for b in range(blocks)]
    extra_sum = pair_sum(n, batch_n, extra, extra_scratch, 0, chip_dests)
    extra_sum.start_pair()
    wait_all(send_two, recv_two, 1)

    per_tile = LANES // chan
    for t in range(tiles if dense else 0):
        at = slice(t * LANES, (t + 1) * LANES)
        left = jnp.concatenate([recv_two[t * parts + i] for i in range(parts)], axis=1)
        back = jnp.dot(left, swap[...], preferred_element_type=f32)
        for u in range(parts):
            j = u % fold
            conv_buf[u // fold, j * rows : (j + 1) * rows, at] = back[:, u * LANES : (u + 1) * LANES]
    for tile in range(0 if dense else width // LANES):
        for j in range(fold):
            conv_acc = jnp.zeros((rows, LANES), f32)
            grad_acc = jnp.zeros((rows, LANES), f32)
            for i in range(per_tile):
                block = recv_two[tile * per_tile + i].astype(f32)
                own = (lane >= i * chan) & (lane < (i + 1) * chan)
                conv_acc = jnp.where(own, lane_roll(block, i * chan - j * step), conv_acc)
                grad_acc = jnp.where(own, lane_roll(block, i * chan - j * step - chan), grad_acc)
            at = pl.ds(j * rows, rows)
            conv_buf[0, at, tile * LANES : (tile + 1) * LANES] = conv_acc
            conv_buf[1, at, tile * LANES : (tile + 1) * LANES] = grad_acc

    conv = conv_buf[0]
    grad_mixed = conv_buf[1]
    gated = (gates[0].astype(f32) * conv).astype(bf16)
    grad_proj = jnp.concatenate(
        [
            (gates[3].astype(f32) * conv).astype(bf16),
            (grad_mixed * gates[2].astype(f32)).astype(bf16),
            (grad_mixed * gates[1].astype(f32)).astype(bf16),
        ],
        axis=1,
    )
    first = (((0,), (0,)), ((), ()))
    pieces = [(gated, og[...])] + [
        (tok[...], grad_proj[:, j * width : (j + 1) * width]) for j in range(3)
    ]
    per_block = len(pieces) // blocks if blocks > 1 else len(pieces)
    for i, (left, right) in enumerate(pieces):
        block = lax.dot_general(left, right, first, preferred_element_type=f32) * scale
        for j in range(tiles):
            at = (i * tiles + j) * width
            pk_out[at : at + width, :] = block[:, j * LANES : (j + 1) * LANES].astype(bf16)
        if (i + 1) % per_block == 0:
            done = (i + 1) // per_block - 1
            stream[done].start_pair()
            if done == 0:
                extra_sum.finish_pair()
                extra_sum.start_scatter()
            else:
                stream[done - 1].finish_pair()
                stream[done - 1].start_scatter()
    stream[-1].finish_pair()
    stream[-1].start_scatter()
    extra_sum.finish_scatter()
    extra_sum.start_gather()
    gt_out[...] = lax.dot_general(
        grad_proj, inw[...], (((1,), (1,)), ((), ())), preferred_element_type=f32
    ).astype(bf16)
    outs = [pltpu.make_async_copy(gt_out, gt_hbm, out_sems.at[0, 0])]
    outs[0].start()
    for item in stream:
        item.finish_scatter()
        item.start_gather()
    extra_sum.finish_gather()
    extra_sum.start_swap()

    def finish(i, item):
        target, base = (b_hbm, 0) if i == 0 else (a_hbm, (i - 1) * item.size)
        for side in range(2):
            core = item.core if side == 0 else 1 - item.core
            at = item.rows(core * item.half, item.half)
            to = item.rows(base + core * item.half, item.half)
            outs.append(
                pltpu.make_async_copy(item.whole.at[at], target.at[to], out_sems.at[1 + i, side])
            )
            if side == 1:
                item.finish_swap()
            outs[-1].start()

    finish(0, extra_sum)
    for item in stream:
        item.finish_gather()
        item.start_swap()
    for i, item in enumerate(stream):
        finish(1 + i, item)
    for item in outs:
        item.wait()


def digits_of(count):
    radices = []
    while count % 2 == 0 and count > 4 and len(radices) < 2:
        radices.append(2)
        count = count // 2
    return [count] + radices


def far_first(count):
    radices = digits_of(count)
    moves = [()]
    for radix in radices:
        moves = [m + (d,) for m in moves for d in range(radix)]
    moves = [m for m in moves if any(m)]
    return sorted(moves, key=lambda m: -2 * min(m[0], radices[0] - m[0]) - sum(m[1:]))


def shifted_all(own, count):
    radices = digits_of(count)
    below, tables = count, []
    for radix in radices:
        below = below // radix
        digit = lax.rem(lax.div(own, below), radix)
        tables.append([lax.rem(digit + step, radix) * below for step in range(radix)])
    made = []
    for move in far_first(count):
        total = tables[0][move[0]]
        for table, step in zip(tables[1:], move[1:]):
            total = total + table[step]
        made.append(total)
    return made


class pair_sum:
    def __init__(self, ns, nb, src, scratch, block, dests):
        self.dests = dests
        got_pair, part, got, whole, sems = (ref.at[block] for ref in scratch)
        self.got_pair, self.part, self.got, self.whole, self.sems = got_pair, part, got, whole, sems
        self.src, self.pairs = src, nb // 2
        me_s, me_b = lax.axis_index("seq"), lax.axis_index("batch")
        self.core = lax.rem(me_b, 2)
        self.chips = ns * self.pairs
        self.own = me_s * self.pairs + lax.div(me_b, 2)
        self.partner = me_b + 1 - 2 * self.core
        self.half = part.shape[0]
        self.size = 2 * self.half
        self.base = block * self.size
        self.unit = self.half // self.chips

    def rows(self, start, size):
        return pl.ds(pl.multiple_of(start, self.unit), size)

    def to_partner(self, which):
        if which == 0:
            src = self.src.at[self.rows(self.base + (1 - self.core) * self.half, self.half)]
            dst = self.got_pair
        else:
            src = dst = self.whole.at[self.rows(self.core * self.half, self.half)]
        return pltpu.make_async_remote_copy(
            src_ref=src,
            dst_ref=dst,
            send_sem=self.sems.at[which, 0, 0],
            recv_sem=self.sems.at[which, 1, 0],
            device_id={"batch": self.partner},
            device_id_type=MESH,
        )

    def to_chips(self, which):
        made = []
        for i, (dest, seq, batch) in enumerate(self.dests):
            if which == 0:
                src = self.part.at[self.rows(dest * self.unit, self.unit)]
                dst = self.got.at[i]
            else:
                at = self.rows(self.core * self.half + self.own * self.unit, self.unit)
                src = dst = self.whole.at[at]
            made.append(
                pltpu.make_async_remote_copy(
                    src_ref=src,
                    dst_ref=dst,
                    send_sem=self.sems.at[which, 0, 1],
                    recv_sem=self.sems.at[which, 1, 1],
                    device_id={"seq": seq, "batch": batch},
                    device_id_type=MESH,
                )
            )
        return made

    def wait_chips(self, which):
        pltpu.make_async_remote_copy(
            src_ref=self.got,
            dst_ref=self.got,
            send_sem=self.sems.at[which, 0, 1],
            recv_sem=self.sems.at[which, 1, 1],
            device_id={"batch": self.partner},
            device_id_type=MESH,
        ).wait()

    def start_pair(self):
        self.to_partner(0).start()

    def finish_pair(self):
        self.to_partner(0).wait()
        mine = self.src[self.rows(self.base + self.core * self.half, self.half), :]
        total = mine.astype(jnp.float32) + self.got_pair[...].astype(jnp.float32)
        self.part[...] = total.astype(self.part.dtype)

    def start_scatter(self):
        for item in self.to_chips(0):
            item.start()

    def finish_scatter(self):
        self.wait_chips(0)
        total = self.part[self.rows(self.own * self.unit, self.unit), :].astype(jnp.float32)
        for k in range(1, self.chips):
            total = total + self.got[k - 1].astype(jnp.float32)
        at = self.rows(self.core * self.half + self.own * self.unit, self.unit)
        self.whole[at, :] = total.astype(self.whole.dtype)

    def start_gather(self):
        for item in self.to_chips(1):
            item.start()

    def finish_gather(self):
        self.wait_chips(1)

    def start_swap(self):
        self.to_partner(1).start()

    def finish_swap(self):
        self.to_partner(1).wait()


def unpack_kernel(main, extra, tokens_in, tokens_out, g_in, g_out, skip, emb, emb_b, hidden, hidden_b, filt, freq):
    width = g_out.shape[0]
    hid = hidden.shape[0]
    tokens_out[...] = tokens_in[...]
    at = 0
    for ref in (g_out, g_in):
        for j in range(ref.shape[1] // LANES):
            ref[:, j * LANES : (j + 1) * LANES] = main[at : at + width, :].astype(jnp.float32)
            at += width
    tiles = width // LANES
    for j in range(tiles):
        filt[:, j * LANES : (j + 1) * LANES] = extra[j * hid : (j + 1) * hid, :]
    base = tiles * hid
    hidden[...] = extra[base : base + hid, 0:hid]
    base += hid
    count = emb.shape[0]
    em = -(-(count + 1) // 8) * 8
    emb[...] = extra[base : base + count, 0:hid]
    emb_b[...] = extra[base + count : base + count + 1, 0:hid]
    hidden_b[...] = extra[base + em + count : base + em + count + 1, 0:hid]
    freq[0:1, :] = extra[base + 2 * em + count : base + 2 * em + count + 1, 0:hid]
    freq[1:2, :] = extra[base + 3 * em + count : base + 3 * em + count + 1, 0:hid]
    base += 4 * em
    for j in range(tiles):
        skip[:, j * LANES : (j + 1) * LANES] = extra[base + j : base + j + 1, :]


def vmem(count):
    return [pl.BlockSpec(memory_space=pltpu.VMEM)] * count


def sine_cosine(angle):
    turns = jnp.round(angle * (1.0 / (2.0 * math.pi)))
    reduced = angle - turns * 6.28125
    reduced = reduced - turns * 0.0019350051879882812
    reduced = reduced - turns * 3.0199157663146e-07
    half = reduced * 0.5
    square = half * half
    sin = half * (
        1.0
        + square
        * (-1.0 / 6 + square * (1.0 / 120 + square * (-1.0 / 5040 + square * (1.0 / 362880 - square / 39916800.0))))
    )
    cos = 1.0 + square * (
        -0.5
        + square
        * (1.0 / 24 + square * (-1.0 / 720 + square * (1.0 / 40320 + square * (-1.0 / 3628800 + square / 479001600.0))))
    )
    return 2.0 * sin * cos, 1.0 - 2.0 * sin * sin


def embedding(length, count):
    rows = np.zeros((-(-(count + 1) // 8) * 8, length), np.float32)
    scaled = np.arange(length) / length
    rows[0] = scaled
    for band_index in range(1, (count - 1) // 2 + 1):
        rows[2 * band_index - 1] = np.cos(2.0 * np.pi * band_index * scaled)
        rows[2 * band_index] = np.sin(2.0 * np.pi * band_index * scaled)
    rows[count] = 1.0
    return jnp.asarray(rows)


def shards(
    tokens,
    out_grad,
    in_weight,
    out_weight,
    skip_bias,
    embed_weight,
    embed_bias,
    hidden_weight,
    hidden_bias,
    filter_weight,
    sine_freq,
    decay_rate,
):
    f32, bf16 = jnp.float32, jnp.bfloat16
    tok, og = tokens[0], out_grad[0]
    pos, width = tok.shape
    ns, nb = lax.axis_size("seq"), lax.axis_size("batch")
    length = pos * ns
    chan = width // ns
    hid = hidden_weight.shape[0]
    count = embed_weight.shape[0]
    embed = embedding(length, count)
    em = embed.shape[0]

    fwd, inv, inner, outer = make_tables(length)
    second_len, double_pad, half = fwd.shape
    rows = pos // (LANES // (2 * chan))
    tiles = width // LANES
    parts = LANES // chan
    chips = ns * (nb // 2)
    unit = 2 * chips * 16
    main_rows = -(-4 * width * tiles // unit) * unit
    blocks = max(b for b in BLOCKS if main_rows % (b * unit) == 0)
    unit = 2 * chips * 8
    extra_rows = -(-(tiles * hid + hid + 4 * em + tiles) // unit) * unit
    swap, place, gather = selections(
        chan, second_len <= rows and nb * parts * rows == length and parts * LANES <= 512
    )
    pair = (ns, rows, LANES)
    shared = (nb, length // nb // (LANES // chan), LANES)
    spectral = (second_len * (double_pad + 1), LANES)
    spaced = (half * (second_len + 1), LANES)
    scratch = []
    for total, kind, count_at in ((main_rows, bf16, blocks), (extra_rows, f32, 1)):
        half_rows = total // count_at // 2
        scratch += [
            pltpu.VMEM((count_at, half_rows, LANES), kind),
            pltpu.VMEM((count_at, half_rows, LANES), kind),
            pltpu.VMEM((count_at, chips - 1, half_rows // chips, LANES), kind),
            pltpu.VMEM((count_at, 2 * half_rows, LANES), kind),
            pltpu.SemaphoreType.DMA((count_at, 2, 2, 2)),
        ]
    grad_tokens, main, extra = pl.pallas_call(
        functools.partial(step_kernel, ns, nb, chan, 1.0 / math.sqrt(nb * length)),
        out_shape=(
            jax.ShapeDtypeStruct((pos, width), bf16),
            jax.ShapeDtypeStruct((main_rows, LANES), bf16),
            jax.ShapeDtypeStruct((extra_rows, LANES), f32),
        ),
        in_specs=[pl.BlockSpec(memory_space=pl.ANY)] * 20,
        out_specs=(pl.BlockSpec(memory_space=pl.ANY),) * 3,
        scratch_shapes=[
            pltpu.VMEM((pos, width), bf16),
            pltpu.SemaphoreType.DMA((2 + blocks, 2)),
            pltpu.VMEM(tok.shape, bf16),
            pltpu.VMEM(og.shape, bf16),
            pltpu.VMEM(in_weight.shape, bf16),
            pltpu.VMEM(out_weight.shape, bf16),
            pltpu.VMEM((em, length // nb), f32),
            pltpu.VMEM(fwd.shape, bf16),
            pltpu.VMEM(inv.shape, bf16),
            pltpu.VMEM(inner.shape, bf16),
            pltpu.VMEM(outer.shape, bf16),
            pltpu.VMEM(embed_weight.shape, f32),
            pltpu.VMEM((1, hid), f32),
            pltpu.VMEM((1, hid), f32),
            pltpu.VMEM(sine_freq.shape, f32),
            pltpu.VMEM(hidden_weight.shape, f32),
            pltpu.VMEM(filter_weight.shape, f32),
            pltpu.VMEM((1, width), f32),
            pltpu.VMEM((1, width), f32),
            pltpu.VMEM(swap.shape, bf16),
            pltpu.VMEM(place.shape, bf16),
            pltpu.VMEM(gather.shape, bf16),
            pltpu.SemaphoreType.DMA((20,)),
            pltpu.VMEM(pair, bf16),
            pltpu.VMEM(pair, bf16),
            pltpu.VMEM(pair, bf16),
            pltpu.VMEM(pair, bf16),
            pltpu.VMEM((4, pos, width), bf16),
            pltpu.VMEM(spaced, f32),
            pltpu.VMEM(spaced, f32),
            pltpu.VMEM(spectral, f32),
            pltpu.VMEM(spectral, f32),
            pltpu.VMEM((6, hid, length // nb), f32),
            pltpu.VMEM(shared, bf16),
            pltpu.VMEM(shared, bf16),
            pltpu.VMEM(shared, bf16),
            pltpu.VMEM(shared[1:], f32),
            pltpu.VMEM((2, pos, width), f32),
            pltpu.SemaphoreType.DMA((4,)),
            pltpu.SemaphoreType.DMA((4,)),
            pltpu.VMEM((main_rows, LANES), bf16),
            pltpu.VMEM((extra_rows, LANES), f32),
            pltpu.VMEM((em, hid), f32),
            pltpu.VMEM((8, hid), f32),
        ]
        + scratch,
        compiler_params=pltpu.CompilerParams(
            collective_id=0, has_side_effects=True, vmem_limit_bytes=VMEM_BYTES
        ),
        name="step",
    )(
        tok,
        og,
        in_weight,
        out_weight,
        embed,
        fwd,
        inv,
        inner,
        outer,
        embed_weight,
        embed_bias[None],
        hidden_bias[None],
        sine_freq,
        hidden_weight,
        filter_weight,
        decay_rate[None],
        skip_bias[None],
        swap,
        place,
        gather,
    )

    shapes = (
        (width, 3 * width),
        (width, width),
        (1, width),
        (count, hid),
        (1, hid),
        (hid, hid),
        (1, hid),
        (hid, width),
        (2, hid),
    )
    out = pl.pallas_call(
        unpack_kernel,
        out_shape=(jax.ShapeDtypeStruct((pos, width), bf16),)
        + tuple(jax.ShapeDtypeStruct(shape, f32) for shape in shapes),
        in_specs=vmem(3),
        out_specs=tuple(vmem(1 + len(shapes))),
        name="unpack",
    )(main, extra, grad_tokens)
    return (
        out[0][None],
        out[1],
        out[2],
        out[3][0],
        out[4],
        out[5][0],
        out[6],
        out[7][0],
        out[8],
        out[9],
    )


def solution(mesh):
    batched = P("batch", "seq", None)
    return jax.shard_map(
        shards,
        mesh=mesh,
        in_specs=(batched, batched) + (P(),) * 10,
        out_specs=(batched,) + (P(),) * 9,
        check_vma=False,
    )
```

```python
import functools
import math

import jax
import jax.numpy as jnp
import numpy as np
from jax import lax
from jax.experimental import pallas as pl
from jax.experimental.pallas import tpu as pltpu
from jax.sharding import PartitionSpec as P

highest = lax.Precision.HIGHEST
MESH = pl.DeviceIdType.MESH
LANES = 128
BLOCKS = (1, 2)
VMEM_BYTES = 66 * 1000 * 1000


def factor(length):
    total = 2 * length
    first_len = 2
    while first_len * first_len < total and total % (2 * first_len) == 0:
        first_len = first_len * 2
    return first_len, total // first_len


def make_tables(length):
    total = 2 * length
    first_len, second_len = factor(length)
    half = first_len // 2
    kept = half + 1
    pad = -(-kept // 8) * 8
    k1 = np.arange(kept)[None, :, None]
    n1 = np.arange(half)[None, None, :]
    n2 = np.arange(second_len)[:, None, None]
    angle = 2.0 * np.pi * ((k1 * (n1 * second_len + n2)) % total) / total
    fwd = np.zeros((second_len, 2 * pad, half), np.float32)
    fwd[:, :kept] = np.cos(angle)
    fwd[:, pad : pad + kept] = -np.sin(angle)
    weight = np.where((k1 == 0) | (k1 == half), 1.0, 2.0) / total
    inv = np.zeros((second_len, half, 2 * pad), np.float32)
    inv[:, :, :kept] = np.swapaxes(weight * np.cos(angle), 1, 2)
    inv[:, :, pad : pad + kept] = np.swapaxes(-weight * np.sin(angle), 1, 2)
    index = np.arange(second_len)
    small = 2.0 * np.pi * ((index[:, None] * index[None, :]) % second_len) / second_len
    cos, sin = np.cos(small), np.sin(small)
    inner = np.block([[cos, sin], [-sin, cos]])
    outer = np.block([[cos, -sin], [sin, cos]])
    return tuple(jnp.asarray(t, jnp.bfloat16) for t in (fwd, inv, inner, outer))


def selections(chan, dense):
    parts = LANES // chan
    fold = parts // 2
    if not dense:
        return tuple(jnp.zeros(s, jnp.bfloat16) for s in ((16, LANES), (1, 16, LANES), (16, LANES)))
    swap = np.zeros((parts * LANES, parts * LANES), np.float32)
    place = np.zeros((parts, 2 * LANES, LANES), np.float32)
    gather = np.zeros((parts * LANES, 3 * LANES), np.float32)
    c = np.arange(chan)
    for i in range(parts):
        for u in range(parts):
            swap[u * LANES + i * chan + c, i * LANES + u * chan + c] = 1.0
    for p in range(parts):
        e, j = p // fold, p % fold
        place[p, j * chan + c, c] = 1.0
        place[p, j * chan + c, 3 * chan + c] = 1.0
        place[p, (fold + j) * chan + c, 2 * chan + c] = 1.0
        place[p, LANES + p * chan + c, chan + c] = 1.0
        gather[p * LANES + chan + c, e * LANES + j * chan + c] = 1.0
        gather[p * LANES + 2 * chan + c, e * LANES + (fold + j) * chan + c] = 1.0
        gather[p * LANES + 3 * chan + c, 2 * LANES + p * chan + c] = 1.0
    return tuple(jnp.asarray(t, jnp.bfloat16) for t in (swap, place, gather))


def lane_roll(value, shift):
    shift = shift % LANES
    return value if shift == 0 else pltpu.roll(value, shift, 1)


def dot_as(left, right, dims):
    return lax.dot_general(
        left,
        right,
        ((dims[:1], dims[1:]), ((), ())),
        precision=highest,
        preferred_element_type=jnp.float32,
    )


def step_kernel(
    axis_n,
    batch_n,
    chan,
    scale,
    tok_hbm,
    og_hbm,
    inw_hbm,
    outw_hbm,
    embed_hbm,
    fwd_hbm,
    inv_hbm,
    inner_hbm,
    outer_hbm,
    embed_raw_hbm,
    embed_b_hbm,
    hidden_b_hbm,
    freqs_hbm,
    hidden_w_hbm,
    filter_w_hbm,
    decay_hbm,
    skip_hbm,
    swap_hbm,
    place_hbm,
    gather_hbm,
    gt_hbm,
    a_hbm,
    b_hbm,
    gt_out,
    tok_t,
    out_sems,
    tok,
    og,
    inw,
    outw,
    embed,
    fwd,
    inv,
    inner,
    outer,
    embed_raw,
    embed_b,
    hidden_b,
    freqs,
    hidden_w,
    filter_w,
    decay_in,
    skip_in,
    swap,
    place,
    gather,
    load_sems,
    send_one,
    recv_one,
    send_two,
    recv_two,
    gates,
    x_buf,
    y_out,
    z_buf,
    v_buf,
    net,
    filt_pk,
    send_grad,
    grad_pk,
    modul,
    conv_buf,
    sems,
    net_sems,
    pk_out,
    extra,
    embed_w,
    vectors,
    *sum_scratch,
):
    n = axis_n
    me = lax.axis_index("seq")
    me_b = lax.axis_index("batch")
    pos, width = tok.shape
    rows = send_one.shape[1]
    fold = pos // rows
    step = 2 * chan
    second_len, double_pad, half = fwd.shape
    pad = double_pad // 2
    kept = half + 1
    f32, bf16 = jnp.float32, jnp.bfloat16

    seq_dests = shifted_all(me, n)
    pairs = batch_n // 2
    chip_dests = [
        (dest, lax.div(dest, pairs), 2 * lax.rem(dest, pairs) + lax.rem(me_b, 2))
        for dest in shifted_all(me * pairs + lax.div(me_b, 2), n * pairs)
    ]
    quarter = embed.shape[1]
    own_part = pl.ds(pl.multiple_of(me_b * quarter, LANES), quarter)
    loads = [
        pltpu.make_async_copy(src, dst, load_sems.at[i])
        for i, (src, dst) in enumerate(
            (
                (tok_hbm, tok),
                (inw_hbm, inw),
                (og_hbm, og),
                (outw_hbm, outw),
                (swap_hbm, swap),
                (embed_hbm.at[:, own_part], embed),
                (embed_raw_hbm, embed_raw),
                (embed_b_hbm, embed_b),
                (hidden_b_hbm, hidden_b),
                (freqs_hbm, freqs),
                (hidden_w_hbm, hidden_w),
                (filter_w_hbm, filter_w),
                (decay_hbm, decay_in),
                (skip_hbm, skip_in),
                (place_hbm, place),
                (fwd_hbm, fwd),
                (inner_hbm, inner),
                (outer_hbm, outer),
                (inv_hbm, inv),
                (gather_hbm, gather),
            )
        )
    ]
    for item in loads:
        item.start()
    barrier = pltpu.get_barrier_semaphore()
    other_core = [
        lax.rem(me_b + k, batch_n) for k in range(1, batch_n, 2)
    ]
    for seq, batch in [dest[1:] for dest in chip_dests] + [(me, peer) for peer in other_core]:
        pl.semaphore_signal(
            barrier, inc=1, device_id={"seq": seq, "batch": batch}, device_id_type=MESH
        )
    for item in loads[:2]:
        item.wait()

    proj = jnp.dot(tok[...], inw[...], preferred_element_type=f32)
    gate_out = proj[:, :width].astype(bf16)
    gate_in = proj[:, width : 2 * width].astype(bf16)
    values = proj[:, 2 * width :].astype(bf16)
    for item in loads[2:4]:
        item.wait()
    gated_grad = lax.dot_general(
        og[...], outw[...], (((1,), (1,)), ((), ())), preferred_element_type=f32
    ).astype(bf16)
    gates[0] = gate_out
    gates[1] = gate_in
    gates[2] = values
    gates[3] = gated_grad
    mixed = (values.astype(f32) * gate_in.astype(f32)).astype(bf16).astype(f32)
    grad = (gated_grad.astype(f32) * gate_out.astype(f32)).astype(bf16).astype(f32)

    lane = lax.broadcasted_iota(jnp.int32, (rows, LANES), 1)
    half_lanes = fold * chan
    parts = LANES // chan
    tiles = width // LANES
    dense = swap.shape[0] == parts * LANES
    loads[4].wait()
    if dense:
        for t in range(tiles):
            at = slice(t * LANES, (t + 1) * LANES)
            left = jnp.concatenate(
                [
                    source[j * rows : (j + 1) * rows, at].astype(bf16)
                    for source in (mixed, grad)
                    for j in range(fold)
                ],
                axis=1,
            )
            packed = jnp.dot(left, swap[...], preferred_element_type=f32).astype(bf16)
            for i in range(parts):
                send_one[t * parts + i] = packed[:, i * LANES : (i + 1) * LANES]
    for d in range(0 if dense else n):
        tile, off = (d * chan) // LANES * LANES, (d * chan) % LANES
        packed = None
        for i in range(2 * fold):
            source, j = (mixed, i) if i < fold else (grad, i - fold)
            part = lane_roll(source[j * rows : (j + 1) * rows, tile : tile + LANES], i * chan - off)
            packed = part if packed is None else jnp.where(lane >= i * chan, part, packed)
        send_one[d] = packed.astype(bf16)

    pl.semaphore_wait(barrier, len(chip_dests) + len(other_core))


    def copy(send, recv, which, k):
        dest = seq_dests[k - 1]
        return pltpu.make_async_remote_copy(
            src_ref=send.at[dest],
            dst_ref=recv.at[me],
            send_sem=sems.at[2 * which],
            recv_sem=sems.at[2 * which + 1],
            device_id={"seq": dest},
            device_id_type=MESH,
        )

    def wait_all(send, recv, which):
        others = pl.ds(0, n - 1)
        pltpu.make_async_remote_copy(
            src_ref=send.at[others],
            dst_ref=recv.at[others],
            send_sem=sems.at[2 * which],
            recv_sem=sems.at[2 * which + 1],
            device_id={"seq": me},
            device_id_type=MESH,
        ).wait()

    for k in range(1, n):
        copy(send_one, recv_one, 0, k).start()
    recv_one[me] = send_one[me]
    tok_t[...] = tok[...].T
    mixed = (gates[2].astype(f32) * gates[1].astype(f32)).astype(bf16).astype(f32)
    grad = (gates[3].astype(f32) * gates[0].astype(f32)).astype(bf16).astype(f32)
    bias_sum = jnp.sum(mixed * grad, axis=0, keepdims=True) * scale
    v_buf[...] = jnp.zeros_like(v_buf)
    extra[...] = jnp.zeros_like(extra)
    length = n * pos
    group = second_len + 1
    stride = double_pad + 1
    hid = hidden_w.shape[0]

    def select_own(value, target):
        lane_v = lax.broadcasted_iota(jnp.int32, (value.shape[0], LANES), 1)
        got = jnp.zeros((value.shape[0], LANES), f32)
        for i in range(n):
            tile, off = (i * chan) // LANES * LANES, (i * chan) % LANES
            part = lane_roll(value[:, tile : tile + LANES], target - off)
            got = jnp.where(jnp.logical_and(me == i, lane_v >= 0), part, got)
        return jnp.where((lane_v >= target) & (lane_v < target + chan), got, 0.0)

    sub = quarter // parts
    for item in loads[5:15]:
        item.wait()
    weight = select_own(filter_w[...], 0)
    decay_own = select_own(decay_in[...], 0)
    decay = decay_own
    for j in range(1, parts):
        decay = decay + lane_roll(decay_own, j * chan)
    skip_own = select_own(skip_in[...], chan)
    skip_other = select_own(skip_in[...], step)
    inputs = embed_raw.shape[0]
    embed_w[...] = jnp.zeros_like(embed_w)
    embed_w[0:inputs, :] = embed_raw[...]
    embed_w[inputs : inputs + 1, :] = embed_b[...]
    vectors[...] = jnp.zeros_like(vectors)
    vectors[0:2, :] = freqs[...]
    vectors[2:3, :] = hidden_b[...]
    eye = (
        lax.broadcasted_iota(jnp.int32, (8, 8), 0) == lax.broadcasted_iota(jnp.int32, (8, 8), 1)
    ).astype(f32)
    columns = dot_as(vectors[...], eye, (0, 0))
    freq_one, freq_two = columns[:, 0:1], columns[:, 1:2]
    tile = min(256, quarter)
    def net_forward(i, _):
        at = pl.ds(pl.multiple_of(i * tile, LANES), tile)
        pre_one = dot_as(embed_w[...], embed[:, at], (0, 0))
        act_one, cos_one = sine_cosine(freq_one * pre_one)
        pre_two = dot_as(hidden_w[...], act_one, (0, 0)) + columns[:, 2:3]
        act_two, cos_two = sine_cosine(freq_two * pre_two)
        net[0, :, at] = pre_one
        net[1, :, at] = act_one
        net[2, :, at] = cos_one
        net[3, :, at] = pre_two
        net[4, :, at] = act_two
        net[5, :, at] = cos_two
        return 0

    lax.fori_loop(0, quarter // tile, net_forward, 0, unroll=2 if quarter // tile % 2 == 0 else 1)
    lane_s = lax.broadcasted_iota(jnp.int32, (sub, LANES), 1)
    time = lax.broadcasted_iota(jnp.int32, (sub, LANES), 0) + me_b * quarter
    for j in range(1, parts):
        time = time + jnp.where(lane_s >= j * chan, sub, 0)
    modul[...] = jnp.exp(-decay * time.astype(f32)) * (4.0 / math.sqrt(length))
    packed_filt = jnp.zeros((sub, LANES), f32)
    for j in range(parts):
        packed_filt = packed_filt + dot_as(
            net[4, :, j * sub : (j + 1) * sub], lane_roll(weight, j * chan), (0, 0)
        )
    filt_pk[me_b] = (packed_filt * modul[...]).astype(bf16)

    def share(which, k):
        dest = lax.rem(me_b + k, batch_n)
        return pltpu.make_async_remote_copy(
            src_ref=filt_pk.at[me_b] if which == 0 else send_grad.at[dest],
            dst_ref=filt_pk.at[me_b] if which == 0 else grad_pk.at[me_b],
            send_sem=net_sems.at[2 * which],
            recv_sem=net_sems.at[2 * which + 1],
            device_id={"batch": dest},
            device_id_type=MESH,
        )

    def share_wait(which):
        others = pl.ds(0, batch_n - 1)
        pltpu.make_async_remote_copy(
            src_ref=grad_pk.at[others],
            dst_ref=grad_pk.at[others],
            send_sem=net_sems.at[2 * which],
            recv_sem=net_sems.at[2 * which + 1],
            device_id={"batch": me_b},
            device_id_type=MESH,
        ).wait()

    for k in range(1, batch_n):
        share(0, k).start()
    wait_all(send_one, recv_one, 0)
    share_wait(0)

    piece = min(rows, second_len)
    lane_p = lax.broadcasted_iota(jnp.int32, (piece, LANES), 1)

    def row_of(position):
        return position // second_len * group + position % second_len

    for block in range(n * fold if dense else 0):
        q, p = block // parts, block % parts
        both = jnp.concatenate([recv_one[block // fold], filt_pk[q]], axis=1)
        placed = jnp.dot(both, place[p], preferred_element_type=f32)
        for low in range(0, rows, piece):
            x_buf[pl.ds(row_of(block * rows + low), piece), :] = placed[low : low + piece]
    for s in range(0 if dense else n):
        for j in range(fold):
            for low in range(0, rows, piece):
                start = s * pos + j * rows + low
                q, rest = start // quarter, start % quarter
                p, row = rest // sub, rest % sub
                block = recv_one[s, low : low + piece, :].astype(f32)
                filt = filt_pk[q, row : row + piece, :].astype(f32)
                x_buf[pl.ds(row_of(start), piece), :] = jnp.where(
                    lane_p < chan,
                    lane_roll(block, -j * chan),
                    jnp.where(
                        lane_p < step,
                        lane_roll(filt, (1 - p) * chan),
                        jnp.where(
                            lane_p < step + chan,
                            lane_roll(block, step - half_lanes - j * chan),
                            lane_roll(block, (3 - j) * chan),
                        ),
                    ),
                )
    for item in loads[15:]:
        item.wait()

    def stage_one(n2, _):
        part = x_buf[pl.ds(n2, half, stride=group), :].astype(bf16)
        z_buf[pl.ds(n2 * stride, double_pad), :] = jnp.dot(
            fwd[n2], part, preferred_element_type=f32
        )
        return 0

    lax.fori_loop(0, second_len, stage_one, 0, unroll=32)

    lane_k = lax.broadcasted_iota(jnp.int32, (second_len, LANES), 1)
    own_sign = jnp.where((lane_k >= 3 * chan) & (lane_k < 4 * chan), -1.0, 1.0).astype(f32)
    other_sign = jnp.where((lane_k >= step) & (lane_k < 3 * chan), -1.0, 1.0).astype(f32)

    def stage_two(k1, _):
        stacked = jnp.concatenate(
            [
                z_buf[pl.ds(k1, second_len, stride=stride), :],
                z_buf[pl.ds(pad + k1, second_len, stride=stride), :],
            ],
            axis=0,
        ).astype(bf16)
        spec = jnp.dot(inner[...], stacked, preferred_element_type=f32)
        re, im = spec[:second_len], spec[second_len:]
        other_re = lane_roll(re, chan) + skip_other
        re = re + skip_own
        other_im = lane_roll(im, chan) * other_sign
        im = im * own_sign
        out = jnp.concatenate(
            [re * other_re - im * other_im, re * other_im + im * other_re], axis=0
        ).astype(bf16)
        back = jnp.dot(outer[...], out, preferred_element_type=f32)
        v_buf[pl.ds(k1, second_len, stride=stride), :] = back[:second_len]
        v_buf[pl.ds(pad + k1, second_len, stride=stride), :] = back[second_len:]
        return 0

    unroll = 33 if kept == 33 else 13 if kept % 13 == 0 else 3 if kept % 3 == 0 else 5 if kept % 5 == 0 else 1
    lax.fori_loop(0, kept, stage_two, 0, unroll=unroll)

    def stage_three(n2, _):
        part = v_buf[pl.ds(n2 * stride, double_pad), :].astype(bf16)
        y_out[pl.ds(n2, half, stride=group), :] = jnp.dot(
            inv[n2], part, preferred_element_type=f32
        )
        return 0

    lax.fori_loop(0, second_len, stage_three, 0, unroll=32)

    for q in range(batch_n if dense else 0):
        left = jnp.concatenate(
            [
                jnp.concatenate(
                    [
                        y_out[pl.ds(row_of((q * parts + p) * rows + low), piece), :]
                        for low in range(0, rows, piece)
                    ],
                    axis=0,
                ).astype(bf16)
                for p in range(parts)
            ],
            axis=1,
        )
        packed = jnp.dot(left, gather[...], preferred_element_type=f32).astype(bf16)
        send_two[2 * q] = packed[:, :LANES]
        send_two[2 * q + 1] = packed[:, LANES : 2 * LANES]
        send_grad[q] = packed[:, 2 * LANES :]
    for d in range(0 if dense else n):
        for low in range(0, rows, piece):
            packed = None
            for j in range(fold):
                at = pl.ds(row_of(d * pos + j * rows + low), piece)
                part = lane_roll(y_out[at, :], j * step - chan)
                packed = part if j == 0 else jnp.where(lane_p >= j * step, part, packed)
            send_two[d, low : low + piece, :] = packed.astype(bf16)
    for k in range(1, n):
        copy(send_two, recv_two, 1, k).start()
    recv_two[me] = send_two[me]

    small = min(sub, piece)
    lane_q = lax.broadcasted_iota(jnp.int32, (small, LANES), 1)
    for q in range(0 if dense else batch_n):
        for low in range(0, sub, small):
            packed = None
            for j in range(parts):
                at = pl.ds(row_of(q * quarter + j * sub + low), small)
                part = lane_roll(y_out[at, :], (j - 3) * chan)
                packed = part if j == 0 else jnp.where(lane_q >= j * chan, part, packed)
            send_grad[q, low : low + small, :] = packed.astype(bf16)
    for k in range(1, batch_n):
        share(1, k).start()
    grad_pk[me_b] = send_grad[me_b]
    share_wait(1)
    total = grad_pk[0].astype(f32)
    for q in range(1, batch_n):
        total = total + grad_pk[q].astype(f32)
    grad_kernel = total * modul[...]

    em = embed.shape[0]
    lane_w = lax.broadcasted_iota(jnp.int32, (hid, LANES), 1)
    grad_weight = jnp.zeros((hid, LANES), f32)
    for j in range(parts):
        at = slice(j * sub, (j + 1) * sub)
        got = dot_as(net[4, :, at], grad_kernel, (1, 0))
        grad_weight = grad_weight + lane_roll(
            jnp.where((lane_w >= j * chan) & (lane_w < (j + 1) * chan), got, 0.0), -j * chan
        )
        net[5, :, at] = dot_as(lane_roll(weight, j * chan), grad_kernel, (1, 1)) * net[5, :, at]

    def net_backward(i, carry):
        at = pl.ds(pl.multiple_of(i * tile, LANES), tile)
        grad_act_two = net[5, :, at]
        grad_pre_two = grad_act_two * freq_two
        grad_hidden = dot_as(net[1, :, at], grad_pre_two, (1, 1))
        grad_act_one = dot_as(hidden_w[...], grad_pre_two, (1, 0)) * net[2, :, at]
        grad_pre_one = grad_act_one * freq_one
        stacked = jnp.concatenate(
            [grad_pre_one, grad_pre_two, grad_act_one * net[0, :, at], grad_act_two * net[3, :, at]],
            axis=0,
        )
        return carry[0] + grad_hidden, carry[1] + dot_as(embed[:, at], stacked, (1, 1))

    zeros = lambda r, c: jnp.zeros((r, c), f32)
    both_sums = lax.fori_loop(
        0,
        quarter // tile,
        net_backward,
        (zeros(hid, hid), zeros(em, 4 * hid)),
        unroll=2 if quarter // tile % 2 == 0 else 1,
    )
    sums = (grad_weight, both_sums[0]) + tuple(
        both_sums[1][:, i * hid : (i + 1) * hid] for i in range(4)
    )
    sums = tuple(term * (scale * 0.25) for term in sums)
    lane_h = lax.broadcasted_iota(jnp.int32, (hid, LANES), 1)
    for tile in range(tiles):
        placed = zeros(hid, LANES)
        for i in range(n):
            if (i * chan) // LANES == tile:
                off = (i * chan) % LANES
                mask = (lane_h >= off) & (lane_h < off + chan) & (me == i)
                placed = jnp.where(mask, lane_roll(sums[0], off), placed)
        extra[tile * hid : (tile + 1) * hid, :] = placed
    base = tiles * hid
    extra[base : base + hid, 0:hid] = sums[1]
    base += hid
    for term in sums[2:]:
        extra[base : base + em, 0:hid] = term
        base += em
    for tile in range(tiles):
        extra[base + tile : base + tile + 1, :] = bias_sum[:, tile * LANES : (tile + 1) * LANES]

    main_scratch, extra_scratch = sum_scratch[:5], sum_scratch[5:]
    blocks = main_scratch[1].shape[0]
    stream = [pair_sum(n, batch_n, pk_out, main_scratch, b, chip_dests) for b in range(blocks)]
    extra_sum = pair_sum(n, batch_n, extra, extra_scratch, 0, chip_dests)
    extra_sum.start_pair()
    wait_all(send_two, recv_two, 1)

    per_tile = LANES // chan
    for t in range(tiles if dense else 0):
        at = slice(t * LANES, (t + 1) * LANES)
        left = jnp.concatenate([recv_two[t * parts + i] for i in range(parts)], axis=1)
        back = jnp.dot(left, swap[...], preferred_element_type=f32)
        for u in range(parts):
            j = u % fold
            conv_buf[u // fold, j * rows : (j + 1) * rows, at] = back[:, u * LANES : (u + 1) * LANES]
    for tile in range(0 if dense else width // LANES):
        for j in range(fold):
            conv_acc = jnp.zeros((rows, LANES), f32)
            grad_acc = jnp.zeros((rows, LANES), f32)
            for i in range(per_tile):
                block = recv_two[tile * per_tile + i].astype(f32)
                own = (lane >= i * chan) & (lane < (i + 1) * chan)
                conv_acc = jnp.where(own, lane_roll(block, i * chan - j * step), conv_acc)
                grad_acc = jnp.where(own, lane_roll(block, i * chan - j * step - chan), grad_acc)
            at = pl.ds(j * rows, rows)
            conv_buf[0, at, tile * LANES : (tile + 1) * LANES] = conv_acc
            conv_buf[1, at, tile * LANES : (tile + 1) * LANES] = grad_acc

    conv = conv_buf[0]
    grad_mixed = conv_buf[1]
    gated = (gates[0].astype(f32) * conv).astype(bf16)
    grad_proj = jnp.concatenate(
        [
            (gates[3].astype(f32) * conv).astype(bf16),
            (grad_mixed * gates[2].astype(f32)).astype(bf16),
            (grad_mixed * gates[1].astype(f32)).astype(bf16),
        ],
        axis=1,
    )
    first = (((0,), (0,)), ((), ()))
    pieces = [(gated, og[...], first)] + [
        (tok_t[...], grad_proj[:, j * width : (j + 1) * width], (((1,), (0,)), ((), ())))
        for j in range(3)
    ]
    per_block = len(pieces) // blocks if blocks > 1 else len(pieces)
    for i, (left, right, dims) in enumerate(pieces):
        block = lax.dot_general(left, right, dims, preferred_element_type=f32) * scale
        for j in range(tiles):
            at = (i * tiles + j) * width
            pk_out[at : at + width, :] = block[:, j * LANES : (j + 1) * LANES].astype(bf16)
        if (i + 1) % per_block == 0:
            done = (i + 1) // per_block - 1
            stream[done].start_pair()
            if done == 0:
                extra_sum.finish_pair()
                extra_sum.start_scatter()
            else:
                stream[done - 1].finish_pair()
                stream[done - 1].start_scatter()
    stream[-1].finish_pair()
    stream[-1].start_scatter()
    extra_sum.finish_scatter()
    extra_sum.start_gather()
    gt_out[...] = lax.dot_general(
        grad_proj, inw[...], (((1,), (1,)), ((), ())), preferred_element_type=f32
    ).astype(bf16)
    outs = [pltpu.make_async_copy(gt_out, gt_hbm, out_sems.at[0, 0])]
    outs[0].start()
    for item in stream:
        item.finish_scatter()
        item.start_gather()
    extra_sum.finish_gather()
    extra_sum.start_swap()

    def finish(i, item):
        target, base = (b_hbm, 0) if i == 0 else (a_hbm, (i - 1) * item.size)
        for side in range(2):
            core = item.core if side == 0 else 1 - item.core
            at = item.rows(core * item.half, item.half)
            to = item.rows(base + core * item.half, item.half)
            outs.append(
                pltpu.make_async_copy(item.whole.at[at], target.at[to], out_sems.at[1 + i, side])
            )
            if side == 1:
                item.finish_swap()
            outs[-1].start()

    finish(0, extra_sum)
    for item in stream:
        item.finish_gather()
        item.start_swap()
    for i, item in enumerate(stream):
        finish(1 + i, item)
    for item in outs:
        item.wait()


def digits_of(count):
    radices = []
    while count % 2 == 0 and count > 4 and len(radices) < 2:
        radices.append(2)
        count = count // 2
    return [count] + radices


def far_first(count):
    radices = digits_of(count)
    moves = [()]
    for radix in radices:
        moves = [m + (d,) for m in moves for d in range(radix)]
    moves = [m for m in moves if any(m)]
    return sorted(moves, key=lambda m: -2 * min(m[0], radices[0] - m[0]) - sum(m[1:]))


def shifted_all(own, count):
    radices = digits_of(count)
    below, tables = count, []
    for radix in radices:
        below = below // radix
        digit = lax.rem(lax.div(own, below), radix)
        tables.append([lax.rem(digit + step, radix) * below for step in range(radix)])
    made = []
    for move in far_first(count):
        total = tables[0][move[0]]
        for table, step in zip(tables[1:], move[1:]):
            total = total + table[step]
        made.append(total)
    return made


class pair_sum:
    def __init__(self, ns, nb, src, scratch, block, dests):
        self.dests = dests
        got_pair, part, got, whole, sems = (ref.at[block] for ref in scratch)
        self.got_pair, self.part, self.got, self.whole, self.sems = got_pair, part, got, whole, sems
        self.src, self.pairs = src, nb // 2
        me_s, me_b = lax.axis_index("seq"), lax.axis_index("batch")
        self.core = lax.rem(me_b, 2)
        self.chips = ns * self.pairs
        self.own = me_s * self.pairs + lax.div(me_b, 2)
        self.partner = me_b + 1 - 2 * self.core
        self.half = part.shape[0]
        self.size = 2 * self.half
        self.base = block * self.size
        self.unit = self.half // self.chips

    def rows(self, start, size):
        return pl.ds(pl.multiple_of(start, self.unit), size)

    def to_partner(self, which):
        if which == 0:
            src = self.src.at[self.rows(self.base + (1 - self.core) * self.half, self.half)]
            dst = self.got_pair
        else:
            src = dst = self.whole.at[self.rows(self.core * self.half, self.half)]
        return pltpu.make_async_remote_copy(
            src_ref=src,
            dst_ref=dst,
            send_sem=self.sems.at[which, 0, 0],
            recv_sem=self.sems.at[which, 1, 0],
            device_id={"batch": self.partner},
            device_id_type=MESH,
        )

    def to_chips(self, which):
        made = []
        for i, (dest, seq, batch) in enumerate(self.dests):
            if which == 0:
                src = self.part.at[self.rows(dest * self.unit, self.unit)]
                dst = self.got.at[i]
            else:
                at = self.rows(self.core * self.half + self.own * self.unit, self.unit)
                src = dst = self.whole.at[at]
            made.append(
                pltpu.make_async_remote_copy(
                    src_ref=src,
                    dst_ref=dst,
                    send_sem=self.sems.at[which, 0, 1],
                    recv_sem=self.sems.at[which, 1, 1],
                    device_id={"seq": seq, "batch": batch},
                    device_id_type=MESH,
                )
            )
        return made

    def wait_chips(self, which):
        pltpu.make_async_remote_copy(
            src_ref=self.got,
            dst_ref=self.got,
            send_sem=self.sems.at[which, 0, 1],
            recv_sem=self.sems.at[which, 1, 1],
            device_id={"batch": self.partner},
            device_id_type=MESH,
        ).wait()

    def start_pair(self):
        self.to_partner(0).start()

    def finish_pair(self):
        self.to_partner(0).wait()
        mine = self.src[self.rows(self.base + self.core * self.half, self.half), :]
        total = mine.astype(jnp.float32) + self.got_pair[...].astype(jnp.float32)
        self.part[...] = total.astype(self.part.dtype)

    def start_scatter(self):
        for item in self.to_chips(0):
            item.start()

    def finish_scatter(self):
        self.wait_chips(0)
        total = self.part[self.rows(self.own * self.unit, self.unit), :].astype(jnp.float32)
        for k in range(1, self.chips):
            total = total + self.got[k - 1].astype(jnp.float32)
        at = self.rows(self.core * self.half + self.own * self.unit, self.unit)
        self.whole[at, :] = total.astype(self.whole.dtype)

    def start_gather(self):
        for item in self.to_chips(1):
            item.start()

    def finish_gather(self):
        self.wait_chips(1)

    def start_swap(self):
        self.to_partner(1).start()

    def finish_swap(self):
        self.to_partner(1).wait()


def unpack_kernel(main, extra, tokens_in, tokens_out, g_in, g_out, skip, emb, emb_b, hidden, hidden_b, filt, freq):
    width = g_out.shape[0]
    hid = hidden.shape[0]
    tokens_out[...] = tokens_in[...]
    at = 0
    for ref in (g_out, g_in):
        for j in range(ref.shape[1] // LANES):
            ref[:, j * LANES : (j + 1) * LANES] = main[at : at + width, :].astype(jnp.float32)
            at += width
    tiles = width // LANES
    for j in range(tiles):
        filt[:, j * LANES : (j + 1) * LANES] = extra[j * hid : (j + 1) * hid, :]
    base = tiles * hid
    hidden[...] = extra[base : base + hid, 0:hid]
    base += hid
    count = emb.shape[0]
    em = -(-(count + 1) // 8) * 8
    emb[...] = extra[base : base + count, 0:hid]
    emb_b[...] = extra[base + count : base + count + 1, 0:hid]
    hidden_b[...] = extra[base + em + count : base + em + count + 1, 0:hid]
    freq[0:1, :] = extra[base + 2 * em + count : base + 2 * em + count + 1, 0:hid]
    freq[1:2, :] = extra[base + 3 * em + count : base + 3 * em + count + 1, 0:hid]
    base += 4 * em
    for j in range(tiles):
        skip[:, j * LANES : (j + 1) * LANES] = extra[base + j : base + j + 1, :]


def vmem(count):
    return [pl.BlockSpec(memory_space=pltpu.VMEM)] * count


def sine_cosine(angle):
    turns = jnp.round(angle * (1.0 / (2.0 * math.pi)))
    reduced = angle - turns * 6.28125
    reduced = reduced - turns * 0.0019350051879882812
    reduced = reduced - turns * 3.0199157663146e-07
    half = reduced * 0.5
    square = half * half
    sin = half * (
        1.0
        + square
        * (-1.0 / 6 + square * (1.0 / 120 + square * (-1.0 / 5040 + square * (1.0 / 362880 - square / 39916800.0))))
    )
    cos = 1.0 + square * (
        -0.5
        + square
        * (1.0 / 24 + square * (-1.0 / 720 + square * (1.0 / 40320 + square * (-1.0 / 3628800 + square / 479001600.0))))
    )
    return 2.0 * sin * cos, 1.0 - 2.0 * sin * sin


def embedding(length, count):
    rows = np.zeros((-(-(count + 1) // 8) * 8, length), np.float32)
    scaled = np.arange(length) / length
    rows[0] = scaled
    for band_index in range(1, (count - 1) // 2 + 1):
        rows[2 * band_index - 1] = np.cos(2.0 * np.pi * band_index * scaled)
        rows[2 * band_index] = np.sin(2.0 * np.pi * band_index * scaled)
    rows[count] = 1.0
    return jnp.asarray(rows)


def shards(
    tokens,
    out_grad,
    in_weight,
    out_weight,
    skip_bias,
    embed_weight,
    embed_bias,
    hidden_weight,
    hidden_bias,
    filter_weight,
    sine_freq,
    decay_rate,
):
    f32, bf16 = jnp.float32, jnp.bfloat16
    tok, og = tokens[0], out_grad[0]
    pos, width = tok.shape
    ns, nb = lax.axis_size("seq"), lax.axis_size("batch")
    length = pos * ns
    chan = width // ns
    hid = hidden_weight.shape[0]
    count = embed_weight.shape[0]
    embed = embedding(length, count)
    em = embed.shape[0]

    fwd, inv, inner, outer = make_tables(length)
    second_len, double_pad, half = fwd.shape
    rows = pos // (LANES // (2 * chan))
    tiles = width // LANES
    parts = LANES // chan
    chips = ns * (nb // 2)
    unit = 2 * chips * 16
    main_rows = -(-4 * width * tiles // unit) * unit
    blocks = max(b for b in BLOCKS if main_rows % (b * unit) == 0)
    unit = 2 * chips * 8
    extra_rows = -(-(tiles * hid + hid + 4 * em + tiles) // unit) * unit
    swap, place, gather = selections(
        chan, second_len <= rows and nb * parts * rows == length and parts * LANES <= 512
    )
    pair = (ns, rows, LANES)
    shared = (nb, length // nb // (LANES // chan), LANES)
    spectral = (second_len * (double_pad + 1), LANES)
    spaced = (half * (second_len + 1), LANES)
    scratch = []
    for total, kind, count_at in ((main_rows, bf16, blocks), (extra_rows, f32, 1)):
        half_rows = total // count_at // 2
        scratch += [
            pltpu.VMEM((count_at, half_rows, LANES), kind),
            pltpu.VMEM((count_at, half_rows, LANES), kind),
            pltpu.VMEM((count_at, chips - 1, half_rows // chips, LANES), kind),
            pltpu.VMEM((count_at, 2 * half_rows, LANES), kind),
            pltpu.SemaphoreType.DMA((count_at, 2, 2, 2)),
        ]
    grad_tokens, main, extra = pl.pallas_call(
        functools.partial(step_kernel, ns, nb, chan, 1.0 / math.sqrt(nb * length)),
        out_shape=(
            jax.ShapeDtypeStruct((pos, width), bf16),
            jax.ShapeDtypeStruct((main_rows, LANES), bf16),
            jax.ShapeDtypeStruct((extra_rows, LANES), f32),
        ),
        in_specs=[pl.BlockSpec(memory_space=pl.ANY)] * 20,
        out_specs=(pl.BlockSpec(memory_space=pl.ANY),) * 3,
        scratch_shapes=[
            pltpu.VMEM((pos, width), bf16),
            pltpu.VMEM((width, pos), bf16),
            pltpu.SemaphoreType.DMA((2 + blocks, 2)),
            pltpu.VMEM(tok.shape, bf16),
            pltpu.VMEM(og.shape, bf16),
            pltpu.VMEM(in_weight.shape, bf16),
            pltpu.VMEM(out_weight.shape, bf16),
            pltpu.VMEM((em, length // nb), f32),
            pltpu.VMEM(fwd.shape, bf16),
            pltpu.VMEM(inv.shape, bf16),
            pltpu.VMEM(inner.shape, bf16),
            pltpu.VMEM(outer.shape, bf16),
            pltpu.VMEM(embed_weight.shape, f32),
            pltpu.VMEM((1, hid), f32),
            pltpu.VMEM((1, hid), f32),
            pltpu.VMEM(sine_freq.shape, f32),
            pltpu.VMEM(hidden_weight.shape, f32),
            pltpu.VMEM(filter_weight.shape, f32),
            pltpu.VMEM((1, width), f32),
            pltpu.VMEM((1, width), f32),
            pltpu.VMEM(swap.shape, bf16),
            pltpu.VMEM(place.shape, bf16),
            pltpu.VMEM(gather.shape, bf16),
            pltpu.SemaphoreType.DMA((20,)),
            pltpu.VMEM(pair, bf16),
            pltpu.VMEM(pair, bf16),
            pltpu.VMEM(pair, bf16),
            pltpu.VMEM(pair, bf16),
            pltpu.VMEM((4, pos, width), bf16),
            pltpu.VMEM(spaced, f32),
            pltpu.VMEM(spaced, f32),
            pltpu.VMEM(spectral, f32),
            pltpu.VMEM(spectral, f32),
            pltpu.VMEM((6, hid, length // nb), f32),
            pltpu.VMEM(shared, bf16),
            pltpu.VMEM(shared, bf16),
            pltpu.VMEM(shared, bf16),
            pltpu.VMEM(shared[1:], f32),
            pltpu.VMEM((2, pos, width), f32),
            pltpu.SemaphoreType.DMA((4,)),
            pltpu.SemaphoreType.DMA((4,)),
            pltpu.VMEM((main_rows, LANES), bf16),
            pltpu.VMEM((extra_rows, LANES), f32),
            pltpu.VMEM((em, hid), f32),
            pltpu.VMEM((8, hid), f32),
        ]
        + scratch,
        compiler_params=pltpu.CompilerParams(
            collective_id=0, has_side_effects=True, vmem_limit_bytes=VMEM_BYTES
        ),
        name="step",
    )(
        tok,
        og,
        in_weight,
        out_weight,
        embed,
        fwd,
        inv,
        inner,
        outer,
        embed_weight,
        embed_bias[None],
        hidden_bias[None],
        sine_freq,
        hidden_weight,
        filter_weight,
        decay_rate[None],
        skip_bias[None],
        swap,
        place,
        gather,
    )

    shapes = (
        (width, 3 * width),
        (width, width),
        (1, width),
        (count, hid),
        (1, hid),
        (hid, hid),
        (1, hid),
        (hid, width),
        (2, hid),
    )
    out = pl.pallas_call(
        unpack_kernel,
        out_shape=(jax.ShapeDtypeStruct((pos, width), bf16),)
        + tuple(jax.ShapeDtypeStruct(shape, f32) for shape in shapes),
        in_specs=vmem(3),
        out_specs=tuple(vmem(1 + len(shapes))),
        name="unpack",
    )(main, extra, grad_tokens)
    return (
        out[0][None],
        out[1],
        out[2],
        out[3][0],
        out[4],
        out[5][0],
        out[6],
        out[7][0],
        out[8],
        out[9],
    )


def solution(mesh):
    batched = P("batch", "seq", None)
    return jax.shard_map(
        shards,
        mesh=mesh,
        in_specs=(batched, batched) + (P(),) * 10,
        out_specs=(batched,) + (P(),) * 9,
        check_vma=False,
    )
```
